32 devices in a mesh: dp: 4 (over x, core), seq: 4 (over z), tensor: 2 (over y).
Axes of the slice: x: 2, y: 2, z: 4, core: 2. Of those that a mesh axis runs over, the one named last changes fastest.
Arguments:
- query_vectors: bfloat16 [896, 4096], P(('dp', 'seq'), 'tensor'), may hold values from -128 to 128
- key_vectors: bfloat16 [896, 2048], P(('dp', 'seq'), 'tensor'), may hold values from -6 to 6
- value_vectors: bfloat16 [896, 2048], P(('dp', 'seq'), 'tensor'), may hold values from -6 to 6
- out_weight: bfloat16 [4096, 3584], P(None, 'tensor'), may hold values from -0.09375 to 0.09375
- residual: bfloat16 [896, 3584], P(('dp', 'seq'), 'tensor'), may hold values from -64 to 64
- post_gain: float32 [3584], P('tensor'), may hold values from 0.1 to 1.9
- final_gain: float32 [3584], P('tensor'), may hold values from 0.1 to 1.9
- vocab_weight: bfloat16 [16000, 3584], P(('dp', 'seq', 'tensor')), may hold values from -4 to 4
- segment_ids: int32 [4, 224], P('dp', 'seq'), may hold values from 0 to 7, as said below
- doc_starts: int32 [4, 8], P('dp'), may hold values from 0 to 223, as said below
- doc_index: int32 [4, 8], P('dp'), may hold values from 0 to 31
- targets: int32 [4, 224], replicated, may hold values from 0 to 15999
Outputs:
- token_logprob: float32 [4, 224], P('dp', 'seq')
- doc_loglik: float32 [32], replicated
- doc_counts: float32 [32], replicated
The draws below stay inside these ranges and needn't reach their ends.
Inputs may be any that keep to these rules, and one draw needn't show every extreme that they name: `segment_ids`: within each row the numbers never fall and every number 0 to 7 appears; segment s of a row begins at doc_starts[row, s]; each segment holds 1 to 168 positions. doc_starts[row, 0] = 0 and the starts rise strictly along each row.
All inputs are finite; a program needn't handle non-finite values.
Results may differ from the reference program's by a relative error of at most 0.00074.
Values may be sent and summed in bfloat16 or wider, within the bound.
A program may use at most 64 MiB of HBM per device.

```python
import math
import jax
import jax.numpy as jnp
import numpy as np
from jax import lax

D = 3584
HEADS = 16
KV_HEADS = 8
HEAD_DIM = 256
SEGS = 8
VOCAB = 16000
LENGTH = 224
ROWS = 4
TOKENS = 896
MOSTDOC = 168
NDOCS = 32


def one_row(key):
    first_key, second_key = jax.random.split(key)
    leftover = LENGTH - MOSTDOC
    picks = jax.random.permutation(first_key, leftover - 1)[:SEGS - 2] + 1
    edges = jnp.concatenate([jnp.zeros((1,), jnp.int32), jnp.sort(picks).astype(jnp.int32), jnp.full((1,), leftover, jnp.int32)])
    others = edges[1:] - edges[:-1]
    padded = jnp.concatenate([others, jnp.zeros((1,), jnp.int32)])
    place = jax.random.randint(second_key, (), 0, SEGS)
    slots = jnp.arange(SEGS, dtype=jnp.int32)
    before = padded[slots]
    after = padded[jnp.maximum(slots - 1, 0)]
    return jnp.where(slots < place, before, jnp.where(slots == place, MOSTDOC, after)).astype(jnp.int32)


def document_layout(key):
    row_keys = jax.random.split(jax.random.fold_in(key, 17), ROWS)
    lengths = jax.vmap(one_row)(row_keys)
    starts = jnp.cumsum(lengths, axis=1) - lengths
    positions = jnp.arange(LENGTH, dtype=jnp.int32)
    segment_ids = jnp.sum((positions[None, :, None] >= starts[:, None, :]).astype(jnp.int32), axis=2) - 1
    return (segment_ids.astype(jnp.int32), starts.astype(jnp.int32))


def draw_segment_ids(key, part):
    return document_layout(key)[0]


def draw_doc_starts(key, part):
    return document_layout(key)[1]


def attention_inputs(key):
    base_key, noise_key, pick_key, strength_key, gap_key = jax.random.split(jax.random.fold_in(key, 41), 5)
    keys = jnp.clip(jax.random.normal(base_key, (TOKENS, KV_HEADS, HEAD_DIM)), -6.0, 6.0)
    noise = jnp.clip(jax.random.normal(noise_key, (TOKENS, HEADS, HEAD_DIM)), -6.0, 6.0)
    picked = (jax.random.randint(pick_key, (TOKENS, HEADS), 0, 8) == 0).astype(jnp.float32)
    strength = jnp.exp(jax.random.uniform(strength_key, (TOKENS, HEADS), minval=math.log(70.0 / 16.0), maxval=math.log(150.0 / 16.0)))
    gap = jax.random.uniform(gap_key, (TOKENS, HEADS), minval=15.0 / 16.0, maxval=40.0 / 16.0)
    group_size = HEADS // KV_HEADS
    own = jnp.repeat(keys, group_size, axis=1)
    prior = jnp.repeat(jnp.roll(keys, 1, axis=0), group_size, axis=1)
    lift = picked * strength
    second = picked * (strength - gap)
    queries = noise + lift[..., None] * own + second[..., None] * prior
    queries = jnp.clip(queries, -128.0, 128.0)
    return (queries.reshape(TOKENS, HEADS * HEAD_DIM), keys.reshape(TOKENS, KV_HEADS * HEAD_DIM))


def draw_query_vectors(key, part):
    return attention_inputs(key)[0].astype(jnp.bfloat16)


def draw_key_vectors(key, part):
    return attention_inputs(key)[1].astype(jnp.bfloat16)


def residual_keys(key):
    return jax.random.split(jax.random.fold_in(key, 29), 4)


def draw_residual(key, part):
    row_key, column_key, base_key, common_key = residual_keys(key)
    row_scale = jnp.exp(jax.random.uniform(row_key, (TOKENS, 1), minval=jnp.log(0.25), maxval=jnp.log(2.5)))
    column_scale = jnp.exp(jax.random.uniform(column_key, (1, D), minval=jnp.log(0.25), maxval=jnp.log(2.5)))
    base = jnp.clip(jax.random.normal(base_key, (TOKENS, D)), -6.0, 6.0)
    return (base * row_scale * column_scale).astype(jnp.bfloat16)


def draw_vocab_weight(key, part):
    base_key = jax.random.fold_in(jax.random.fold_in(key, 53), 0)
    spread = float(D // 9) ** (-0.5)
    weights = jnp.clip(jax.random.normal(base_key, (VOCAB, D)), -6.0, 6.0) * spread
    return weights.astype(jnp.bfloat16)


def with_ends(drawn, key, smallest, high):
    dims = drawn.shape
    spot = [jax.random.randint(jax.random.fold_in(key, axis), (), 0, dims[axis]) for axis in range(len(dims))]
    drawn = drawn.at[tuple(spot)].set(smallest)
    longest = dims.index(max(dims))
    spot[longest] = (spot[longest] + 1) % dims[longest]
    return drawn.at[tuple(spot)].set(high)


def steps_of(key, extent, pieces, smallest, top_value):
    loudness, own = 1.0, jax.random.fold_in(key, 6)
    for dim, blocks in pieces:
        heights = jnp.exp(jax.random.uniform(jax.random.fold_in(own, dim), (blocks,), jnp.float32, smallest / len(pieces), top_value / len(pieces)))
        loudness = loudness * jnp.repeat(heights, extent[dim] // blocks).reshape([-1 if axis == dim else 1 for axis in range(len(extent))])
    return loudness


def rank_bounds(number_of, skew):
    loads = [(1 << 20) // math.isqrt(standing ** skew) + 1 for standing in range(1, number_of + 1)]
    scale = 1 + sum(loads) // (1 << 30)
    return np.cumsum(np.array([max(1, weight // scale) for weight in loads]))


def ranked_ids(stream_key, shape, amount, lean):
    listing = rank_bounds(amount, lean)
    pick = jax.random.randint(jax.random.fold_in(stream_key, 1), shape, 0, int(listing[amount - 1]))
    rank = jnp.searchsorted(jnp.asarray(listing, jnp.int32), pick, side="right")
    return jax.random.permutation(jax.random.fold_in(stream_key, 2), amount)[rank].astype(jnp.int32)


def gaussian(rng, shape, scale, bound, pieces=(), kind=jnp.bfloat16):
    result = jax.random.normal(rng, shape, jnp.float32) * scale
    if len(pieces) > 0:
        result = steps_of(rng, shape, pieces, -0.22, 0.18) * result
    return jnp.clip(result, min=-bound, max=bound).astype(kind)


def setup_inputs(seed: int = 0) -> dict:
    streams_of = jax.random.split(jax.random.key(seed), 13)
    return {
        "query_vectors": draw_query_vectors(jax.random.fold_in(streams_of[12], 71), 0),
        "key_vectors": draw_key_vectors(jax.random.fold_in(streams_of[12], 71), 0),
        "value_vectors": gaussian(streams_of[2], (TOKENS, KV_HEADS * HEAD_DIM), 1.0, 6.0, ((0, 16), (1, 2))),
        "out_weight": gaussian(streams_of[3], (HEADS * HEAD_DIM, D), (HEADS * HEAD_DIM) ** -0.5, 0.09375, ((1, 2),)),
        "residual": draw_residual(jax.random.fold_in(streams_of[12], 71), 0),
        "post_gain": jnp.clip(1.0 + 0.18 * jax.random.normal(streams_of[5], (D,), jnp.float32), 0.1, 1.9),
        "final_gain": jnp.clip(1.0 + 0.18 * jax.random.normal(streams_of[6], (D,), jnp.float32), 0.1, 1.9),
        "vocab_weight": draw_vocab_weight(jax.random.fold_in(streams_of[12], 71), 0),
        "segment_ids": draw_segment_ids(jax.random.fold_in(streams_of[12], 71), 0),
        "doc_starts": draw_doc_starts(jax.random.fold_in(streams_of[12], 71), 0),
        "doc_index": with_ends(jax.random.randint(streams_of[10], (ROWS, SEGS), 0, NDOCS), jax.random.fold_in(streams_of[10], 1), 0, NDOCS - 1).astype(jnp.int32),
        "targets": with_ends(ranked_ids(streams_of[11], (ROWS, LENGTH), VOCAB, 2), jax.random.fold_in(streams_of[11], 3), 0, VOCAB - 1).astype(jnp.int32),
    }


ATTENTION_CAP = 50.0
LOGIT_CAP = 30.0
EPSILON = 1e-06

def first_positions(segment_row, start_row):
    segment_match = segment_row[:, None] == jnp.arange(SEGS, dtype=jnp.int32)[None, :]
    return lax.optimization_barrier(jnp.sum(jnp.where(segment_match, start_row[None, :], 0), axis=1)).astype(jnp.int32)

def attend_row(inputs):
    query_row, key_row, value_row, segment_row, start_row = inputs
    group_size = HEADS // KV_HEADS
    query_heads = query_row.astype(jnp.float32).reshape(LENGTH, KV_HEADS, group_size, HEAD_DIM)
    key_heads = key_row.astype(jnp.float32).reshape(LENGTH, KV_HEADS, HEAD_DIM)
    value_heads = value_row.astype(jnp.float32).reshape(LENGTH, KV_HEADS, HEAD_DIM)
    raw_scores = jnp.einsum('ikgd,jkd->ikgj', query_heads, key_heads)
    capped = ATTENTION_CAP * jnp.tanh(raw_scores * HEAD_DIM ** (-0.5) / ATTENTION_CAP)
    positions = jnp.arange(LENGTH, dtype=jnp.int32)
    doc_first = first_positions(segment_row, start_row)
    visible = (positions[None, :] <= positions[:, None]) & (positions[None, :] >= doc_first[:, None])
    weights = jnp.where(visible[:, None, None, :], jnp.exp(capped), 0.0)
    denominator = lax.optimization_barrier(jnp.sum(weights, axis=-1))
    rounded = lax.optimization_barrier(weights.astype(jnp.bfloat16)).astype(jnp.float32)
    numerator = jnp.einsum('ikgj,jkd->ikgd', rounded, value_heads)
    attended = numerator / denominator[..., None]
    return attended.reshape(LENGTH, HEADS * HEAD_DIM).astype(jnp.bfloat16)

def reference(query_vectors, key_vectors, value_vectors, out_weight, residual, post_gain, final_gain, vocab_weight, segment_ids, doc_starts, doc_index, targets):
    attended = lax.map(attend_row, (query_vectors.reshape(ROWS, LENGTH, HEADS * HEAD_DIM), key_vectors.reshape(ROWS, LENGTH, KV_HEADS * HEAD_DIM), value_vectors.reshape(ROWS, LENGTH, KV_HEADS * HEAD_DIM), segment_ids, doc_starts))
    attended = attended.reshape(TOKENS, HEADS * HEAD_DIM)
    branch = jnp.dot(attended, out_weight, preferred_element_type=jnp.float32)
    branch_rms = jnp.sqrt(lax.optimization_barrier(jnp.mean(branch * branch, axis=1, keepdims=True)) + EPSILON)
    updated = residual.astype(jnp.float32) + post_gain[None, :] * branch / branch_rms
    updated_rms = jnp.sqrt(lax.optimization_barrier(jnp.mean(updated * updated, axis=1, keepdims=True)) + EPSILON)
    hidden = (final_gain[None, :] * updated / updated_rms).astype(jnp.bfloat16)
    block_rows = math.gcd(TOKENS, 256)

    def head_block(inputs):
        rows_in, label_rows = inputs
        logits = lax.dot_general(rows_in, vocab_weight, (((1,), (1,)), ((), ())), preferred_element_type=jnp.float32)
        capped = LOGIT_CAP * jnp.tanh(logits / LOGIT_CAP)
        totals = lax.optimization_barrier(jnp.sum(jnp.exp(capped), axis=1))
        chosen = jnp.take_along_axis(capped, label_rows[:, None], axis=1)[:, 0]
        return (totals, chosen)
    totals, chosen = lax.map(head_block, (hidden.reshape(TOKENS // block_rows, block_rows, D), targets.reshape(TOKENS // block_rows, block_rows)))
    totals = totals.reshape(ROWS, LENGTH)
    chosen = chosen.reshape(ROWS, LENGTH)
    positions = jnp.arange(LENGTH, dtype=jnp.int32)
    segment_slots = jnp.arange(SEGS, dtype=jnp.int32)
    next_segment = segment_ids + 1
    doc_end = lax.optimization_barrier(jnp.sum(jnp.where(segment_slots[None, None, :] == next_segment[:, :, None], doc_starts[:, None, :], 0), axis=2))
    doc_end = doc_end + jnp.where(next_segment == SEGS, LENGTH, 0)
    counted = (positions[None, :] + 1 < doc_end).astype(jnp.float32)
    token_logprob = counted * (chosen - jnp.log(totals))
    doc_of = lax.optimization_barrier(jnp.sum(jnp.where(segment_slots[None, None, :] == segment_ids[:, :, None], doc_index[:, None, :], 0), axis=2))
    doc_match = (doc_of.reshape(TOKENS)[:, None] == jnp.arange(NDOCS, dtype=jnp.int32)[None, :]).astype(jnp.float32)
    doc_loglik = lax.optimization_barrier(jnp.sum(token_logprob.reshape(TOKENS)[:, None] * doc_match, axis=0))
    doc_counts = lax.optimization_barrier(jnp.sum(counted.reshape(TOKENS)[:, None] * doc_match, axis=0))
    return (token_logprob, doc_loglik, doc_counts)
```

```python
import functools

import jax
import jax.numpy as jnp
from jax import lax
from jax.experimental import pallas as pl
from jax.experimental.pallas import tpu as pltpu
from jax.sharding import PartitionSpec as P

HEAD_DIM = 256
ATTENTION_CAP = 50.0
LOGIT_CAP = 30.0
EPSILON = 1e-06
MESH = pl.DeviceIdType.MESH
PAD = 64
NT = (((1,), (1,)), ((), ()))
NN = (((1,), (0,)), ((), ()))


def dot(a, b, dims):
    return lax.dot_general(a, b, dims, preferred_element_type=jnp.float32)


def body(
    sizes,
    q_hbm, k_hbm, v_hbm, w_hbm, res_hbm, pg_hbm, fg_hbm, voc_hbm, seg_hbm, start_hbm, index_hbm, target_hbm,
    out_ref,
    q_ref, k_ref, v_ref, res_ref, pg_ref, fg_ref, seg_ref, start_ref, index_ref, target_ref,
    w_ref, voc_ref, kv, num, den, att, branch, stat, hid, held, lab_ref, early_buf, late_buf, twin_buf,
    local_sem, kv_send, kv_recv, att_send, att_recv, st_send, st_recv,
    hid_recv, z_send, y_send, x_send, voc_send, voc_recv, f_send, f_recv, tw_send, tw_recv,
):
    ND, NZ, NY, docs = sizes
    NC = 2 if ND % 2 == 0 else 1
    NX = ND // NC
    D = voc_hbm.shape[-1] if voc_hbm.ndim == 2 else voc_hbm.shape[0] * voc_hbm.shape[2]
    me_d, me_z, me_t = lax.axis_index("dp"), lax.axis_index("seq"), lax.axis_index("tensor")
    me_x, me_c = me_d // NC, me_d % NC
    twin = [me_x * NC + 1 - me_c] if NC == 2 else []
    rows = q_ref.shape[0]
    kvw = k_ref.shape[1]
    groups = kvw // HEAD_DIM
    per = q_ref.shape[1] // kvw
    heads = groups * per
    qw = q_ref.shape[1]
    fw = w_hbm.shape[1]

    pairs = [
        (k_hbm, k_ref), (v_hbm, v_ref), (q_hbm, q_ref), (seg_hbm, seg_ref), (start_hbm, start_ref),
        (index_hbm, index_ref), (target_hbm, target_ref), (res_hbm, res_ref), (pg_hbm, pg_ref), (fg_hbm, fg_ref),
        (w_hbm, w_ref), (voc_hbm, voc_ref.at[me_c]),
    ]
    loads = [pltpu.make_async_copy(src, dst, local_sem.at[i]) for i, (src, dst) in enumerate(pairs)]
    for c in loads:
        c.start()
    w_copy = loads[10]

    def dev(d=None, z=None, t=None):
        return (me_d if d is None else d, me_z if z is None else z, me_t if t is None else t)

    def remote(src, dst, send, recv, device):
        return pltpu.make_async_remote_copy(
            src_ref=src, dst_ref=dst, send_sem=send, recv_sem=recv, device_id=device, device_id_type=MESH
        )

    def others(me, n):
        return [lax.rem(me + i, n) for i in range(1, n)]

    barrier = pltpu.get_barrier_semaphore()
    peers = [dev(d=p * NC + me_c) for p in others(me_x, NX)] + [dev(d=p) for p in twin]
    peers += [dev(t=p) for p in others(me_t, NY)]
    ups = [(me_z + 1 < NZ, dev(z=lax.rem(me_z + 1, NZ))), (me_z >= 1, dev(z=lax.rem(me_z + NZ - 1, NZ)))]
    for p in peers:
        pl.semaphore_signal(barrier, inc=1, device_id=p, device_id_type=MESH)
    for there, p in ups:
        @pl.when(there)
        def _(p=p):
            pl.semaphore_signal(barrier, inc=1, device_id=p, device_id_type=MESH)
    for c in loads[:7]:
        c.wait()

    def kv_copy(block, g):
        cols = pl.ds(g * HEAD_DIM, HEAD_DIM)
        up = dev(z=lax.rem(me_z + 1, NZ))
        if block is None:
            pairs = [(k_ref.at[:, cols], kv.at[me_z, 0, :, cols]), (v_ref.at[:, cols], kv.at[me_z, 1, :, cols])]
            where = me_z
        else:
            pairs = [(kv.at[block, i, :, cols],) * 2 for i in range(2)]
            where = block
        return [
            remote(src, dst, kv_send.at[where, g, i], kv_recv.at[where, g, i], up)
            for i, (src, dst) in enumerate(pairs)
        ]

    seg = seg_ref[...]
    first_row = jnp.zeros((1, rows), jnp.int32)
    end_row = jnp.zeros((1, rows), jnp.int32)
    doc_row = jnp.zeros((1, rows), jnp.int32)
    segs = start_ref.shape[1]
    for n in range(segs):
        here = seg == n
        first_row = jnp.where(here, start_ref[0, n], first_row)
        end_row = jnp.where(here, start_ref[0, n + 1] if n + 1 < segs else rows * NZ, end_row)
        doc_row = jnp.where(here, index_ref[0, n], doc_row)
    spot = me_z * rows + lax.broadcasted_iota(jnp.int32, (1, rows), 1)
    code_row = doc_row + jnp.where(spot + 1 < end_row, docs, 0)
    i_pos = lax.broadcasted_iota(jnp.int32, (rows, rows), 0)
    j_pos = lax.broadcasted_iota(jnp.int32, (rows, rows), 1)

    def column_of(row):
        full = jnp.broadcast_to(row.astype(jnp.float32), (rows, rows))
        return jnp.sum(jnp.where(i_pos == j_pos, full, 0.0), axis=1, keepdims=True)

    first = column_of(first_row).astype(jnp.int32)
    lines = NX * PAD
    lanes = lax.broadcasted_iota(jnp.int32, (rows, lines), 1)
    sub = lax.broadcasted_iota(jnp.int32, (rows, lines), 0)
    placed = jnp.where(lanes == sub + me_x * PAD, column_of(code_row), 0.0)
    code_line = jnp.sum(placed, axis=0, keepdims=True)
    gap = jnp.zeros((1, PAD - rows), jnp.int32)
    for z in range(NZ):
        pieces = []
        for x in range(NX):
            part = target_ref[x * NC:x * NC + 1, z * rows:(z + 1) * rows]
            for c in range(1, NC):
                part = jnp.where(me_c == c, target_ref[x * NC + c:x * NC + c + 1, z * rows:(z + 1) * rows], part)
            pieces += [part, gap]
        lab_ref[z] = jnp.concatenate(pieces, axis=1)

    def attend(block, g):
        cols = slice(g * HEAD_DIM, (g + 1) * HEAD_DIM)
        if block is None:
            kk, vv = k_ref[:, cols], v_ref[:, cols]
            seen = (me_z * rows + j_pos >= first) & (j_pos <= i_pos)
        else:
            kk, vv = kv[block, 0, :, cols], kv[block, 1, :, cols]
            seen = block * rows + j_pos >= first
        for h in range(g * per, (g + 1) * per):
            raw = dot(q_ref[:, h * HEAD_DIM:(h + 1) * HEAD_DIM], kk, NT)
            capped = ATTENTION_CAP * jnp.tanh(raw * (HEAD_DIM ** (-0.5) / ATTENTION_CAP))
            wt = jnp.where(seen, jnp.exp(capped), 0.0)
            top = dot(wt.astype(jnp.bfloat16), vv, NN)
            low = jnp.broadcast_to(jnp.sum(wt, axis=1, keepdims=True), (rows, 128))
            if block is None:
                num[h] = top
                den[h] = low
            else:
                num[h] = num[h] + top
                den[h] = den[h] + low

    def arrived(block, g):
        for c in kv_copy(block, g):
            c.wait_recv()

        @pl.when(me_z + 1 < NZ)
        def _():
            for c in kv_copy(block, g):
                c.start()

    @pl.when(me_z >= 0)
    def _():
        for g in range(groups):
            attend(None, g)

    ends = lax.div(me_z + NZ - 1, NZ) + lax.div(2 * NZ - 2 - me_z, NZ)
    pl.semaphore_wait(barrier, len(peers) + ends)
    @pl.when(me_z + 1 < NZ)
    def _():
        for g in range(groups):
            for c in kv_copy(None, g):
                c.start()
    voc_copies = [
        remote(voc_hbm, voc_ref.at[me_c], voc_send.at[0], voc_recv.at[me_c], dev(d=p)) for p in twin
    ]
    for c in voc_copies:
        c.start()
    for block in range(NZ - 2, 0, -1):
        @pl.when(block < me_z)
        def _(block=block):
            for g in range(groups):
                arrived(block, g)
                attend(block, g)

    gw = per * HEAD_DIM

    def att_copy(g, peer, idx):
        ref = att.at[me_t, :, pl.ds(g * gw, gw)]
        return remote(ref, ref, att_send.at[idx, g], att_recv.at[me_t, g], dev(t=peer))

    step = 256 if fw % 256 == 0 else fw

    def project(t, g, begin):
        base = pl.multiple_of(t * qw + g * gw, gw)
        left = att[t, :, g * gw:(g + 1) * gw]
        for n in range(fw // step):
            cols = slice(n * step, (n + 1) * step)
            got = dot(left, w_ref[pl.ds(base, gw), cols], NN)
            branch[:, cols] = got if begin else branch[:, cols] + got

    for g in range(groups):
        if NZ > 1:
            @pl.when(me_z > 0)
            def _(g=g):
                arrived(0, g)
                attend(0, g)
        for h in range(g * per, (g + 1) * per):
            att[me_t, :, h * HEAD_DIM:(h + 1) * HEAD_DIM] = (num[h] / den[h][:, :1]).astype(jnp.bfloat16)
        for i, p in enumerate(others(me_t, NY)):
            att_copy(g, p, i).start()
        if g == 0:
            w_copy.wait()
        project(me_t, g, g == 0)
    for g in range(groups):
        for p in others(me_t, NY):
            ref = att.at[p, :, pl.ds(g * gw, gw)]
            remote(ref, ref, att_send.at[0, 0], att_recv.at[p, g], dev()).wait_recv()
            project(p, g, False)

    for c in loads[7:10]:
        c.wait()
    br = branch[...]
    carried = res_ref[...].astype(jnp.float32)
    gained = pg_ref[...].reshape(1, fw) * br
    lane = lax.broadcasted_iota(jnp.int32, (rows, 128), 1)
    packed = jnp.zeros((rows, 128), jnp.float32)
    for i, prod in enumerate((br * br, carried * carried, carried * gained, gained * gained)):
        packed = jnp.where(lane == i, jnp.sum(prod, axis=1, keepdims=True), packed)
    stat[me_t] = packed

    def stat_copy(peer, i):
        return remote(stat.at[me_t], stat.at[me_t], st_send.at[i], st_recv.at[me_t], dev(t=peer))

    for i, p in enumerate(others(me_t, NY)):
        stat_copy(p, i).start()
    for p in others(me_t, NY):
        remote(stat.at[p], stat.at[p], st_send.at[0], st_recv.at[p], dev()).wait_recv()
    total = stat[0]
    for t in range(1, NY):
        total = total + stat[t]
    sq_branch, sq_carried, cross, sq_gained = (total[:, i:i + 1] for i in range(4))
    inv_branch = 1.0 / jnp.sqrt(sq_branch / D + EPSILON)
    sq_total = sq_carried + 2.0 * inv_branch * cross + inv_branch * inv_branch * sq_gained
    inv_total = 1.0 / jnp.sqrt(sq_total / D + EPSILON)
    hid[me_z, me_t, me_x, :rows, :] = (
        fg_ref[...].reshape(1, fw) * (carried + gained * inv_branch) * inv_total
    ).astype(jnp.bfloat16)

    y_peers = others(me_t, NY)
    x_peers = others(me_x, NX)
    cut = min(rows, (rows // 2 + 7) // 8 * 8)
    spans = [(0, cut)] + ([(cut, rows - cut)] if cut < rows else [])
    K = len(spans)

    def xdev(x):
        return dev(d=x * NC + me_c)

    def block(z, t, x, k):
        return hid.at[z, t, x, pl.ds(*spans[k]), :]

    def send(z, t, x, k, sem, device):
        return remote(block(z, t, x, k), block(z, t, x, k), sem, hid_recv.at[z, t, x, k], device)

    def landed(z, t, x, k):
        send(z, t, x, k, z_send.at[0, 0, 0], dev()).wait_recv()

    def step_of(n):
        return me_z if n == 0 else jnp.where(n <= me_z, me_z - n, n)

    def spread(n, act, wait):
        z = step_of(n)
        for k in range(K):
            if wait and n > 0:
                landed(z, me_t, me_x, k)

            @pl.when((me_z + 1 < NZ) & (z <= me_z))
            def _(k=k):
                act(send(z, me_t, me_x, k, z_send.at[z, k, 0], dev(z=lax.rem(me_z + 1, NZ))))

            @pl.when((me_z >= 1) & (z >= me_z))
            def _(k=k):
                act(send(z, me_t, me_x, k, z_send.at[z, k, 1], dev(z=lax.rem(me_z + NZ - 1, NZ))))

            for i, p in enumerate(x_peers):
                act(send(z, me_t, me_x, k, x_send.at[0, z, k, i], xdev(p)))
            for i, p in enumerate(y_peers):
                act(send(z, me_t, me_x, k, y_send.at[0, z, k, i], dev(t=p)))

    def relay(n, act, wait):
        z = step_of(n)
        for j, x in enumerate(x_peers):
            if wait:
                landed(z, me_t, x, 0)
            for i, p in enumerate(y_peers):
                act(send(z, me_t, x, 0, y_send.at[1 + j, z, 0, i], dev(t=p)))
        for j, t in enumerate(y_peers):
            if wait:
                landed(z, t, me_x, K - 1)
            if K > 1:
                for i, p in enumerate(x_peers):
                    act(send(z, t, me_x, K - 1, x_send.at[1 + j, z, K - 1, i], xdev(p)))

    def start(c):
        c.start()

    count = voc_hbm.shape[-2]
    home = (me_x * NZ + me_z) * NY + me_t
    row_ids = lax.broadcasted_iota(jnp.int32, (count, lines), 0)

    def product(c, z, t):
        right = hid[z, t].reshape(lines, fw)
        if len(voc_ref.shape) == 3:
            start_col = t * fw if isinstance(t, int) else pl.multiple_of(t * fw, 128)
            left = voc_ref[c, :, pl.ds(start_col, fw)]
        else:
            left = voc_ref[c, t]
        return dot(left, right, NT)

    def gather(z, t, begin):
        @pl.loop(0, NC)
        def _(c):
            got = product(c, z, t)
            held[c] = got if begin else held[c] + got

    def finish(z, t, begin):
        label = lab_ref[z]

        def part(c, sums):
            acc = product(c, z, t)
            if not begin:
                acc = held[c] + acc
            capped = LOGIT_CAP * jnp.tanh(acc * (1.0 / LOGIT_CAP))
            base = (((me_x * NC + c) * NZ + me_z) * NY + me_t) * count
            tot = sums[0] + jnp.sum(jnp.exp(capped), axis=0, keepdims=True)
            cho = sums[1] + jnp.sum(jnp.where(row_ids == label - base, capped, 0.0), axis=0, keepdims=True)
            return tot, cho

        zero = jnp.zeros((1, lines), jnp.float32)
        return lax.fori_loop(0, NC, part, (zero, zero))

    def compute(n, before_last=None):
        z = step_of(n)
        for x in x_peers:
            for k in range(1, K):
                landed(z, me_t, x, k)
        if NY > 1:
            gather(z, me_t, True)
        last = me_t
        for i, t in enumerate(y_peers):
            for k in range(K - 1):
                landed(z, t, me_x, k)
            for x in x_peers:
                for k in range(K):
                    landed(z, t, x, k)
            last = t
            if i + 1 < len(y_peers):
                gather(z, t, False)
        if before_last is not None:
            before_last()
        return z, *finish(z, last, NY == 1)

    family = [(x, z, t) for x in range(NX) for z in range(NZ) for t in range(NY)]
    G = len(family)

    def kin(i):
        other = lax.rem(home + i, G)
        return dev(d=(other // (NZ * NY)) * NC + me_c, z=lax.rem(other // NY, NZ), t=lax.rem(other, NY))

    def early(i):
        return remote(early_buf.at[home], early_buf.at[home], f_send.at[0, i], f_recv.at[0, home], kin(i))

    def late(i):
        return remote(late_buf.at[home], late_buf.at[home], f_send.at[1, i], f_recv.at[1, home], kin(i))

    def send_early():
        for i in range(1, G):
            early(i).start()

    def voc_ready():
        loads[11].wait()
        for p in twin:
            other = lax.rem(p, NC)
            remote(voc_hbm, voc_ref.at[other], voc_send.at[0], voc_recv.at[other], dev()).wait_recv()

    spread(0, start, True)
    relay(0, start, True)
    for n in range(NZ):
        if n + 1 < NZ:
            spread(n + 1, start, True)
            relay(n + 1, start, True)
            if n == 0:
                voc_ready()
            z, tot, cho = compute(n)
            early_buf[home, pl.ds(z, 1), :] = tot
            early_buf[home, pl.ds(NZ + z, 1), :] = cho
        else:
            if n == 0:
                voc_ready()
            early_buf[home, pl.ds(step_of(n), 1), :] = code_line
            early_buf[home, pl.ds(NZ + step_of(n), 1), :] = jnp.zeros((1, lines), jnp.float32)
            z, tot, cho = compute(n, send_early)
            late_buf[home, 0:1, :] = tot
            late_buf[home, 1:2, :] = cho
    for i in range(1, G):
        late(i).start()
    for i in range(1, G):
        other = lax.rem(home + i, G)
        remote(early_buf.at[other], early_buf.at[other], f_send.at[0, 0], f_recv.at[0, other], dev()).wait_recv()
    for i in range(1, G):
        other = lax.rem(home + i, G)
        remote(late_buf.at[other], late_buf.at[other], f_send.at[1, 0], f_recv.at[1, other], dev()).wait_recv()

    def last_of(z):
        return NZ - 1 if z < NZ - 1 else 0

    empty = jnp.zeros((1, lines), jnp.float32)
    totals, chosen, codes = [empty] * NZ, [empty] * NZ, [empty] * NZ
    for i, (x, z, t) in enumerate(family):
        for w in range(NZ):
            if w == last_of(z):
                totals[w] = totals[w] + late_buf[i, 0:1, :]
                chosen[w] = chosen[w] + late_buf[i, 1:2, :]
                if t == 0:
                    codes[z] = codes[z] + early_buf[i, w:w + 1, :]
            else:
                totals[w] = totals[w] + early_buf[i, w:w + 1, :]
                chosen[w] = chosen[w] + early_buf[i, NZ + w:NZ + w + 1, :]
    totals, chosen, code = (jnp.concatenate(p, axis=0) for p in (totals, chosen, codes))
    inside = lax.rem(lax.broadcasted_iota(jnp.int32, (NZ, lines), 1), PAD) < rows
    counted = jnp.where(inside & (code >= docs), 1.0, 0.0)
    doc = jnp.where(code >= docs, code - docs, code)
    logprob = jnp.where(inside, counted * (chosen - jnp.log(totals)), 0.0)
    names = lax.broadcasted_iota(jnp.int32, (docs, lines), 0).astype(jnp.float32)
    like = jnp.zeros((docs, lines), jnp.float32)
    cnt = jnp.zeros((docs, lines), jnp.float32)
    for r in range(NZ):
        hit = names == doc[r:r + 1, :]
        like = like + jnp.where(hit, logprob[r:r + 1, :], 0.0)
        cnt = cnt + jnp.where(hit, counted[r:r + 1, :], 0.0)
    docs_eye = lax.broadcasted_iota(jnp.int32, (docs, 128), 0) == lax.broadcasted_iota(jnp.int32, (docs, 128), 1)
    sums = [
        jnp.sum(jnp.where(docs_eye, jnp.sum(v, axis=1, keepdims=True), 0.0), axis=0, keepdims=True)
        for v in (like, cnt)
    ]
    twin_buf[me_c, 0:1, :] = sums[0]
    twin_buf[me_c, 1:2, :] = sums[1]
    twin_copies = [
        remote(twin_buf.at[me_c], twin_buf.at[me_c], tw_send.at[0], tw_recv.at[me_c], dev(d=p)) for p in twin
    ]
    for c in twin_copies:
        c.start()
    mine = jnp.zeros((1, rows), jnp.float32)
    for z in range(NZ):
        for x in range(NX):
            mine = jnp.where((me_z == z) & (me_x == x), logprob[z:z + 1, x * PAD:x * PAD + rows], mine)
    out_ref[0:1, :rows] = mine
    for i, p in enumerate(others(me_t, NY)):
        for g in range(groups):
            att_copy(g, p, i).wait_send()
        stat_copy(p, i).wait_send()

    def drain(c):
        c.wait_send()

    for n in range(NZ):
        spread(n, drain, False)
        relay(n, drain, False)
    for block in [None, *range(NZ - 1)]:
        @pl.when((me_z + 1 < NZ) if block is None else (me_z > block) & (me_z + 1 < NZ))
        def _(block=block):
            for g in range(groups):
                for c in kv_copy(block, g):
                    c.wait_send()
    for i in range(1, G):
        early(i).wait_send()
        late(i).wait_send()
    for c in voc_copies:
        c.wait_send()
    for p in twin:
        other = lax.rem(p, NC)
        remote(twin_buf.at[other], twin_buf.at[other], tw_send.at[0], tw_recv.at[other], dev()).wait_recv()
    for c in twin_copies:
        c.wait_send()
    both = twin_buf[0]
    for c in range(1, NC):
        both = both + twin_buf[c]
    out_ref[1:3, :] = both


def split(packed, lp_ref, like_ref, cnt_ref):
    lp_ref[...] = packed[0:1, :lp_ref.shape[1]]
    like_ref[...] = packed[1:2, :like_ref.shape[1]]
    cnt_ref[...] = packed[2:3, :cnt_ref.shape[1]]


def local(
    mesh, query_vectors, key_vectors, value_vectors, out_weight, residual, post_gain, final_gain,
    vocab_weight, segment_ids, doc_starts, doc_index, targets,
):
    ND, NZ, NY = mesh.shape["dp"], mesh.shape["seq"], mesh.shape["tensor"]
    rows = query_vectors.shape[0]
    docs = doc_starts.shape[1] * ND
    blocks = ND * NZ
    fw = out_weight.shape[1]
    voc = vocab_weight
    if fw % 128 != 0:
        voc = voc.reshape(voc.shape[0], NY, fw).transpose(1, 0, 2)
    kvw, qw = key_vectors.shape[1], query_vectors.shape[1]
    heads = qw // HEAD_DIM
    groups = kvw // HEAD_DIM
    NC = 2 if ND % 2 == 0 else 1
    NX = ND // NC
    R = blocks * PAD // 128
    f32, bf16, i32 = jnp.float32, jnp.bfloat16, jnp.int32
    dma = pltpu.SemaphoreType.DMA
    lines = NX * PAD
    G = NX * NZ * NY
    anyspace = pl.BlockSpec(memory_space=pl.ANY)
    packed = pl.pallas_call(
        functools.partial(body, (ND, NZ, NY, docs)),
        out_shape=jax.ShapeDtypeStruct((8, 128), f32),
        in_specs=[anyspace] * 12,
        out_specs=pl.BlockSpec(memory_space=pltpu.VMEM),
        scratch_shapes=[
            pltpu.VMEM(query_vectors.shape, bf16),
            pltpu.VMEM(key_vectors.shape, bf16),
            pltpu.VMEM(value_vectors.shape, bf16),
            pltpu.VMEM(residual.shape, bf16),
            pltpu.VMEM(post_gain.shape, f32),
            pltpu.VMEM(final_gain.shape, f32),
            pltpu.VMEM(segment_ids.shape, i32),
            pltpu.SMEM(doc_starts.shape, i32),
            pltpu.SMEM(doc_index.shape, i32),
            pltpu.VMEM(targets.shape, i32),
            pltpu.VMEM(out_weight.shape, bf16),
            pltpu.VMEM((NC, *voc.shape), bf16),
            pltpu.VMEM((NZ, 2, rows, kvw), bf16),
            pltpu.VMEM((heads, rows, HEAD_DIM), f32),
            pltpu.VMEM((heads, rows, 128), f32),
            pltpu.VMEM((NY, rows, qw), bf16),
            pltpu.VMEM((rows, fw), f32),
            pltpu.VMEM((NY, rows, 128), f32),
            pltpu.VMEM((NZ, NY, NX, PAD, fw), bf16),
            pltpu.VMEM((NC, voc.shape[-2], lines), f32),
            pltpu.VMEM((NZ, 1, lines), i32),
            pltpu.VMEM((G, 2 * NZ, lines), f32),
            pltpu.VMEM((G, 2, lines), f32),
            pltpu.VMEM((NC, 2, 128), f32),
            dma((12,)),
            dma((NZ, groups, 2)), dma((NZ, groups, 2)),
            dma((NY, groups)), dma((NY, groups)),
            dma((NY,)), dma((NY,)),
            dma((NZ, NY, NX, 2)),
            dma((NZ, 2, 2)),
            dma((NX, NZ, 2, NY)),
            dma((NY, NZ, 2, NX)),
            dma((1,)), dma((NC,)),
            dma((2, G)), dma((2, G)),
            dma((1,)), dma((NC,)),
        ],
        compiler_params=pltpu.CompilerParams(
            collective_id=0, has_side_effects=True, vmem_limit_bytes=60 * 1024 * 1024
        ),
        name="packed_loglik",
    )(
        query_vectors, key_vectors, value_vectors, out_weight, residual, post_gain, final_gain, voc,
        segment_ids, doc_starts, doc_index, targets,
    )
    sums = jax.ShapeDtypeStruct((1, docs), f32)
    logprob, like, counts = pl.pallas_call(
        split, out_shape=(jax.ShapeDtypeStruct((1, rows), f32), sums, sums), name="split"
    )(packed)
    return (logprob, like[0], counts[0])


def solution(mesh):
    in_specs = (
        P(("dp", "seq"), "tensor"),
        P(("dp", "seq"), "tensor"),
        P(("dp", "seq"), "tensor"),
        P(None, "tensor"),
        P(("dp", "seq"), "tensor"),
        P("tensor"),
        P("tensor"),
        P(("dp", "seq", "tensor"), None),
        P("dp", "seq"),
        P("dp", None),
        P("dp", None),
        P(),
    )
    out_specs = (P("dp", "seq"), P(), P())
    return jax.shard_map(
        functools.partial(local, mesh), mesh=mesh, in_specs=in_specs, out_specs=out_specs, check_vma=False
    )
```

```python
import functools

import jax
import jax.numpy as jnp
from jax import lax
from jax.experimental import pallas as pl
from jax.experimental.pallas import tpu as pltpu
from jax.sharding import PartitionSpec as P

HEAD_DIM = 256
ATTENTION_CAP = 50.0
LOGIT_CAP = 30.0
EPSILON = 1e-06
MESH = pl.DeviceIdType.MESH
PAD = 64
NT = (((1,), (1,)), ((), ()))
NN = (((1,), (0,)), ((), ()))


def dot(a, b, dims):
    return lax.dot_general(a, b, dims, preferred_element_type=jnp.float32)


def body(
    sizes,
    q_hbm, k_hbm, v_hbm, w_hbm, res_hbm, pg_hbm, fg_hbm, voc_hbm, seg_hbm, start_hbm, index_hbm, target_hbm,
    out_ref,
    q_ref, k_ref, v_ref, res_ref, pg_ref, fg_ref, seg_ref, start_ref, index_ref, target_ref,
    w_ref, voc_ref, kv, num, den, att, branch, stat, hid, held, lab_ref, early_buf, late_buf, twin_buf,
    local_sem, kv_send, kv_recv, att_send, att_recv, st_send, st_recv,
    hid_recv, z_send, d_send, u_send, token, y_send, x_send, voc_send, voc_recv, f_send, f_recv, tw_send, tw_recv,
):
    ND, NZ, NY, docs = sizes
    NC = 2 if ND % 2 == 0 else 1
    NX = ND // NC
    D = voc_hbm.shape[-1] if voc_hbm.ndim == 2 else voc_hbm.shape[0] * voc_hbm.shape[2]
    me_d, me_z, me_t = lax.axis_index("dp"), lax.axis_index("seq"), lax.axis_index("tensor")
    me_x, me_c = me_d // NC, me_d % NC
    twin = [me_x * NC + 1 - me_c] if NC == 2 else []
    rows = q_ref.shape[0]
    kvw = k_ref.shape[1]
    groups = kvw // HEAD_DIM
    per = q_ref.shape[1] // kvw
    heads = groups * per
    qw = q_ref.shape[1]
    fw = w_hbm.shape[1]

    pairs = [
        (k_hbm, k_ref), (v_hbm, v_ref), (q_hbm, q_ref), (seg_hbm, seg_ref), (start_hbm, start_ref),
        (index_hbm, index_ref), (target_hbm, target_ref), (res_hbm, res_ref), (pg_hbm, pg_ref), (fg_hbm, fg_ref),
        (w_hbm, w_ref), (voc_hbm, voc_ref.at[me_c]),
    ]
    loads = [pltpu.make_async_copy(src, dst, local_sem.at[i]) for i, (src, dst) in enumerate(pairs)]
    for c in loads:
        c.start()
    w_copy = loads[10]

    def dev(d=None, z=None, t=None):
        return (me_d if d is None else d, me_z if z is None else z, me_t if t is None else t)

    def remote(src, dst, send, recv, device):
        return pltpu.make_async_remote_copy(
            src_ref=src, dst_ref=dst, send_sem=send, recv_sem=recv, device_id=device, device_id_type=MESH
        )

    def others(me, n):
        return [jnp.where(me + i >= n, me + i - n, me + i) for i in range(1, n)]

    barrier = pltpu.get_barrier_semaphore()
    peers = [dev(d=p * NC + me_c) for p in others(me_x, NX)] + [dev(d=p) for p in twin]
    peers += [dev(t=p) for p in others(me_t, NY)]
    ups = [(me_z + 1 < NZ, dev(z=lax.rem(me_z + 1, NZ))), (me_z >= 1, dev(z=lax.rem(me_z + NZ - 1, NZ)))]
    for p in peers:
        pl.semaphore_signal(barrier, inc=1, device_id=p, device_id_type=MESH)
    for there, p in ups:
        @pl.when(there)
        def _(p=p):
            pl.semaphore_signal(barrier, inc=1, device_id=p, device_id_type=MESH)
    for c in loads[:2]:
        c.wait()

    def kv_copy(block, g):
        cols = pl.ds(g * HEAD_DIM, HEAD_DIM)
        up = dev(z=lax.rem(me_z + 1, NZ))
        if block is None:
            pairs = [(k_ref.at[:, cols], kv.at[me_z, 0, :, cols]), (v_ref.at[:, cols], kv.at[me_z, 1, :, cols])]
            where = me_z
        else:
            pairs = [(kv.at[block, i, :, cols],) * 2 for i in range(2)]
            where = block
        return [
            remote(src, dst, kv_send.at[where, g, i], kv_recv.at[where, g, i], up)
            for i, (src, dst) in enumerate(pairs)
        ]

    ends = lax.div(me_z + NZ - 1, NZ) + lax.div(2 * NZ - 2 - me_z, NZ)
    pl.semaphore_wait(barrier, len(peers) + ends)
    @pl.when(me_z + 1 < NZ)
    def _():
        for g in range(groups):
            for c in kv_copy(None, g):
                c.start()
    voc_copies = [
        remote(voc_hbm, voc_ref.at[me_c], voc_send.at[0], voc_recv.at[me_c], dev(d=p)) for p in twin
    ]
    for c in voc_copies:
        c.start()
    for c in loads[2:7]:
        c.wait()
    seg = seg_ref[...]
    first_row = jnp.zeros((1, rows), jnp.int32)
    end_row = jnp.zeros((1, rows), jnp.int32)
    doc_row = jnp.zeros((1, rows), jnp.int32)
    segs = start_ref.shape[1]
    for n in range(segs):
        here = seg == n
        first_row = jnp.where(here, start_ref[0, n], first_row)
        end_row = jnp.where(here, start_ref[0, n + 1] if n + 1 < segs else rows * NZ, end_row)
        doc_row = jnp.where(here, index_ref[0, n], doc_row)
    spot = me_z * rows + lax.broadcasted_iota(jnp.int32, (1, rows), 1)
    code_row = doc_row + jnp.where(spot + 1 < end_row, docs, 0)
    i_pos = lax.broadcasted_iota(jnp.int32, (rows, rows), 0)
    j_pos = lax.broadcasted_iota(jnp.int32, (rows, rows), 1)

    def column_of(row):
        full = jnp.broadcast_to(row.astype(jnp.float32), (rows, rows))
        return jnp.sum(jnp.where(i_pos == j_pos, full, 0.0), axis=1, keepdims=True)

    first = column_of(first_row).astype(jnp.int32)
    lines = NX * PAD
    lanes = lax.broadcasted_iota(jnp.int32, (rows, lines), 1)
    sub = lax.broadcasted_iota(jnp.int32, (rows, lines), 0)
    placed = jnp.where(lanes == sub + me_x * PAD, column_of(code_row), 0.0)
    code_line = jnp.sum(placed, axis=0, keepdims=True)
    gap = jnp.zeros((1, PAD - rows), jnp.int32)
    for z in range(NZ):
        pieces = []
        for x in range(NX):
            part = target_ref[x * NC:x * NC + 1, z * rows:(z + 1) * rows]
            for c in range(1, NC):
                part = jnp.where(me_c == c, target_ref[x * NC + c:x * NC + c + 1, z * rows:(z + 1) * rows], part)
            pieces += [part, gap]
        lab_ref[z] = jnp.concatenate(pieces, axis=1)

    def attend(block, g):
        cols = slice(g * HEAD_DIM, (g + 1) * HEAD_DIM)
        if block is None:
            kk, vv = k_ref[:, cols], v_ref[:, cols]
            seen = (me_z * rows + j_pos >= first) & (j_pos <= i_pos)
        else:
            kk, vv = kv[block, 0, :, cols], kv[block, 1, :, cols]
            seen = block * rows + j_pos >= first
        for h in range(g * per, (g + 1) * per):
            raw = dot(q_ref[:, h * HEAD_DIM:(h + 1) * HEAD_DIM], kk, NT)
            capped = ATTENTION_CAP * jnp.tanh(raw * (HEAD_DIM ** (-0.5) / ATTENTION_CAP))
            wt = jnp.where(seen, jnp.exp(capped), 0.0)
            top = dot(wt.astype(jnp.bfloat16), vv, NN)
            low = jnp.broadcast_to(jnp.sum(wt, axis=1, keepdims=True), (rows, 128))
            if block is None:
                num[h] = top
                den[h] = low
            else:
                num[h] = num[h] + top
                den[h] = den[h] + low

    def arrived(block, g):
        for c in kv_copy(block, g):
            c.wait_recv()

        @pl.when(me_z + 1 < NZ)
        def _():
            for c in kv_copy(block, g):
                c.start()

    @pl.when(me_z >= 0)
    def _():
        for g in range(groups):
            attend(None, g)

    top, bottom = me_z == NZ - 1, me_z == 0
    under = jnp.logical_not(top) if NZ > 2 else me_z >= 0

    def tell(i, z):
        pl.semaphore_signal(token.at[i], inc=1, device_id=dev(z=lax.rem(z + NZ, NZ)), device_id_type=MESH)

    if NZ > 1:
        @pl.when(bottom)
        def _():
            tell(0, me_z + 1)

        @pl.when(top)
        def _():
            tell(1, me_z - 1)

        @pl.when(jnp.logical_not(bottom | top))
        def _():
            pl.semaphore_wait(token.at[1], 1)
            tell(1, me_z - 1)
            pl.semaphore_wait(token.at[0], 1)
            tell(0, me_z + 1)

    for block in range(NZ - 2, 0, -1):
        @pl.when(block < me_z)
        def _(block=block):
            for g in range(groups):
                arrived(block, g)
                attend(block, g)

    gw = per * HEAD_DIM

    def att_copy(g, peer, idx):
        ref = att.at[me_t, :, pl.ds(g * gw, gw)]
        return remote(ref, ref, att_send.at[idx, g], att_recv.at[me_t, g], dev(t=peer))

    step = 256 if fw % 256 == 0 else fw

    def project(t, g, begin):
        base = pl.multiple_of(t * qw + g * gw, gw)
        left = att[t, :, g * gw:(g + 1) * gw]
        for n in range(fw // step):
            cols = slice(n * step, (n + 1) * step)
            got = dot(left, w_ref[pl.ds(base, gw), cols], NN)
            branch[:, cols] = got if begin else branch[:, cols] + got

    for g in range(groups):
        if NZ > 1:
            @pl.when(me_z > 0)
            def _(g=g):
                arrived(0, g)
                attend(0, g)
        for h in range(g * per, (g + 1) * per):
            att[me_t, :, h * HEAD_DIM:(h + 1) * HEAD_DIM] = (num[h] / den[h][:, :1]).astype(jnp.bfloat16)
        for i, p in enumerate(others(me_t, NY)):
            att_copy(g, p, i).start()
        if g == 0:
            w_copy.wait()
        project(me_t, g, g == 0)
    for g in range(groups):
        for p in others(me_t, NY):
            ref = att.at[p, :, pl.ds(g * gw, gw)]
            remote(ref, ref, att_send.at[0, 0], att_recv.at[p, g], dev()).wait_recv()
            project(p, g, False)

    for c in loads[7:10]:
        c.wait()
    br = branch[...]
    carried = res_ref[...].astype(jnp.float32)
    gained = pg_ref[...].reshape(1, fw) * br
    lane = lax.broadcasted_iota(jnp.int32, (rows, 128), 1)
    packed = jnp.zeros((rows, 128), jnp.float32)
    for i, prod in enumerate((br * br, carried * carried, carried * gained, gained * gained)):
        packed = jnp.where(lane == i, jnp.sum(prod, axis=1, keepdims=True), packed)
    stat[me_t] = packed

    def stat_copy(peer, i):
        return remote(stat.at[me_t], stat.at[me_t], st_send.at[i], st_recv.at[me_t], dev(t=peer))

    for i, p in enumerate(others(me_t, NY)):
        stat_copy(p, i).start()
    for p in others(me_t, NY):
        remote(stat.at[p], stat.at[p], st_send.at[0], st_recv.at[p], dev()).wait_recv()
    total = stat[0]
    for t in range(1, NY):
        total = total + stat[t]
    sq_branch, sq_carried, cross, sq_gained = (total[:, i:i + 1] for i in range(4))
    inv_branch = 1.0 / jnp.sqrt(sq_branch / D + EPSILON)
    sq_total = sq_carried + 2.0 * inv_branch * cross + inv_branch * inv_branch * sq_gained
    inv_total = 1.0 / jnp.sqrt(sq_total / D + EPSILON)
    hid[me_z, me_t, me_x, :rows, :] = (
        fg_ref[...].reshape(1, fw) * (carried + gained * inv_branch) * inv_total
    ).astype(jnp.bfloat16)

    y_peers = others(me_t, NY)
    x_peers = others(me_x, NX)
    cut = min(rows, (rows // 2 + 7) // 8 * 8)
    spans = [(0, cut)] + ([(cut, rows - cut)] if cut < rows else [])
    K = len(spans)

    def xdev(x):
        return dev(d=x * NC + me_c)

    def block(z, t, x, k):
        return hid.at[z, t, x, pl.ds(*spans[k]), :]

    def send(z, t, x, k, sem, device):
        return remote(block(z, t, x, k), block(z, t, x, k), sem, hid_recv.at[z, t, x, k], device)

    def landed(z, t, x, k):
        send(z, t, x, k, z_send.at[0, 0], dev()).wait_recv()

    def step_of(n):
        return me_z if n == 0 else jnp.where(n <= me_z, me_z - n, n)

    def spread(n, act, wait):
        z = step_of(n)
        for k in range(K):
            if wait and n > 0:
                landed(z, me_t, me_x, k)
            for i, p in enumerate(x_peers):
                act(send(z, me_t, me_x, k, x_send.at[0, z, k, i], xdev(p)))
            for i, p in enumerate(y_peers):
                act(send(z, me_t, me_x, k, y_send.at[0, z, k, i], dev(t=p)))

            @pl.when(jnp.logical_not(top) & (z <= me_z))
            def _(k=k):
                act(send(z, me_t, me_x, k, z_send.at[z, k], dev(z=lax.rem(me_z + 1, NZ))))
        if n == 0:
            for off in range(1, NZ):
                @pl.when(off <= me_z)
                def _(off=off):
                    for k in range(K):
                        p = lax.rem(me_z + NZ - off, NZ)
                        act(send(me_z, me_t, me_x, k, d_send.at[off - 1, k], dev(z=p)))

    def lift(act):
        for j, x in enumerate(x_peers):
            for i, t in enumerate(y_peers):
                for k in range(K):
                    act(send(me_z, t, x, k, u_send.at[j, i, k], dev(z=NZ - 1)))

    def relay(n, act, wait):
        z = step_of(n)
        for j, x in enumerate(x_peers):
            if wait:
                landed(z, me_t, x, 0)
            for i, p in enumerate(y_peers):
                act(send(z, me_t, x, 0, y_send.at[1 + j, z, 0, i], dev(t=p)))
        for j, t in enumerate(y_peers):
            if wait:
                landed(z, t, me_x, K - 1)
            if K > 1:
                for i, p in enumerate(x_peers):
                    act(send(z, t, me_x, K - 1, x_send.at[1 + j, z, K - 1, i], xdev(p)))

    def start(c):
        c.start()

    count = voc_hbm.shape[-2]
    home = (me_x * NZ + me_z) * NY + me_t
    row_ids = lax.broadcasted_iota(jnp.int32, (count, lines), 0)

    def product(c, z, t):
        right = hid[z, t].reshape(lines, fw)
        if len(voc_ref.shape) == 3:
            start_col = t * fw if isinstance(t, int) else pl.multiple_of(t * fw, 128)
            left = voc_ref[c, :, pl.ds(start_col, fw)]
        else:
            left = voc_ref[c, t]
        return dot(left, right, NT)

    def gather(n, z, t, begin):
        @pl.loop(0, NC)
        def _(c):
            got = product(c, z, t)
            held[n, c] = got if begin else held[n, c] + got

    def finish(n, z, t, begin):
        label = lab_ref[z]

        def part(c, sums):
            acc = product(c, z, t)
            if not begin:
                acc = held[n, c] + acc
            capped = LOGIT_CAP * jnp.tanh(acc * (1.0 / LOGIT_CAP))
            base = (((me_x * NC + c) * NZ + me_z) * NY + me_t) * count
            tot = sums[0] + jnp.sum(jnp.exp(capped), axis=0, keepdims=True)
            cho = sums[1] + jnp.sum(jnp.where(row_ids == label - base, capped, 0.0), axis=0, keepdims=True)
            return tot, cho

        zero = jnp.zeros((1, lines), jnp.float32)
        return lax.fori_loop(0, NC, part, (zero, zero))

    def begin_slice(n):
        z = step_of(n)
        for x in x_peers:
            for k in range(1, K):
                landed(z, me_t, x, k)
        if n > 0 and NZ > 2:
            @pl.when(top)
            def _():
                for x in x_peers:
                    landed(z, me_t, x, 0)
        if n == 0:
            voc_ready()
        if NY > 1:
            gather(n, z, me_t, True)

    def end_slice(n, before_last=None):
        z = step_of(n)
        if n > 0 and NZ > 2:
            @pl.when(top)
            def _():
                for t in y_peers:
                    landed(z, t, me_x, K - 1)
        last = me_t
        for i, t in enumerate(y_peers):
            for k in range(K - 1):
                landed(z, t, me_x, k)
            for x in x_peers:
                for k in range(K):
                    landed(z, t, x, k)
            last = t
            if i + 1 < len(y_peers):
                gather(n, z, t, False)
        if before_last is not None:
            before_last()
        return z, *finish(n, z, last, NY == 1)

    family = [(x, z, t) for x in range(NX) for z in range(NZ) for t in range(NY)]
    G = len(family)

    def wrap(v, n):
        return jnp.where(v >= n, v - n, v)

    def kin_of(i):
        return wrap(me_x + i // (NZ * NY), NX), wrap(me_z + i // NY % NZ, NZ), wrap(me_t + i % NY, NY)

    def kin(i):
        x, z, t = kin_of(i)
        return dev(d=x * NC + me_c, z=z, t=t)

    def seat(i):
        x, z, t = kin_of(i)
        return (x * NZ + z) * NY + t

    def early(i):
        return remote(early_buf.at[home], early_buf.at[home], f_send.at[0, i], f_recv.at[0, home], kin(i))

    def late(i):
        return remote(late_buf.at[home], late_buf.at[home], f_send.at[1, i], f_recv.at[1, home], kin(i))

    def send_early():
        for i in range(1, G):
            early(i).start()

    def voc_ready():
        loads[11].wait()
        for p in twin:
            other = lax.rem(p, NC)
            remote(voc_hbm, voc_ref.at[other], voc_send.at[0], voc_recv.at[other], dev()).wait_recv()

    def score(n):
        if n + 1 < NZ:
            z, tot, cho = end_slice(n)
            early_buf[home, pl.ds(z, 1), :] = tot
            early_buf[home, pl.ds(NZ + z, 1), :] = cho
        else:
            early_buf[home, pl.ds(step_of(n), 1), :] = code_line
            early_buf[home, pl.ds(NZ + step_of(n), 1), :] = jnp.zeros((1, lines), jnp.float32)
            z, tot, cho = end_slice(n, send_early)
            late_buf[home, 0:1, :] = tot
            late_buf[home, 1:2, :] = cho

    if NZ > 1:
        @pl.when(top)
        def _():
            pl.semaphore_wait(token.at[0], 1)

    spread(0, start, True)

    @pl.when(bottom)
    def _():
        relay(0, start, True)

    if NZ > 1:
        @pl.when(bottom)
        def _():
            pl.semaphore_wait(token.at[1], 1)

        spread(1, start, True)

        @pl.when(jnp.logical_not(bottom))
        def _():
            relay(0, start, True)

    for n in range(2, NZ):
        @pl.when(n <= me_z)
        def _(n=n):
            spread(n, start, True)

    if NZ > 1:
        @pl.when(under)
        def _():
            relay(1, start, True)

    if NZ > 3:
        @pl.when(me_z == NZ - 2)
        def _():
            spread(NZ - 1, start, True)

    for n in range(2, NZ):
        @pl.when((n > me_z) & ((n < NZ - 1) | (me_z != NZ - 2) | (NZ == 3)))
        def _(n=n):
            spread(n, start, True)

        if n == 2:
            begin_slice(0)
        else:
            begin_slice(n - 1)
        score(n - 2)
        if n == 2 and NZ > 3:
            begin_slice(1)

        @pl.when(under)
        def _(n=n):
            relay(n, start, True)
            if n == 2:
                lift(start)

    if NZ < 3:
        begin_slice(0)
    if NZ == 3:
        begin_slice(1)
    if NZ > 1:
        begin_slice(NZ - 1)
        score(NZ - 2)
    score(NZ - 1)
    for i in range(1, G):
        late(i).start()
    for i in range(1, G):
        other = seat(i)
        remote(early_buf.at[other], early_buf.at[other], f_send.at[0, 0], f_recv.at[0, other], dev()).wait_recv()
    def last_of(z):
        return NZ - 1 if z < NZ - 1 else 0

    empty = jnp.zeros((1, lines), jnp.float32)
    totals, chosen, codes = [empty] * NZ, [empty] * NZ, [empty] * NZ
    for i, (x, z, t) in enumerate(family):
        for w in range(NZ):
            if w != last_of(z):
                totals[w] = totals[w] + early_buf[i, w:w + 1, :]
                chosen[w] = chosen[w] + early_buf[i, NZ + w:NZ + w + 1, :]
            elif t == 0:
                codes[z] = codes[z] + early_buf[i, w:w + 1, :]
    for i in range(1, G):
        other = seat(i)
        remote(late_buf.at[other], late_buf.at[other], f_send.at[1, 0], f_recv.at[1, other], dev()).wait_recv()
    for i, (x, z, t) in enumerate(family):
        w = last_of(z)
        totals[w] = totals[w] + late_buf[i, 0:1, :]
        chosen[w] = chosen[w] + late_buf[i, 1:2, :]
    totals, chosen, code = (jnp.concatenate(p, axis=0) for p in (totals, chosen, codes))
    inside = lax.rem(lax.broadcasted_iota(jnp.int32, (NZ, lines), 1), PAD) < rows
    counted = jnp.where(inside & (code >= docs), 1.0, 0.0)
    doc = jnp.where(code >= docs, code - docs, code)
    logprob = jnp.where(inside, counted * (chosen - jnp.log(totals)), 0.0)
    names = lax.broadcasted_iota(jnp.int32, (docs, lines), 0).astype(jnp.float32)
    like = jnp.zeros((docs, lines), jnp.float32)
    cnt = jnp.zeros((docs, lines), jnp.float32)
    for r in range(NZ):
        hit = names == doc[r:r + 1, :]
        like = like + jnp.where(hit, logprob[r:r + 1, :], 0.0)
        cnt = cnt + jnp.where(hit, counted[r:r + 1, :], 0.0)
    docs_eye = lax.broadcasted_iota(jnp.int32, (docs, 128), 0) == lax.broadcasted_iota(jnp.int32, (docs, 128), 1)
    sums = [
        jnp.sum(jnp.where(docs_eye, jnp.sum(v, axis=1, keepdims=True), 0.0), axis=0, keepdims=True)
        for v in (like, cnt)
    ]
    twin_buf[me_c, 0:1, :] = sums[0]
    twin_buf[me_c, 1:2, :] = sums[1]
    twin_copies = [
        remote(twin_buf.at[me_c], twin_buf.at[me_c], tw_send.at[0], tw_recv.at[me_c], dev(d=p)) for p in twin
    ]
    for c in twin_copies:
        c.start()
    mine = jnp.zeros((1, rows), jnp.float32)
    for z in range(NZ):
        for x in range(NX):
            mine = jnp.where((me_z == z) & (me_x == x), logprob[z:z + 1, x * PAD:x * PAD + rows], mine)
    out_ref[0:1, :rows] = mine
    for i, p in enumerate(others(me_t, NY)):
        for g in range(groups):
            att_copy(g, p, i).wait_send()
        stat_copy(p, i).wait_send()

    def drain(c):
        c.wait_send()

    relay(0, drain, False)
    for n in range(NZ):
        spread(n, drain, False)

    @pl.when(under)
    def _():
        if NZ > 2:
            lift(drain)
        for n in range(1, NZ):
            relay(n, drain, False)
    for block in [None, *range(NZ - 1)]:
        @pl.when((me_z + 1 < NZ) if block is None else (me_z > block) & (me_z + 1 < NZ))
        def _(block=block):
            for g in range(groups):
                for c in kv_copy(block, g):
                    c.wait_send()
    for i in range(1, G):
        early(i).wait_send()
        late(i).wait_send()
    for c in voc_copies:
        c.wait_send()
    for p in twin:
        other = lax.rem(p, NC)
        remote(twin_buf.at[other], twin_buf.at[other], tw_send.at[0], tw_recv.at[other], dev()).wait_recv()
    for c in twin_copies:
        c.wait_send()
    both = twin_buf[0]
    for c in range(1, NC):
        both = both + twin_buf[c]
    out_ref[1:3, :] = both


def split(packed, lp_ref, like_ref, cnt_ref):
    lp_ref[...] = packed[0:1, :lp_ref.shape[1]]
    like_ref[...] = packed[1:2, :like_ref.shape[1]]
    cnt_ref[...] = packed[2:3, :cnt_ref.shape[1]]


def local(
    mesh, query_vectors, key_vectors, value_vectors, out_weight, residual, post_gain, final_gain,
    vocab_weight, segment_ids, doc_starts, doc_index, targets,
):
    ND, NZ, NY = mesh.shape["dp"], mesh.shape["seq"], mesh.shape["tensor"]
    rows = query_vectors.shape[0]
    docs = doc_starts.shape[1] * ND
    blocks = ND * NZ
    fw = out_weight.shape[1]
    voc = vocab_weight
    if fw % 128 != 0:
        voc = voc.reshape(voc.shape[0], NY, fw).transpose(1, 0, 2)
    kvw, qw = key_vectors.shape[1], query_vectors.shape[1]
    heads = qw // HEAD_DIM
    groups = kvw // HEAD_DIM
    NC = 2 if ND % 2 == 0 else 1
    NX = ND // NC
    R = blocks * PAD // 128
    f32, bf16, i32 = jnp.float32, jnp.bfloat16, jnp.int32
    dma = pltpu.SemaphoreType.DMA
    lines = NX * PAD
    G = NX * NZ * NY
    anyspace = pl.BlockSpec(memory_space=pl.ANY)
    packed = pl.pallas_call(
        functools.partial(body, (ND, NZ, NY, docs)),
        out_shape=jax.ShapeDtypeStruct((8, 128), f32),
        in_specs=[anyspace] * 12,
        out_specs=pl.BlockSpec(memory_space=pltpu.VMEM),
        scratch_shapes=[
            pltpu.VMEM(query_vectors.shape, bf16),
            pltpu.VMEM(key_vectors.shape, bf16),
            pltpu.VMEM(value_vectors.shape, bf16),
            pltpu.VMEM(residual.shape, bf16),
            pltpu.VMEM(post_gain.shape, f32),
            pltpu.VMEM(final_gain.shape, f32),
            pltpu.VMEM(segment_ids.shape, i32),
            pltpu.SMEM(doc_starts.shape, i32),
            pltpu.SMEM(doc_index.shape, i32),
            pltpu.VMEM(targets.shape, i32),
            pltpu.VMEM(out_weight.shape, bf16),
            pltpu.VMEM((NC, *voc.shape), bf16),
            pltpu.VMEM((NZ, 2, rows, kvw), bf16),
            pltpu.VMEM((heads, rows, HEAD_DIM), f32),
            pltpu.VMEM((heads, rows, 128), f32),
            pltpu.VMEM((NY, rows, qw), bf16),
            pltpu.VMEM((rows, fw), f32),
            pltpu.VMEM((NY, rows, 128), f32),
            pltpu.VMEM((NZ, NY, NX, PAD, fw), bf16),
            pltpu.VMEM((NZ, NC, voc.shape[-2], lines), f32),
            pltpu.VMEM((NZ, 1, lines), i32),
            pltpu.VMEM((G, 2 * NZ, lines), f32),
            pltpu.VMEM((G, 2, lines), f32),
            pltpu.VMEM((NC, 2, 128), f32),
            dma((12,)),
            dma((NZ, groups, 2)), dma((NZ, groups, 2)),
            dma((NY, groups)), dma((NY, groups)),
            dma((NY,)), dma((NY,)),
            dma((NZ, NY, NX, 2)),
            dma((NZ, 2)),
            dma((NZ, 2)),
            dma((NX, NY, 2)),
            pltpu.SemaphoreType.REGULAR((2,)),
            dma((NX, NZ, 2, NY)),
            dma((NY, NZ, 2, NX)),
            dma((1,)), dma((NC,)),
            dma((2, G)), dma((2, G)),
            dma((1,)), dma((NC,)),
        ],
        compiler_params=pltpu.CompilerParams(
            collective_id=0, has_side_effects=True, vmem_limit_bytes=60 * 1024 * 1024
        ),
        name="packed_loglik",
    )(
        query_vectors, key_vectors, value_vectors, out_weight, residual, post_gain, final_gain, voc,
        segment_ids, doc_starts, doc_index, targets,
    )
    sums = jax.ShapeDtypeStruct((1, docs), f32)
    logprob, like, counts = pl.pallas_call(
        split, out_shape=(jax.ShapeDtypeStruct((1, rows), f32), sums, sums), name="split"
    )(packed)
    return (logprob, like[0], counts[0])


def solution(mesh):
    in_specs = (
        P(("dp", "seq"), "tensor"),
        P(("dp", "seq"), "tensor"),
        P(("dp", "seq"), "tensor"),
        P(None, "tensor"),
        P(("dp", "seq"), "tensor"),
        P("tensor"),
        P("tensor"),
        P(("dp", "seq", "tensor"), None),
        P("dp", "seq"),
        P("dp", None),
        P("dp", None),
        P(),
    )
    out_specs = (P("dp", "seq"), P(), P())
    return jax.shard_map(
        functools.partial(local, mesh), mesh=mesh, in_specs=in_specs, out_specs=out_specs, check_vma=False
    )
```

```python
import functools

import jax
import jax.numpy as jnp
from jax import lax
from jax.experimental import pallas as pl
from jax.experimental.pallas import tpu as pltpu
from jax.sharding import PartitionSpec as P

HEAD_DIM = 256
ATTENTION_CAP = 50.0
LOGIT_CAP = 30.0
EPSILON = 1e-06
MESH = pl.DeviceIdType.MESH
PAD = 64
NT = (((1,), (1,)), ((), ()))
NN = (((1,), (0,)), ((), ()))


def dot(a, b, dims):
    return lax.dot_general(a, b, dims, preferred_element_type=jnp.float32)


def body(
    sizes,
    q_hbm, k_hbm, v_hbm, w_hbm, res_hbm, pg_hbm, fg_hbm, voc_hbm, seg_hbm, start_hbm, index_hbm, target_hbm,
    out_ref,
    q_ref, res_ref, pg_ref, fg_ref, seg_ref, start_ref, index_ref, target_ref,
    w_ref, voc_ref, kv, num, den, att, branch, stat, hid, held, lab_ref, early_buf, late_buf, twin_buf,
    local_sem, kv_send, kv_recv, att_send, att_recv, st_send, st_recv,
    hid_recv, z_send, d_send, u_send, token, y_send, x_send, voc_send, voc_recv, f_send, f_recv, tw_send, tw_recv,
):
    ND, NZ, NY, docs = sizes
    NC = 2 if ND % 2 == 0 else 1
    NX = ND // NC
    D = voc_hbm.shape[-1] if voc_hbm.ndim == 2 else voc_hbm.shape[0] * voc_hbm.shape[2]
    me_d, me_z, me_t = lax.axis_index("dp"), lax.axis_index("seq"), lax.axis_index("tensor")
    me_x, me_c = me_d // NC, me_d % NC
    twin = [me_x * NC + 1 - me_c] if NC == 2 else []
    rows = q_ref.shape[0]
    kvw = k_hbm.shape[1]
    groups = kvw // HEAD_DIM
    per = q_ref.shape[1] // kvw
    heads = groups * per
    qw = q_ref.shape[1]
    fw = w_hbm.shape[1]

    pairs = [
        (k_hbm, kv.at[me_z, 0]), (v_hbm, kv.at[me_z, 1]), (q_hbm, q_ref), (seg_hbm, seg_ref), (start_hbm, start_ref),
        (index_hbm, index_ref), (target_hbm, target_ref), (res_hbm, res_ref), (pg_hbm, pg_ref), (fg_hbm, fg_ref),
        (w_hbm, w_ref), (voc_hbm, voc_ref.at[me_c]),
    ]
    loads = [pltpu.make_async_copy(src, dst, local_sem.at[i]) for i, (src, dst) in enumerate(pairs)]
    for c in loads:
        c.start()
    w_copy = loads[10]

    def dev(d=None, z=None, t=None):
        return (me_d if d is None else d, me_z if z is None else z, me_t if t is None else t)

    def remote(src, dst, send, recv, device):
        return pltpu.make_async_remote_copy(
            src_ref=src, dst_ref=dst, send_sem=send, recv_sem=recv, device_id=device, device_id_type=MESH
        )

    def others(me, n):
        return [jnp.where(me + i >= n, me + i - n, me + i) for i in range(1, n)]

    barrier = pltpu.get_barrier_semaphore()
    peers = [dev(d=p * NC + me_c) for p in others(me_x, NX)] + [dev(d=p) for p in twin]
    peers += [dev(t=p) for p in others(me_t, NY)]
    ups = [(me_z + 1 < NZ, dev(z=lax.rem(me_z + 1, NZ))), (me_z >= 1, dev(z=lax.rem(me_z + NZ - 1, NZ)))]
    for p in peers:
        pl.semaphore_signal(barrier, inc=1, device_id=p, device_id_type=MESH)
    for there, p in ups:
        @pl.when(there)
        def _(p=p):
            pl.semaphore_signal(barrier, inc=1, device_id=p, device_id_type=MESH)
    for c in loads[:2]:
        c.wait()

    def kv_copy(block, g):
        ref = kv.at[block, :, :, pl.ds(g * HEAD_DIM, HEAD_DIM)]
        return remote(ref, ref, kv_send.at[block], kv_recv.at[block, g], dev(z=lax.rem(me_z + 1, NZ)))

    def kv_sent(block):
        remote(kv.at[block], kv.at[block], kv_send.at[block], kv_recv.at[block, 0], dev()).wait_send()

    ends = lax.div(me_z + NZ - 1, NZ) + lax.div(2 * NZ - 2 - me_z, NZ)
    pl.semaphore_wait(barrier, len(peers) + ends)
    @pl.when(me_z + 1 < NZ)
    def _():
        for g in range(groups):
            kv_copy(me_z, g).start()
    voc_copies = [
        remote(voc_hbm, voc_ref.at[me_c], voc_send.at[0], voc_recv.at[me_c], dev(d=p)) for p in twin
    ]
    for c in voc_copies:
        c.start()
    for c in loads[2:7]:
        c.wait()
    seg = seg_ref[...]
    first_row = jnp.zeros((1, rows), jnp.int32)
    end_row = jnp.zeros((1, rows), jnp.int32)
    doc_row = jnp.zeros((1, rows), jnp.int32)
    segs = start_ref.shape[1]
    for n in range(segs):
        here = seg == n
        first_row = jnp.where(here, start_ref[0, n], first_row)
        end_row = jnp.where(here, start_ref[0, n + 1] if n + 1 < segs else rows * NZ, end_row)
        doc_row = jnp.where(here, index_ref[0, n], doc_row)
    spot = me_z * rows + lax.broadcasted_iota(jnp.int32, (1, rows), 1)
    code_row = doc_row + jnp.where(spot + 1 < end_row, docs, 0)
    i_pos = lax.broadcasted_iota(jnp.int32, (rows, rows), 0)
    j_pos = lax.broadcasted_iota(jnp.int32, (rows, rows), 1)

    def column_of(row):
        full = jnp.broadcast_to(row.astype(jnp.float32), (rows, rows))
        return jnp.sum(jnp.where(i_pos == j_pos, full, 0.0), axis=1, keepdims=True)

    first = column_of(first_row).astype(jnp.int32)
    lines = NX * PAD
    lanes = lax.broadcasted_iota(jnp.int32, (rows, lines), 1)
    sub = lax.broadcasted_iota(jnp.int32, (rows, lines), 0)
    placed = jnp.where(lanes == sub + me_x * PAD, column_of(code_row), 0.0)
    code_line = jnp.sum(placed, axis=0, keepdims=True) * jnp.where(me_t == 0, 1.0, 0.0)
    gap = jnp.zeros((1, PAD - rows), jnp.int32)
    for z in range(NZ):
        pieces = []
        for x in range(NX):
            part = target_ref[x * NC:x * NC + 1, z * rows:(z + 1) * rows]
            for c in range(1, NC):
                part = jnp.where(me_c == c, target_ref[x * NC + c:x * NC + c + 1, z * rows:(z + 1) * rows], part)
            pieces += [part, gap]
        lab_ref[z] = jnp.concatenate(pieces, axis=1)

    def attend(block, g):
        cols = slice(g * HEAD_DIM, (g + 1) * HEAD_DIM)
        if block is None:
            kk, vv = kv[me_z, 0, :, cols], kv[me_z, 1, :, cols]
            seen = (me_z * rows + j_pos >= first) & (j_pos <= i_pos)
        else:
            kk, vv = kv[block, 0, :, cols], kv[block, 1, :, cols]
            seen = block * rows + j_pos >= first
        for h in range(g * per, (g + 1) * per):
            raw = dot(q_ref[:, h * HEAD_DIM:(h + 1) * HEAD_DIM], kk, NT)
            capped = ATTENTION_CAP * jnp.tanh(raw * (HEAD_DIM ** (-0.5) / ATTENTION_CAP))
            wt = jnp.where(seen, jnp.exp(capped), 0.0)
            top = dot(wt.astype(jnp.bfloat16), vv, NN)
            low = jnp.broadcast_to(jnp.sum(wt, axis=1, keepdims=True), (rows, 128))
            if block is None:
                num[h] = top
                den[h] = low
            else:
                num[h] = num[h] + top
                den[h] = den[h] + low

    def arrived(block, g):
        kv_copy(block, g).wait_recv()

        @pl.when(me_z + 1 < NZ)
        def _():
            kv_copy(block, g).start()

    @pl.when(me_z >= 0)
    def _():
        for g in range(groups):
            attend(None, g)

    top, bottom = me_z == NZ - 1, me_z == 0
    under = jnp.logical_not(top) if NZ > 2 else me_z >= 0

    def tell(i, z):
        pl.semaphore_signal(token.at[i], inc=1, device_id=dev(z=lax.rem(z + NZ, NZ)), device_id_type=MESH)

    if NZ > 1:
        @pl.when(bottom)
        def _():
            tell(0, me_z + 1)

        @pl.when(top)
        def _():
            tell(1, me_z - 1)

        @pl.when(jnp.logical_not(bottom | top))
        def _():
            pl.semaphore_wait(token.at[1], 1)
            tell(1, me_z - 1)
            pl.semaphore_wait(token.at[0], 1)
            tell(0, me_z + 1)

    for block in range(NZ - 2, 0, -1):
        @pl.when(block < me_z)
        def _(block=block):
            for g in range(groups):
                arrived(block, g)
                attend(block, g)

    gw = per * HEAD_DIM

    def att_copy(g, peer, idx):
        ref = att.at[me_t, :, pl.ds(g * gw, gw)]
        return remote(ref, ref, att_send.at[idx], att_recv.at[me_t, g], dev(t=peer))

    step = 256 if fw % 256 == 0 else fw

    def project(t, g, begin):
        base = pl.multiple_of(t * qw + g * gw, gw)
        left = att[t, :, g * gw:(g + 1) * gw]
        for n in range(fw // step):
            cols = slice(n * step, (n + 1) * step)
            got = dot(left, w_ref[pl.ds(base, gw), cols], NN)
            branch[:, cols] = got if begin else branch[:, cols] + got

    for g in range(groups):
        if NZ > 1:
            @pl.when(me_z > 0)
            def _(g=g):
                arrived(0, g)
                attend(0, g)
        for h in range(g * per, (g + 1) * per):
            att[me_t, :, h * HEAD_DIM:(h + 1) * HEAD_DIM] = (num[h] / den[h][:, :1]).astype(jnp.bfloat16)
        for i, p in enumerate(others(me_t, NY)):
            att_copy(g, p, i).start()
        if g == 0:
            w_copy.wait()
        project(me_t, g, g == 0)
    for g in range(groups):
        for p in others(me_t, NY):
            ref = att.at[p, :, pl.ds(g * gw, gw)]
            remote(ref, ref, att_send.at[0], att_recv.at[p, g], dev()).wait_recv()
            project(p, g, False)

    for c in loads[7:10]:
        c.wait()
    br = branch[...]
    carried = res_ref[...].astype(jnp.float32)
    gained = pg_ref[...].reshape(1, fw) * br
    lane = lax.broadcasted_iota(jnp.int32, (rows, 128), 1)
    packed = jnp.zeros((rows, 128), jnp.float32)
    for i, prod in enumerate((br * br, carried * carried, carried * gained, gained * gained)):
        packed = jnp.where(lane == i, jnp.sum(prod, axis=1, keepdims=True), packed)
    stat[me_t] = packed

    def stat_copy(peer, i):
        return remote(stat.at[me_t], stat.at[me_t], st_send.at[i], st_recv.at[me_t], dev(t=peer))

    for i, p in enumerate(others(me_t, NY)):
        stat_copy(p, i).start()
    for p in others(me_t, NY):
        remote(stat.at[p], stat.at[p], st_send.at[0], st_recv.at[p], dev()).wait_recv()
    total = stat[0]
    for t in range(1, NY):
        total = total + stat[t]
    sq_branch, sq_carried, cross, sq_gained = (total[:, i:i + 1] for i in range(4))
    inv_branch = 1.0 / jnp.sqrt(sq_branch / D + EPSILON)
    sq_total = sq_carried + 2.0 * inv_branch * cross + inv_branch * inv_branch * sq_gained
    inv_total = 1.0 / jnp.sqrt(sq_total / D + EPSILON)
    hid[me_z, me_t, me_x, :rows, :] = (
        fg_ref[...].reshape(1, fw) * (carried + gained * inv_branch) * inv_total
    ).astype(jnp.bfloat16)

    y_peers = others(me_t, NY)
    x_peers = others(me_x, NX)
    cut = min(rows, (rows // 2 + 7) // 8 * 8)
    spans = [(0, cut)] + ([(cut, rows - cut)] if cut < rows else [])
    K = len(spans)

    def xdev(x):
        return dev(d=x * NC + me_c)

    def block(z, t, x, k):
        return hid.at[z, t, x, pl.ds(*spans[k]), :]

    def send(z, t, x, k, sem, device):
        return remote(block(z, t, x, k), block(z, t, x, k), sem, hid_recv.at[z, t, x, k], device)

    def landed(z, t, x, k):
        send(z, t, x, k, z_send.at[0], dev()).wait_recv()

    def step_of(n):
        return me_z if n == 0 else jnp.where(n <= me_z, me_z - n, n)

    def spread(n, act, wait):
        z = step_of(n)
        for k in range(K):
            if wait and n > 0:
                landed(z, me_t, me_x, k)
            for i, p in enumerate(x_peers):
                act(send(z, me_t, me_x, k, x_send.at[0, i], xdev(p)))
            for i, p in enumerate(y_peers):
                act(send(z, me_t, me_x, k, y_send.at[0, i], dev(t=p)))

            @pl.when(jnp.logical_not(top) & (z <= me_z))
            def _(k=k):
                act(send(z, me_t, me_x, k, z_send.at[z], dev(z=lax.rem(me_z + 1, NZ))))
        if n == 0:
            for off in range(1, NZ):
                @pl.when(off <= me_z)
                def _(off=off):
                    for k in range(K):
                        p = lax.rem(me_z + NZ - off, NZ)
                        act(send(me_z, me_t, me_x, k, d_send.at[off - 1], dev(z=p)))

    def lift(act):
        for j, x in enumerate(x_peers):
            for i, t in enumerate(y_peers):
                for k in range(K):
                    act(send(me_z, t, x, k, u_send.at[j, i], dev(z=NZ - 1)))

    def relay(n, act, wait):
        z = step_of(n)
        for j, x in enumerate(x_peers):
            if wait:
                landed(z, me_t, x, 0)
            for i, p in enumerate(y_peers):
                act(send(z, me_t, x, 0, y_send.at[1 + j, i], dev(t=p)))
        for j, t in enumerate(y_peers):
            if wait:
                landed(z, t, me_x, K - 1)
            if K > 1:
                for i, p in enumerate(x_peers):
                    act(send(z, t, me_x, K - 1, x_send.at[1 + j, i], xdev(p)))

    def start(c):
        c.start()

    count = voc_hbm.shape[-2]
    home = (me_x * NZ + me_z) * NY + me_t
    row_ids = lax.broadcasted_iota(jnp.int32, (count, lines), 0)

    def product(c, z, t):
        right = hid[z, t].reshape(lines, fw)
        if len(voc_ref.shape) == 3:
            start_col = t * fw if isinstance(t, int) else pl.multiple_of(t * fw, 128)
            left = voc_ref[c, :, pl.ds(start_col, fw)]
        else:
            left = voc_ref[c, t]
        return dot(left, right, NT)

    def gather(n, z, t, begin):
        @pl.loop(0, NC)
        def _(c):
            got = product(c, z, t)
            held[n, c] = got if begin else held[n, c] + got

    def finish(n, z, t, begin):
        label = lab_ref[z]

        def part(c, sums):
            acc = product(c, z, t)
            if not begin:
                acc = held[n, c] + acc
            capped = LOGIT_CAP * jnp.tanh(acc * (1.0 / LOGIT_CAP))
            base = (((me_x * NC + c) * NZ + me_z) * NY + me_t) * count
            tot = sums[0] + jnp.sum(jnp.exp(capped), axis=0, keepdims=True)
            cho = sums[1] + jnp.sum(jnp.where(row_ids == label - base, capped, 0.0), axis=0, keepdims=True)
            return tot, cho

        zero = jnp.zeros((1, lines), jnp.float32)
        return lax.fori_loop(0, NC, part, (zero, zero))

    def begin_slice(n):
        z = step_of(n)
        for x in x_peers:
            for k in range(1, K):
                landed(z, me_t, x, k)
        if n > 0 and NZ > 2:
            @pl.when(top)
            def _():
                for x in x_peers:
                    landed(z, me_t, x, 0)
        if n == 0:
            voc_ready()
        if NY > 1:
            gather(n, z, me_t, True)

    def end_slice(n, before_last=None):
        z = step_of(n)
        if n > 0 and NZ > 2:
            @pl.when(top)
            def _():
                for t in y_peers:
                    landed(z, t, me_x, K - 1)
        last = me_t
        for i, t in enumerate(y_peers):
            for k in range(K - 1):
                landed(z, t, me_x, k)
            for x in x_peers:
                for k in range(K):
                    landed(z, t, x, k)
            last = t
            if i + 1 < len(y_peers):
                gather(n, z, t, False)
        if before_last is not None:
            before_last()
        return z, *finish(n, z, last, NY == 1)

    family = [(x, z, t) for x in range(NX) for z in range(NZ) for t in range(NY)]
    G = len(family)

    def wrap(v, n):
        return jnp.where(v >= n, v - n, v)

    def kin_of(i):
        return wrap(me_x + i // (NZ * NY), NX), wrap(me_z + i // NY % NZ, NZ), wrap(me_t + i % NY, NY)

    def kin(i):
        x, z, t = kin_of(i)
        return dev(d=x * NC + me_c, z=z, t=t)

    def early(i):
        return remote(early_buf.at[home], early_buf.at[home], f_send.at[0], f_recv.at[0], kin(i))

    def late(i):
        return remote(late_buf.at[home], late_buf.at[home], f_send.at[1], f_recv.at[1], kin(i))

    def send_early():
        for i in range(1, G):
            early(i).start()

    def voc_ready():
        loads[11].wait()
        for p in twin:
            other = lax.rem(p, NC)
            remote(voc_hbm, voc_ref.at[other], voc_send.at[0], voc_recv.at[other], dev()).wait_recv()

    def score(n):
        if n + 1 < NZ:
            z, tot, cho = end_slice(n)
            early_buf[home, pl.ds(z, 1), :] = tot
            early_buf[home, pl.ds(NZ + z, 1), :] = cho
        else:
            early_buf[home, pl.ds(step_of(n), 1), :] = code_line
            early_buf[home, pl.ds(NZ + step_of(n), 1), :] = jnp.zeros((1, lines), jnp.float32)
            z, tot, cho = end_slice(n, send_early)
            late_buf[home, 0:1, :] = tot
            late_buf[home, 1:2, :] = cho

    if NZ > 1:
        @pl.when(top)
        def _():
            pl.semaphore_wait(token.at[0], 1)

    spread(0, start, True)

    @pl.when(bottom)
    def _():
        relay(0, start, True)

    if NZ > 1:
        @pl.when(bottom)
        def _():
            pl.semaphore_wait(token.at[1], 1)

        spread(1, start, True)

        @pl.when(jnp.logical_not(bottom))
        def _():
            relay(0, start, True)

    for n in range(2, NZ):
        @pl.when(n <= me_z)
        def _(n=n):
            spread(n, start, True)

    if NZ > 1:
        @pl.when(under)
        def _():
            relay(1, start, True)

    if NZ > 3:
        @pl.when(me_z == NZ - 2)
        def _():
            spread(NZ - 1, start, True)

    for n in range(2, NZ):
        @pl.when((n > me_z) & ((n < NZ - 1) | (me_z != NZ - 2) | (NZ == 3)))
        def _(n=n):
            spread(n, start, True)

        if n == 2:
            begin_slice(0)
        else:
            begin_slice(n - 1)
        score(n - 2)
        if n == 2 and NZ > 3:
            begin_slice(1)

        @pl.when(under)
        def _(n=n):
            relay(n, start, True)
            if n == 2:
                lift(start)

    if NZ < 3:
        begin_slice(0)
    if NZ == 3:
        begin_slice(1)
    if NZ > 1:
        begin_slice(NZ - 1)
        score(NZ - 2)
    score(NZ - 1)
    for i in range(1, G):
        late(i).start()
    def others_of(buf, k):
        ref = buf.at[pl.ds(0, G - 1)]
        return remote(ref, ref, f_send.at[k], f_recv.at[k], dev())

    if G > 1:
        others_of(early_buf, 0).wait_recv()

    def last_of(z):
        return NZ - 1 if z < NZ - 1 else 0

    def summed(buf, z):
        out = None
        for x in range(NX):
            for t in range(NY):
                part = buf[(x * NZ + z) * NY + t]
                out = part if out is None else out + part
        return out

    empty = jnp.zeros((1, lines), jnp.float32)
    totals, chosen, codes = [empty] * NZ, [empty] * NZ, [empty] * NZ
    for z in range(NZ):
        sums = summed(early_buf, z)
        for w in range(NZ):
            if w == last_of(z):
                codes[z] = sums[w:w + 1]
            else:
                totals[w] = totals[w] + sums[w:w + 1]
                chosen[w] = chosen[w] + sums[NZ + w:NZ + w + 1]
    if G > 1:
        others_of(late_buf, 1).wait_recv()
    for z in range(NZ):
        sums = summed(late_buf, z)
        totals[last_of(z)] = totals[last_of(z)] + sums[0:1]
        chosen[last_of(z)] = chosen[last_of(z)] + sums[1:2]
    totals, chosen, code = (jnp.concatenate(p, axis=0) for p in (totals, chosen, codes))
    inside = lax.rem(lax.broadcasted_iota(jnp.int32, (NZ, lines), 1), PAD) < rows
    counted = jnp.where(inside & (code >= docs), 1.0, 0.0)
    doc = jnp.where(code >= docs, code - docs, code)
    logprob = jnp.where(inside, counted * (chosen - jnp.log(totals)), 0.0)
    names = lax.broadcasted_iota(jnp.int32, (docs, lines), 0).astype(jnp.float32)
    like = jnp.zeros((docs, lines), jnp.float32)
    cnt = jnp.zeros((docs, lines), jnp.float32)
    for r in range(NZ):
        hit = names == doc[r:r + 1, :]
        like = like + jnp.where(hit, logprob[r:r + 1, :], 0.0)
        cnt = cnt + jnp.where(hit, counted[r:r + 1, :], 0.0)
    docs_eye = lax.broadcasted_iota(jnp.int32, (docs, 128), 0) == lax.broadcasted_iota(jnp.int32, (docs, 128), 1)
    sums = [
        jnp.sum(jnp.where(docs_eye, jnp.sum(v, axis=1, keepdims=True), 0.0), axis=0, keepdims=True)
        for v in (like, cnt)
    ]
    twin_buf[me_c, 0:1, :] = sums[0]
    twin_buf[me_c, 1:2, :] = sums[1]
    twin_copies = [
        remote(twin_buf.at[me_c], twin_buf.at[me_c], tw_send.at[0], tw_recv.at[me_c], dev(d=p)) for p in twin
    ]
    for c in twin_copies:
        c.start()
    mine = jnp.zeros((1, rows), jnp.float32)
    for z in range(NZ):
        for x in range(NX):
            mine = jnp.where((me_z == z) & (me_x == x), logprob[z:z + 1, x * PAD:x * PAD + rows], mine)
    out_ref[0:1, :rows] = mine
    for i, p in enumerate(others(me_t, NY)):
        remote(att.at[me_t], att.at[me_t], att_send.at[i], att_recv.at[me_t, 0], dev()).wait_send()
        stat_copy(p, i).wait_send()

    def sent(ref, sem):
        remote(ref, ref, sem, hid_recv.at[0, 0, 0, 0], dev()).wait_send()

    def portion(k, n):
        return hid.at[pl.ds(0, n), 0, 0, pl.ds(*k), :]

    whole = (0, rows)
    for i in range(len(x_peers)):
        sent(portion(whole, NZ), x_send.at[0, i])
    for i in range(len(y_peers)):
        sent(portion(whole, NZ), y_send.at[0, i])

    def relays_sent(n):
        for j in range(len(x_peers)):
            for i in range(len(y_peers)):
                sent(portion(spans[0], n), y_send.at[1 + j, i])
        for j in range(len(y_peers)):
            if K > 1:
                for i in range(len(x_peers)):
                    sent(portion(spans[K - 1], n), x_send.at[1 + j, i])

    @pl.when(under)
    def _():
        relays_sent(NZ)
        if NZ > 2:
            for j in range(len(x_peers)):
                for i in range(len(y_peers)):
                    sent(portion(whole, 1), u_send.at[j, i])

    if NZ > 2:
        @pl.when(top)
        def _():
            relays_sent(1)

    for z in range(NZ - 1):
        @pl.when(jnp.logical_not(top) & (z <= me_z))
        def _(z=z):
            sent(portion(whole, 1), z_send.at[z])

        @pl.when(z < me_z)
        def _(z=z):
            sent(portion(whole, 1), d_send.at[z])
    for block in range(NZ - 1):
        @pl.when((me_z >= block) & (me_z + 1 < NZ))
        def _(block=block):
            kv_sent(block)
    if G > 1:
        others_of(early_buf, 0).wait_send()
        others_of(late_buf, 1).wait_send()
    for c in voc_copies:
        c.wait_send()
    for p in twin:
        other = lax.rem(p, NC)
        remote(twin_buf.at[other], twin_buf.at[other], tw_send.at[0], tw_recv.at[other], dev()).wait_recv()
    for c in twin_copies:
        c.wait_send()
    both = twin_buf[0]
    for c in range(1, NC):
        both = both + twin_buf[c]
    out_ref[1:3, :] = both


def split(packed, lp_ref, like_ref, cnt_ref):
    lp_ref[...] = packed[0:1, :lp_ref.shape[1]]
    like_ref[...] = packed[1:2, :like_ref.shape[1]]
    cnt_ref[...] = packed[2:3, :cnt_ref.shape[1]]


def local(
    mesh, query_vectors, key_vectors, value_vectors, out_weight, residual, post_gain, final_gain,
    vocab_weight, segment_ids, doc_starts, doc_index, targets,
):
    ND, NZ, NY = mesh.shape["dp"], mesh.shape["seq"], mesh.shape["tensor"]
    rows = query_vectors.shape[0]
    docs = doc_starts.shape[1] * ND
    blocks = ND * NZ
    fw = out_weight.shape[1]
    voc = vocab_weight
    if fw % 128 != 0:
        voc = voc.reshape(voc.shape[0], NY, fw).transpose(1, 0, 2)
    kvw, qw = key_vectors.shape[1], query_vectors.shape[1]
    heads = qw // HEAD_DIM
    groups = kvw // HEAD_DIM
    NC = 2 if ND % 2 == 0 else 1
    NX = ND // NC
    R = blocks * PAD // 128
    f32, bf16, i32 = jnp.float32, jnp.bfloat16, jnp.int32
    dma = pltpu.SemaphoreType.DMA
    lines = NX * PAD
    G = NX * NZ * NY
    anyspace = pl.BlockSpec(memory_space=pl.ANY)
    packed = pl.pallas_call(
        functools.partial(body, (ND, NZ, NY, docs)),
        out_shape=jax.ShapeDtypeStruct((8, 128), f32),
        in_specs=[anyspace] * 12,
        out_specs=pl.BlockSpec(memory_space=pltpu.VMEM),
        scratch_shapes=[
            pltpu.VMEM(query_vectors.shape, bf16),
            pltpu.VMEM(residual.shape, bf16),
            pltpu.VMEM(post_gain.shape, f32),
            pltpu.VMEM(final_gain.shape, f32),
            pltpu.VMEM(segment_ids.shape, i32),
            pltpu.SMEM(doc_starts.shape, i32),
            pltpu.SMEM(doc_index.shape, i32),
            pltpu.VMEM(targets.shape, i32),
            pltpu.VMEM(out_weight.shape, bf16),
            pltpu.VMEM((NC, *voc.shape), bf16),
            pltpu.VMEM((NZ, 2, rows, kvw), bf16),
            pltpu.VMEM((heads, rows, HEAD_DIM), f32),
            pltpu.VMEM((heads, rows, 128), f32),
            pltpu.VMEM((NY, rows, qw), bf16),
            pltpu.VMEM((rows, fw), f32),
            pltpu.VMEM((NY, rows, 128), f32),
            pltpu.VMEM((NZ, NY, NX, PAD, fw), bf16),
            pltpu.VMEM((NZ, NC, voc.shape[-2], lines), f32),
            pltpu.VMEM((NZ, 1, lines), i32),
            pltpu.VMEM((G, 2 * NZ, lines), f32),
            pltpu.VMEM((G, 2, lines), f32),
            pltpu.VMEM((NC, 2, 128), f32),
            dma((12,)),
            dma((NZ,)), dma((NZ, groups)),
            dma((NY,)), dma((NY, groups)),
            dma((NY,)), dma((NY,)),
            dma((NZ, NY, NX, 2)),
            dma((NZ,)),
            dma((NZ,)),
            dma((NX, NY)),
            pltpu.SemaphoreType.REGULAR((2,)),
            dma((NX, NY)),
            dma((NY, NX)),
            dma((1,)), dma((NC,)),
            dma((2,)), dma((2,)),
            dma((1,)), dma((NC,)),
        ],
        compiler_params=pltpu.CompilerParams(
            collective_id=0, has_side_effects=True, vmem_limit_bytes=60 * 1024 * 1024
        ),
        name="packed_loglik",
    )(
        query_vectors, key_vectors, value_vectors, out_weight, residual, post_gain, final_gain, voc,
        segment_ids, doc_starts, doc_index, targets,
    )
    sums = jax.ShapeDtypeStruct((1, docs), f32)
    logprob, like, counts = pl.pallas_call(
        split, out_shape=(jax.ShapeDtypeStruct((1, rows), f32), sums, sums), name="split"
    )(packed)
    return (logprob, like[0], counts[0])


def solution(mesh):
    in_specs = (
        P(("dp", "seq"), "tensor"),
        P(("dp", "seq"), "tensor"),
        P(("dp", "seq"), "tensor"),
        P(None, "tensor"),
        P(("dp", "seq"), "tensor"),
        P("tensor"),
        P("tensor"),
        P(("dp", "seq", "tensor"), None),
        P("dp", "seq"),
        P("dp", None),
        P("dp", None),
        P(),
    )
    out_specs = (P("dp", "seq"), P(), P())
    return jax.shard_map(
        functools.partial(local, mesh), mesh=mesh, in_specs=in_specs, out_specs=out_specs, check_vma=False
    )
```

```python
import functools

import jax
import jax.numpy as jnp
from jax import lax
from jax.experimental import pallas as pl
from jax.experimental.pallas import tpu as pltpu
from jax.sharding import PartitionSpec as P

HEAD_DIM = 256
ATTENTION_CAP = 50.0
LOGIT_CAP = 30.0
EPSILON = 1e-06
MESH = pl.DeviceIdType.MESH
PAD = 64
NT = (((1,), (1,)), ((), ()))
NN = (((1,), (0,)), ((), ()))


def dot(a, b, dims):
    return lax.dot_general(a, b, dims, preferred_element_type=jnp.float32)


def body(
    sizes,
    q_hbm, k_hbm, v_hbm, w_hbm, res_hbm, pg_hbm, fg_hbm, voc_hbm, seg_hbm, start_hbm, index_hbm, target_hbm,
    out_ref,
    q_ref, top_first, over, under_sum, res_ref, pg_ref, fg_ref, seg_ref, start_ref, index_ref, target_ref,
    w_ref, voc_ref, kv, num, den, att, branch, stat, hid, held, lab_ref, early_buf, late_buf, twin_buf,
    local_sem, q_send, q_recv, o_send, o_recv, kv_send, kv_recv, att_send, att_recv, st_send, st_recv,
    hid_recv, z_send, d_send, u_send, token, y_send, x_send, voc_send, voc_recv, f_send, f_recv, tw_send, tw_recv,
):
    ND, NZ, NY, docs = sizes
    NC = 2 if ND % 2 == 0 else 1
    NX = ND // NC
    D = voc_hbm.shape[-1] if voc_hbm.ndim == 2 else voc_hbm.shape[0] * voc_hbm.shape[2]
    me_d, me_z, me_t = lax.axis_index("dp"), lax.axis_index("seq"), lax.axis_index("tensor")
    me_x, me_c = me_d // NC, me_d % NC
    twin = [me_x * NC + 1 - me_c] if NC == 2 else []
    rows = q_hbm.shape[0]
    kvw = k_hbm.shape[1]
    groups = kvw // HEAD_DIM
    per = q_hbm.shape[1] // kvw
    heads = groups * per
    qw = q_hbm.shape[1]
    fw = w_hbm.shape[1]

    pairs = [
        (k_hbm, kv.at[me_z, 0]), (v_hbm, kv.at[me_z, 1]), (q_hbm, q_ref.at[0]), (seg_hbm, seg_ref.at[0]), (start_hbm, start_ref),
        (index_hbm, index_ref), (target_hbm, target_ref), (res_hbm, res_ref), (pg_hbm, pg_ref), (fg_hbm, fg_ref),
        (w_hbm, w_ref), (voc_hbm, voc_ref.at[me_c]),
    ]
    loads = [pltpu.make_async_copy(src, dst, local_sem.at[i]) for i, (src, dst) in enumerate(pairs)]
    for c in loads:
        c.start()
    w_copy = loads[10]

    def dev(d=None, z=None, t=None):
        return (me_d if d is None else d, me_z if z is None else z, me_t if t is None else t)

    def remote(src, dst, send, recv, device):
        return pltpu.make_async_remote_copy(
            src_ref=src, dst_ref=dst, send_sem=send, recv_sem=recv, device_id=device, device_id_type=MESH
        )

    def others(me, n):
        return [jnp.where(me + i >= n, me + i - n, me + i) for i in range(1, n)]

    barrier = pltpu.get_barrier_semaphore()
    peers = [dev(d=p * NC + me_c) for p in others(me_x, NX)] + [dev(d=p) for p in twin]
    peers += [dev(t=p) for p in others(me_t, NY)]
    ups = [(me_z + 1 < NZ, dev(z=lax.rem(me_z + 1, NZ))), (me_z >= 1, dev(z=lax.rem(me_z + NZ - 1, NZ)))]
    for p in peers:
        pl.semaphore_signal(barrier, inc=1, device_id=p, device_id_type=MESH)
    for there, p in ups:
        @pl.when(there)
        def _(p=p):
            pl.semaphore_signal(barrier, inc=1, device_id=p, device_id_type=MESH)
    for c in loads[:2]:
        c.wait()

    def kv_copy(block, g):
        ref = kv.at[block, :, :, pl.ds(g * HEAD_DIM, HEAD_DIM)]
        return remote(ref, ref, kv_send.at[block], kv_recv.at[block, g], dev(z=lax.rem(me_z + 1, NZ)))

    def kv_sent(block):
        remote(kv.at[block], kv.at[block], kv_send.at[block], kv_recv.at[block, 0], dev()).wait_send()

    ends = lax.div(me_z + NZ - 1, NZ) + lax.div(2 * NZ - 2 - me_z, NZ)
    pl.semaphore_wait(barrier, len(peers) + ends)
    @pl.when(me_z < NZ - 2)
    def _():
        for g in range(groups):
            kv_copy(me_z, g).start()
    voc_copies = [
        remote(voc_hbm, voc_ref.at[me_c], voc_send.at[0], voc_recv.at[me_c], dev(d=p)) for p in twin
    ]
    for c in voc_copies:
        c.start()
    for c in loads[2:7]:
        c.wait()
    def first_of(seg):
        out = jnp.zeros((1, rows), jnp.int32)
        for n in range(start_ref.shape[1]):
            out = jnp.where(seg == n, start_ref[0, n], out)
        return out

    seg = seg_ref[0]
    first_row = jnp.zeros((1, rows), jnp.int32)
    end_row = jnp.zeros((1, rows), jnp.int32)
    doc_row = jnp.zeros((1, rows), jnp.int32)
    segs = start_ref.shape[1]
    for n in range(segs):
        here = seg == n
        first_row = jnp.where(here, start_ref[0, n], first_row)
        end_row = jnp.where(here, start_ref[0, n + 1] if n + 1 < segs else rows * NZ, end_row)
        doc_row = jnp.where(here, index_ref[0, n], doc_row)
    spot = me_z * rows + lax.broadcasted_iota(jnp.int32, (1, rows), 1)
    code_row = doc_row + jnp.where(spot + 1 < end_row, docs, 0)
    i_pos = lax.broadcasted_iota(jnp.int32, (rows, rows), 0)
    j_pos = lax.broadcasted_iota(jnp.int32, (rows, rows), 1)

    def column_of(row):
        full = jnp.broadcast_to(row.astype(jnp.float32), (rows, rows))
        return jnp.sum(jnp.where(i_pos == j_pos, full, 0.0), axis=1, keepdims=True)

    first = column_of(first_row).astype(jnp.int32)
    top, bottom, helper = me_z == NZ - 1, me_z == 0, me_z == NZ - 2
    gw = per * HEAD_DIM

    def query_copy(g):
        cols = pl.ds(g * gw, gw)
        return remote(
            q_ref.at[0, :, cols], q_ref.at[1, :, cols], q_send.at[0], q_recv.at[g], dev(z=lax.rem(me_z + NZ - 1, NZ))
        )

    def segment_copy():
        return remote(seg_ref.at[0], seg_ref.at[1], q_send.at[1], q_recv.at[groups], dev(z=lax.rem(me_z + NZ - 1, NZ)))

    def part_copies(g):
        cols = pl.ds(g * gw, gw)
        above = dev(z=lax.rem(me_z + 1, NZ))
        return [
            remote(over.at[:, cols], over.at[:, cols], o_send.at[0], o_recv.at[0, g], above),
            remote(under_sum.at[g], under_sum.at[g], o_send.at[1], o_recv.at[1, g], above),
        ]

    if NZ > 1:
        @pl.when(top)
        def _():
            segment_copy().start()
            for g in range(groups):
                query_copy(g).start()

    lines = NX * PAD
    lanes = lax.broadcasted_iota(jnp.int32, (rows, lines), 1)
    sub = lax.broadcasted_iota(jnp.int32, (rows, lines), 0)
    placed = jnp.where(lanes == sub + me_x * PAD, column_of(code_row), 0.0)
    code_line = jnp.sum(placed, axis=0, keepdims=True) * jnp.where(me_t == 0, 1.0, 0.0)
    gap = jnp.zeros((1, PAD - rows), jnp.int32)
    for z in range(NZ):
        pieces = []
        for x in range(NX):
            part = target_ref[x * NC:x * NC + 1, z * rows:(z + 1) * rows]
            for c in range(1, NC):
                part = jnp.where(me_c == c, target_ref[x * NC + c:x * NC + c + 1, z * rows:(z + 1) * rows], part)
            pieces += [part, gap]
        lab_ref[z] = jnp.concatenate(pieces, axis=1)

    def attend(g, *jobs):
        cols = slice(g * HEAD_DIM, (g + 1) * HEAD_DIM)
        span = range(g * per, (g + 1) * per)
        raws, parts = [], {}
        for who, block in jobs:
            kk = kv[me_z if block is None else block, 0, :, cols]
            for h in span:
                raws.append(dot(q_ref[who, :, h * HEAD_DIM:(h + 1) * HEAD_DIM], kk, NT))
        wts = []
        for i, raw in enumerate(raws):
            who, block = jobs[i // per]
            if block is None:
                seen = (me_z * rows + j_pos >= first) & (j_pos <= i_pos)
            else:
                seen = block * rows + j_pos >= (first if who == 0 else top_first[:, :1])
            capped = ATTENTION_CAP * jnp.tanh(raw * (HEAD_DIM ** (-0.5) / ATTENTION_CAP))
            wts.append(jnp.where(seen, jnp.exp(capped), 0.0))
        for i, wt in enumerate(wts):
            who, block = jobs[i // per]
            vv = kv[me_z if block is None else block, 1, :, cols]
            up = dot(wt.astype(jnp.bfloat16), vv, NN)
            low = jnp.broadcast_to(jnp.sum(wt, axis=1, keepdims=True), (rows, 128))
            at = who * heads + span[i % per]
            if at in parts:
                parts[at] = (parts[at][0] + up, parts[at][1] + low)
            elif who == 0 and block is not None:
                parts[at] = (num[at] + up, den[at] + low)
            else:
                parts[at] = (up, low)
        for at, (up, low) in parts.items():
            num[at] = up
            den[at] = low

    def arrived(block, g):
        kv_copy(block, g).wait_recv()

        @pl.when(me_z < NZ - 2)
        def _():
            kv_copy(block, g).start()

    @pl.when(me_z >= 0)
    def _():
        for g in range(groups):
            attend(g, (0, None))

    under = jnp.logical_not(top) if NZ > 2 else me_z >= 0

    def tell(i, z):
        pl.semaphore_signal(token.at[i], inc=1, device_id=dev(z=lax.rem(z + NZ, NZ)), device_id_type=MESH)

    if NZ > 1:
        @pl.when(bottom)
        def _():
            tell(0, me_z + 1)

        @pl.when(top)
        def _():
            tell(1, me_z - 1)

        @pl.when(jnp.logical_not(bottom | top))
        def _():
            pl.semaphore_wait(token.at[1], 1)
            tell(1, me_z - 1)
            pl.semaphore_wait(token.at[0], 1)
            tell(0, me_z + 1)

    for block in range(NZ - 3, 0, -1):
        @pl.when((block < me_z) & jnp.logical_not(top))
        def _(block=block):
            for g in range(groups):
                arrived(block, g)
                attend(g, (0, block))

    if NZ > 1:
        @pl.when(helper)
        def _():
            segment_copy().wait_recv()
            top_first[...] = jnp.broadcast_to(column_of(first_of(seg_ref[1])).astype(jnp.int32), (rows, 128))
            under_sum[...] = jnp.zeros(under_sum.shape, jnp.float32)
    def att_copy(g, peer, idx):
        ref = att.at[me_t, :, pl.ds(g * gw, gw)]
        return remote(ref, ref, att_send.at[idx], att_recv.at[me_t, g], dev(t=peer))

    step = 256 if fw % 256 == 0 else fw

    def project(t, g, begin):
        base = pl.multiple_of(t * qw + g * gw, gw)
        left = att[t, :, g * gw:(g + 1) * gw]
        for n in range(fw // step):
            cols = slice(n * step, (n + 1) * step)
            got = dot(left, w_ref[pl.ds(base, gw), cols], NN)
            branch[:, cols] = got if begin else branch[:, cols] + got

    for g in range(groups):
        if NZ > 1:
            @pl.when((me_z > 0) & jnp.logical_not(top | helper))
            def _(g=g):
                arrived(0, g)
                attend(g, (0, 0))

            @pl.when(helper)
            def _(g=g):
                query_copy(g).wait_recv()
                if NZ > 2:
                    arrived(0, g)
                    attend(g, (0, 0), *[(1, block) for block in range(NZ - 1)])
                else:
                    attend(g, (1, 0))

            @pl.when(top)
            def _(g=g):
                for c in part_copies(g):
                    c.wait_recv()
                for h in range(g * per, (g + 1) * per):
                    num[h] = num[h] + over[:, h * HEAD_DIM:(h + 1) * HEAD_DIM].astype(jnp.float32)
                    r = h - g * per
                    den[h] = den[h] + jnp.broadcast_to(column_of(under_sum[g, r:r + 1, :rows]), (rows, 128))

        for h in range(g * per, (g + 1) * per):
            att[me_t, :, h * HEAD_DIM:(h + 1) * HEAD_DIM] = (num[h] / den[h][:, :1]).astype(jnp.bfloat16)
        for i, p in enumerate(others(me_t, NY)):
            att_copy(g, p, i).start()
        if NZ > 1:
            @pl.when(helper)
            def _(g=g):
                for h in range(g * per, (g + 1) * per):
                    over[:, h * HEAD_DIM:(h + 1) * HEAD_DIM] = num[heads + h].astype(jnp.bfloat16)
                    wide = jnp.broadcast_to(den[heads + h][:, :1], (rows, rows))
                    r = h - g * per
                    under_sum[g, r:r + 1, :rows] = jnp.sum(jnp.where(i_pos == j_pos, wide, 0.0), axis=0, keepdims=True)
                for c in part_copies(g):
                    c.start()

        if g == 0:
            w_copy.wait()
        project(me_t, g, g == 0)
    for g in range(groups):
        for p in others(me_t, NY):
            ref = att.at[p, :, pl.ds(g * gw, gw)]
            remote(ref, ref, att_send.at[0], att_recv.at[p, g], dev()).wait_recv()
            project(p, g, False)

    for c in loads[7:10]:
        c.wait()
    br = branch[...]
    carried = res_ref[...].astype(jnp.float32)
    gained = pg_ref[...].reshape(1, fw) * br
    lane = lax.broadcasted_iota(jnp.int32, (rows, 128), 1)
    packed = jnp.zeros((rows, 128), jnp.float32)
    for i, prod in enumerate((br * br, carried * carried, carried * gained, gained * gained)):
        packed = jnp.where(lane == i, jnp.sum(prod, axis=1, keepdims=True), packed)
    stat[me_t] = packed

    def stat_copy(peer, i):
        return remote(stat.at[me_t], stat.at[me_t], st_send.at[i], st_recv.at[me_t], dev(t=peer))

    for i, p in enumerate(others(me_t, NY)):
        stat_copy(p, i).start()
    for p in others(me_t, NY):
        remote(stat.at[p], stat.at[p], st_send.at[0], st_recv.at[p], dev()).wait_recv()
    total = stat[0]
    for t in range(1, NY):
        total = total + stat[t]
    sq_branch, sq_carried, cross, sq_gained = (total[:, i:i + 1] for i in range(4))
    inv_branch = 1.0 / jnp.sqrt(sq_branch / D + EPSILON)
    sq_total = sq_carried + 2.0 * inv_branch * cross + inv_branch * inv_branch * sq_gained
    inv_total = 1.0 / jnp.sqrt(sq_total / D + EPSILON)
    hid[me_z, me_t, me_x, :rows, :] = (
        fg_ref[...].reshape(1, fw) * (carried + gained * inv_branch) * inv_total
    ).astype(jnp.bfloat16)

    y_peers = others(me_t, NY)
    x_peers = others(me_x, NX)
    cut = min(rows, (rows // 2 + 7) // 8 * 8)
    spans = [(0, cut)] + ([(cut, rows - cut)] if cut < rows else [])
    K = len(spans)

    def xdev(x):
        return dev(d=x * NC + me_c)

    def block(z, t, x, k):
        return hid.at[z, t, x, pl.ds(*spans[k]), :]

    def send(z, t, x, k, sem, device):
        return remote(block(z, t, x, k), block(z, t, x, k), sem, hid_recv.at[z, t, x, k], device)

    def landed(z, t, x, k):
        send(z, t, x, k, z_send.at[0], dev()).wait_recv()

    def step_of(n):
        if n == 0:
            return me_z
        out = jnp.where(n <= me_z, me_z - n, n)
        return jnp.where(top, 0 if n == 1 else me_z - n + 1, out) if NZ > 2 else out

    def climbs(z):
        up = jnp.logical_not(top) & (z <= me_z)
        return up & jnp.logical_not(helper & (z == 0)) if NZ > 2 else up

    def falls(z):
        return (me_z > 0) & (z > me_z) & (z < NZ - 1)

    def spread(n, act, wait):
        z = step_of(n)
        for k in range(K):
            if wait and n > 0:
                landed(z, me_t, me_x, k)
            for i, p in enumerate(x_peers):
                act(send(z, me_t, me_x, k, x_send.at[0, i], xdev(p)))
            for i, p in enumerate(y_peers):
                act(send(z, me_t, me_x, k, y_send.at[0, i], dev(t=p)))

            if n > 0:
                @pl.when(falls(z))
                def _(k=k):
                    act(send(z, me_t, me_x, k, d_send.at[z], dev(z=lax.rem(me_z + NZ - 1, NZ))))

            @pl.when(climbs(z))
            def _(k=k):
                act(send(z, me_t, me_x, k, z_send.at[z], dev(z=lax.rem(me_z + 1, NZ))))
        if n == 0 and NZ > 2:
            @pl.when(bottom)
            def _():
                for k in range(K):
                    act(send(me_z, me_t, me_x, k, z_send.at[NZ - 1], dev(z=NZ - 1)))
        if n == 0:
            for off in range(1, NZ):
                @pl.when((off <= me_z) & (top | (off == 1)))
                def _(off=off):
                    for k in range(K):
                        p = lax.rem(me_z + NZ - off, NZ)
                        act(send(me_z, me_t, me_x, k, d_send.at[off - 1], dev(z=p)))

    def lift(act):
        for j, x in enumerate(x_peers):
            for i, t in enumerate(y_peers):
                for k in range(K):
                    act(send(me_z, t, x, k, u_send.at[j, i], dev(z=NZ - 1)))

    def relay(n, act, wait):
        z = step_of(n)
        for j, x in enumerate(x_peers):
            if wait:
                landed(z, me_t, x, 0)
            for i, p in enumerate(y_peers):
                act(send(z, me_t, x, 0, y_send.at[1 + j, i], dev(t=p)))
        for j, t in enumerate(y_peers):
            if wait:
                landed(z, t, me_x, K - 1)
            if K > 1:
                for i, p in enumerate(x_peers):
                    act(send(z, t, me_x, K - 1, x_send.at[1 + j, i], xdev(p)))

    def start(c):
        c.start()

    count = voc_hbm.shape[-2]
    home = (me_x * NZ + me_z) * NY + me_t
    row_ids = lax.broadcasted_iota(jnp.int32, (count, lines), 0)

    def product(c, z, t):
        right = hid[z, t].reshape(lines, fw)
        if len(voc_ref.shape) == 3:
            start_col = t * fw if isinstance(t, int) else pl.multiple_of(t * fw, 128)
            left = voc_ref[c, :, pl.ds(start_col, fw)]
        else:
            left = voc_ref[c, t]
        return dot(left, right, NT)

    def gather(n, z, t, begin):
        @pl.loop(0, NC)
        def _(c):
            got = product(c, z, t)
            held[n, c] = got if begin else held[n, c] + got

    def finish(n, z, t, begin):
        label = lab_ref[z]

        def part(c, sums):
            acc = product(c, z, t)
            if not begin:
                acc = held[n, c] + acc
            capped = LOGIT_CAP * jnp.tanh(acc * (1.0 / LOGIT_CAP))
            base = (((me_x * NC + c) * NZ + me_z) * NY + me_t) * count
            tot = sums[0] + jnp.sum(jnp.exp(capped), axis=0, keepdims=True)
            cho = sums[1] + jnp.sum(jnp.where(row_ids == label - base, capped, 0.0), axis=0, keepdims=True)
            return tot, cho

        zero = jnp.zeros((1, lines), jnp.float32)
        return lax.fori_loop(0, NC, part, (zero, zero))

    def begin_slice(n):
        z = step_of(n)
        for x in x_peers:
            for k in range(1, K):
                landed(z, me_t, x, k)
        if n > 0 and NZ > 2:
            @pl.when(top)
            def _():
                for x in x_peers:
                    landed(z, me_t, x, 0)
        if n == 0:
            voc_ready()
        if NY > 1:
            gather(n, z, me_t, True)

    def end_slice(n, before_last=None):
        z = step_of(n)
        if n > 0 and NZ > 2:
            @pl.when(top)
            def _():
                for t in y_peers:
                    landed(z, t, me_x, K - 1)
        last = me_t
        for i, t in enumerate(y_peers):
            for k in range(K - 1):
                landed(z, t, me_x, k)
            for x in x_peers:
                for k in range(K):
                    landed(z, t, x, k)
            last = t
            if i + 1 < len(y_peers):
                gather(n, z, t, False)
        if before_last is not None:
            before_last()
        return z, *finish(n, z, last, NY == 1)

    family = [(x, z, t) for x in range(NX) for z in range(NZ) for t in range(NY)]
    G = len(family)

    def wrap(v, n):
        return jnp.where(v >= n, v - n, v)

    def kin_of(i):
        return wrap(me_x + i // (NZ * NY), NX), wrap(me_z + i // NY % NZ, NZ), wrap(me_t + i % NY, NY)

    def kin(i):
        x, z, t = kin_of(i)
        return dev(d=x * NC + me_c, z=z, t=t)

    def early(i):
        return remote(early_buf.at[home], early_buf.at[home], f_send.at[0], f_recv.at[0], kin(i))

    def late(i):
        return remote(late_buf.at[home], late_buf.at[home], f_send.at[1], f_recv.at[1], kin(i))

    def send_early():
        for i in range(1, G):
            early(i).start()

    def voc_ready():
        loads[11].wait()
        for p in twin:
            other = lax.rem(p, NC)
            remote(voc_hbm, voc_ref.at[other], voc_send.at[0], voc_recv.at[other], dev()).wait_recv()

    def score(n):
        if n + 1 < NZ:
            z, tot, cho = end_slice(n)
            early_buf[home, pl.ds(z, 1), :] = tot
            early_buf[home, pl.ds(NZ + z, 1), :] = cho
        else:
            early_buf[home, pl.ds(step_of(n), 1), :] = code_line
            early_buf[home, pl.ds(NZ + step_of(n), 1), :] = jnp.zeros((1, lines), jnp.float32)
            z, tot, cho = end_slice(n, send_early)
            late_buf[home, 0:1, :] = tot
            late_buf[home, 1:2, :] = cho

    if NZ > 1:
        @pl.when(top)
        def _():
            pl.semaphore_wait(token.at[0], 1)

        @pl.when(bottom)
        def _():
            pl.semaphore_wait(token.at[1], 1)

    spread(0, start, True)

    @pl.when(bottom)
    def _():
        relay(0, start, True)

    if NZ > 1:
        spread(1, start, True)

        @pl.when(jnp.logical_not(bottom))
        def _():
            relay(0, start, True)

    for n in range(2, NZ):
        @pl.when(n <= me_z)
        def _(n=n):
            spread(n, start, True)

    if NZ > 1:
        @pl.when(under)
        def _():
            relay(1, start, True)

    if NZ > 3:
        @pl.when(me_z == NZ - 2)
        def _():
            spread(NZ - 1, start, True)

    for n in range(2, NZ):
        @pl.when((n > me_z) & ((n < NZ - 1) | (me_z != NZ - 2) | (NZ == 3)))
        def _(n=n):
            spread(n, start, True)

        if n == 2:
            begin_slice(0)
        else:
            begin_slice(n - 1)
        score(n - 2)
        if n == 2 and NZ > 3:
            begin_slice(1)

        @pl.when(under)
        def _(n=n):
            if n == 2:
                lift(start)
            relay(n, start, True)

    if NZ < 3:
        begin_slice(0)
    if NZ == 3:
        begin_slice(1)
    if NZ > 1:
        begin_slice(NZ - 1)
        score(NZ - 2)
    score(NZ - 1)
    for i in range(1, G):
        late(i).start()
    def others_of(buf, k):
        ref = buf.at[pl.ds(0, G - 1)]
        return remote(ref, ref, f_send.at[k], f_recv.at[k], dev())

    if G > 1:
        others_of(early_buf, 0).wait_recv()

    def last_of(z):
        return NZ - 1 if z < NZ - 1 else min(1, max(NZ - 2, 0))

    def summed(buf, z):
        out = None
        for x in range(NX):
            for t in range(NY):
                part = buf[(x * NZ + z) * NY + t]
                out = part if out is None else out + part
        return out

    empty = jnp.zeros((1, lines), jnp.float32)
    totals, chosen, codes = [empty] * NZ, [empty] * NZ, [empty] * NZ
    for z in range(NZ):
        sums = summed(early_buf, z)
        for w in range(NZ):
            if w == last_of(z):
                codes[z] = sums[w:w + 1]
            else:
                totals[w] = totals[w] + sums[w:w + 1]
                chosen[w] = chosen[w] + sums[NZ + w:NZ + w + 1]
    if G > 1:
        others_of(late_buf, 1).wait_recv()
    for z in range(NZ):
        sums = summed(late_buf, z)
        totals[last_of(z)] = totals[last_of(z)] + sums[0:1]
        chosen[last_of(z)] = chosen[last_of(z)] + sums[1:2]
    totals, chosen, code = (jnp.concatenate(p, axis=0) for p in (totals, chosen, codes))
    inside = lax.rem(lax.broadcasted_iota(jnp.int32, (NZ, lines), 1), PAD) < rows
    counted = jnp.where(inside & (code >= docs), 1.0, 0.0)
    doc = jnp.where(code >= docs, code - docs, code)
    logprob = jnp.where(inside, counted * (chosen - jnp.log(totals)), 0.0)
    names = lax.broadcasted_iota(jnp.int32, (docs, lines), 0).astype(jnp.float32)
    like = jnp.zeros((docs, lines), jnp.float32)
    cnt = jnp.zeros((docs, lines), jnp.float32)
    for r in range(NZ):
        hit = names == doc[r:r + 1, :]
        like = like + jnp.where(hit, logprob[r:r + 1, :], 0.0)
        cnt = cnt + jnp.where(hit, counted[r:r + 1, :], 0.0)
    docs_eye = lax.broadcasted_iota(jnp.int32, (docs, 128), 0) == lax.broadcasted_iota(jnp.int32, (docs, 128), 1)
    sums = [
        jnp.sum(jnp.where(docs_eye, jnp.sum(v, axis=1, keepdims=True), 0.0), axis=0, keepdims=True)
        for v in (like, cnt)
    ]
    twin_buf[me_c, 0:1, :] = sums[0]
    twin_buf[me_c, 1:2, :] = sums[1]
    twin_copies = [
        remote(twin_buf.at[me_c], twin_buf.at[me_c], tw_send.at[0], tw_recv.at[me_c], dev(d=p)) for p in twin
    ]
    for c in twin_copies:
        c.start()
    mine = jnp.zeros((1, rows), jnp.float32)
    for z in range(NZ):
        for x in range(NX):
            mine = jnp.where((me_z == z) & (me_x == x), logprob[z:z + 1, x * PAD:x * PAD + rows], mine)
    out_ref[0:1, :rows] = mine
    for i, p in enumerate(others(me_t, NY)):
        remote(att.at[me_t], att.at[me_t], att_send.at[i], att_recv.at[me_t, 0], dev()).wait_send()
        stat_copy(p, i).wait_send()

    def sent(ref, sem):
        remote(ref, ref, sem, hid_recv.at[0, 0, 0, 0], dev()).wait_send()

    def portion(k, n):
        return hid.at[pl.ds(0, n), 0, 0, pl.ds(*k), :]

    whole = (0, rows)
    for i in range(len(x_peers)):
        sent(portion(whole, NZ), x_send.at[0, i])
    for i in range(len(y_peers)):
        sent(portion(whole, NZ), y_send.at[0, i])

    def relays_sent(n):
        for j in range(len(x_peers)):
            for i in range(len(y_peers)):
                sent(portion(spans[0], n), y_send.at[1 + j, i])
        for j in range(len(y_peers)):
            if K > 1:
                for i in range(len(x_peers)):
                    sent(portion(spans[K - 1], n), x_send.at[1 + j, i])

    @pl.when(under)
    def _():
        relays_sent(NZ)
        if NZ > 2:
            for j in range(len(x_peers)):
                for i in range(len(y_peers)):
                    sent(portion(whole, 1), u_send.at[j, i])

    if NZ > 2:
        @pl.when(bottom)
        def _():
            sent(portion(whole, 1), z_send.at[NZ - 1])

        @pl.when(top)
        def _():
            relays_sent(1)

    for z in range(NZ - 1):
        @pl.when(climbs(z))
        def _(z=z):
            sent(portion(whole, 1), z_send.at[z])

        @pl.when(((z < me_z) & (top | (z == 0))) | falls(z))
        def _(z=z):
            sent(portion(whole, 1), d_send.at[z])
    if NZ > 1:
        @pl.when(top)
        def _():
            segment_copy().wait_send()
            remote(q_ref.at[0], q_ref.at[1], q_send.at[0], q_recv.at[0], dev()).wait_send()

        @pl.when(helper)
        def _():
            remote(over, over, o_send.at[0], o_recv.at[0, 0], dev()).wait_send()
            remote(under_sum, under_sum, o_send.at[1], o_recv.at[1, 0], dev()).wait_send()

    for block in range(NZ - 2):
        @pl.when((me_z >= block) & (me_z < NZ - 2))
        def _(block=block):
            kv_sent(block)
    if G > 1:
        others_of(early_buf, 0).wait_send()
        others_of(late_buf, 1).wait_send()
    for c in voc_copies:
        c.wait_send()
    for p in twin:
        other = lax.rem(p, NC)
        remote(twin_buf.at[other], twin_buf.at[other], tw_send.at[0], tw_recv.at[other], dev()).wait_recv()
    for c in twin_copies:
        c.wait_send()
    both = twin_buf[0]
    for c in range(1, NC):
        both = both + twin_buf[c]
    out_ref[1:3, :] = both


def split(packed, lp_ref, like_ref, cnt_ref):
    lp_ref[...] = packed[0:1, :lp_ref.shape[1]]
    like_ref[...] = packed[1:2, :like_ref.shape[1]]
    cnt_ref[...] = packed[2:3, :cnt_ref.shape[1]]


def local(
    mesh, query_vectors, key_vectors, value_vectors, out_weight, residual, post_gain, final_gain,
    vocab_weight, segment_ids, doc_starts, doc_index, targets,
):
    ND, NZ, NY = mesh.shape["dp"], mesh.shape["seq"], mesh.shape["tensor"]
    rows = query_vectors.shape[0]
    docs = doc_starts.shape[1] * ND
    blocks = ND * NZ
    fw = out_weight.shape[1]
    voc = vocab_weight
    if fw % 128 != 0:
        voc = voc.reshape(voc.shape[0], NY, fw).transpose(1, 0, 2)
    kvw, qw = key_vectors.shape[1], query_vectors.shape[1]
    heads = qw // HEAD_DIM
    groups = kvw // HEAD_DIM
    NC = 2 if ND % 2 == 0 else 1
    NX = ND // NC
    R = blocks * PAD // 128
    f32, bf16, i32 = jnp.float32, jnp.bfloat16, jnp.int32
    dma = pltpu.SemaphoreType.DMA
    lines = NX * PAD
    G = NX * NZ * NY
    anyspace = pl.BlockSpec(memory_space=pl.ANY)
    packed = pl.pallas_call(
        functools.partial(body, (ND, NZ, NY, docs)),
        out_shape=jax.ShapeDtypeStruct((8, 128), f32),
        in_specs=[anyspace] * 12,
        out_specs=pl.BlockSpec(memory_space=pltpu.VMEM),
        scratch_shapes=[
            pltpu.VMEM((2, *query_vectors.shape), bf16),
            pltpu.VMEM((rows, 128), i32),
            pltpu.VMEM(query_vectors.shape, bf16),
            pltpu.VMEM((groups, 8, 128), f32),
            pltpu.VMEM(residual.shape, bf16),
            pltpu.VMEM(post_gain.shape, f32),
            pltpu.VMEM(final_gain.shape, f32),
            pltpu.VMEM((2, *segment_ids.shape), i32),
            pltpu.SMEM(doc_starts.shape, i32),
            pltpu.SMEM(doc_index.shape, i32),
            pltpu.VMEM(targets.shape, i32),
            pltpu.VMEM(out_weight.shape, bf16),
            pltpu.VMEM((NC, *voc.shape), bf16),
            pltpu.VMEM((NZ, 2, rows, kvw), bf16),
            pltpu.VMEM((2 * heads, rows, HEAD_DIM), f32),
            pltpu.VMEM((2 * heads, rows, 128), f32),
            pltpu.VMEM((NY, rows, qw), bf16),
            pltpu.VMEM((rows, fw), f32),
            pltpu.VMEM((NY, rows, 128), f32),
            pltpu.VMEM((NZ, NY, NX, PAD, fw), bf16),
            pltpu.VMEM((NZ, NC, voc.shape[-2], lines), f32),
            pltpu.VMEM((NZ, 1, lines), i32),
            pltpu.VMEM((G, 2 * NZ, lines), f32),
            pltpu.VMEM((G, 2, lines), f32),
            pltpu.VMEM((NC, 2, 128), f32),
            dma((12,)),
            dma((2,)), dma((groups + 1,)),
            dma((2,)), dma((2, groups)),
            dma((NZ,)), dma((NZ, groups)),
            dma((NY,)), dma((NY, groups)),
            dma((NY,)), dma((NY,)),
            dma((NZ, NY, NX, 2)),
            dma((NZ,)),
            dma((NZ,)),
            dma((NX, NY)),
            pltpu.SemaphoreType.REGULAR((2,)),
            dma((NX, NY)),
            dma((NY, NX)),
            dma((1,)), dma((NC,)),
            dma((2,)), dma((2,)),
            dma((1,)), dma((NC,)),
        ],
        compiler_params=pltpu.CompilerParams(
            collective_id=0, has_side_effects=True, vmem_limit_bytes=60 * 1024 * 1024
        ),
        name="packed_loglik",
    )(
        query_vectors, key_vectors, value_vectors, out_weight, residual, post_gain, final_gain, voc,
        segment_ids, doc_starts, doc_index, targets,
    )
    sums = jax.ShapeDtypeStruct((1, docs), f32)
    logprob, like, counts = pl.pallas_call(
        split, out_shape=(jax.ShapeDtypeStruct((1, rows), f32), sums, sums), name="split"
    )(packed)
    return (logprob, like[0], counts[0])


def solution(mesh):
    in_specs = (
        P(("dp", "seq"), "tensor"),
        P(("dp", "seq"), "tensor"),
        P(("dp", "seq"), "tensor"),
        P(None, "tensor"),
        P(("dp", "seq"), "tensor"),
        P("tensor"),
        P("tensor"),
        P(("dp", "seq", "tensor"), None),
        P("dp", "seq"),
        P("dp", None),
        P("dp", None),
        P(),
    )
    out_specs = (P("dp", "seq"), P(), P())
    return jax.shard_map(
        functools.partial(local, mesh), mesh=mesh, in_specs=in_specs, out_specs=out_specs, check_vma=False
    )
```

```python
import functools

import jax
import jax.numpy as jnp
from jax import lax
from jax.experimental import pallas as pl
from jax.experimental.pallas import tpu as pltpu
from jax.sharding import PartitionSpec as P

HEAD_DIM = 256
ATTENTION_CAP = 50.0
LOGIT_CAP = 30.0
EPSILON = 1e-06
MESH = pl.DeviceIdType.MESH
PAD = 64
NT = (((1,), (1,)), ((), ()))
NN = (((1,), (0,)), ((), ()))


def dot(a, b, dims):
    return lax.dot_general(a, b, dims, preferred_element_type=jnp.float32)


def body(
    sizes,
    q_hbm, k_hbm, v_hbm, w_hbm, res_hbm, pg_hbm, fg_hbm, voc_hbm, seg_hbm, start_hbm, index_hbm, target_hbm,
    out_ref,
    q_ref, top_first, over, under_sum, res_ref, pg_ref, fg_ref, seg_ref, start_ref, index_ref, target_ref,
    w_ref, voc_ref, kv, num, den, att, branch, stat, hid, held, lab_ref, early_buf, late_buf, twin_buf,
    local_sem, q_send, q_recv, o_send, o_recv, kv_send, kv_recv, att_send, att_recv, st_send, st_recv,
    hid_recv, z_send, d_send, u_send, token, y_send, x_send, voc_send, voc_recv, f_send, f_recv, tw_send, tw_recv,
):
    ND, NZ, NY, docs = sizes
    NC = 2 if ND % 2 == 0 else 1
    NX = ND // NC
    D = voc_hbm.shape[-1] if voc_hbm.ndim == 2 else voc_hbm.shape[0] * voc_hbm.shape[2]
    me_d, me_z, me_t = lax.axis_index("dp"), lax.axis_index("seq"), lax.axis_index("tensor")
    me_x, me_c = me_d // NC, me_d % NC
    twin = [me_x * NC + 1 - me_c] if NC == 2 else []
    rows = q_hbm.shape[0]
    kvw = k_hbm.shape[1]
    groups = kvw // HEAD_DIM
    per = q_hbm.shape[1] // kvw
    heads = groups * per
    qw = q_hbm.shape[1]
    fw = w_hbm.shape[1]

    pairs = [
        (k_hbm, kv.at[me_z, 0]), (v_hbm, kv.at[me_z, 1]), (q_hbm, q_ref.at[0]), (seg_hbm, seg_ref.at[0]), (start_hbm, start_ref),
        (index_hbm, index_ref), (target_hbm, target_ref), (res_hbm, res_ref), (pg_hbm, pg_ref), (fg_hbm, fg_ref),
        (w_hbm, w_ref), (voc_hbm, voc_ref.at[me_c]),
    ]
    loads = [pltpu.make_async_copy(src, dst, local_sem.at[i]) for i, (src, dst) in enumerate(pairs)]
    for c in loads:
        c.start()
    w_copy = loads[10]

    def dev(d=None, z=None, t=None):
        return (me_d if d is None else d, me_z if z is None else z, me_t if t is None else t)

    def remote(src, dst, send, recv, device):
        return pltpu.make_async_remote_copy(
            src_ref=src, dst_ref=dst, send_sem=send, recv_sem=recv, device_id=device, device_id_type=MESH
        )

    def others(me, n):
        return [jnp.where(me + i >= n, me + i - n, me + i) for i in range(1, n)]

    barrier = pltpu.get_barrier_semaphore()
    peers = [dev(d=p * NC + me_c) for p in others(me_x, NX)] + [dev(d=p) for p in twin]
    peers += [dev(t=p) for p in others(me_t, NY)]
    ups = [(me_z + 1 < NZ, dev(z=lax.rem(me_z + 1, NZ))), (me_z >= 1, dev(z=lax.rem(me_z + NZ - 1, NZ)))]
    for p in peers:
        pl.semaphore_signal(barrier, inc=1, device_id=p, device_id_type=MESH)
    for there, p in ups:
        @pl.when(there)
        def _(p=p):
            pl.semaphore_signal(barrier, inc=1, device_id=p, device_id_type=MESH)
    for c in loads[:2]:
        c.wait()

    def kv_copy(block, g):
        ref = kv.at[block, :, :, pl.ds(g * HEAD_DIM, HEAD_DIM)]
        return remote(ref, ref, kv_send.at[block], kv_recv.at[block, g], dev(z=lax.rem(me_z + 1, NZ)))

    def kv_sent(block):
        remote(kv.at[block], kv.at[block], kv_send.at[block], kv_recv.at[block, 0], dev()).wait_send()

    ends = lax.div(me_z + NZ - 1, NZ) + lax.div(2 * NZ - 2 - me_z, NZ)
    pl.semaphore_wait(barrier, len(peers) + ends)
    @pl.when(me_z < NZ - 2)
    def _():
        for g in range(groups):
            kv_copy(me_z, g).start()
    voc_copies = [
        remote(voc_hbm, voc_ref.at[me_c], voc_send.at[0], voc_recv.at[me_c], dev(d=p)) for p in twin
    ]
    for c in voc_copies:
        c.start()
    for c in loads[2:7]:
        c.wait()
    def first_of(seg):
        out = jnp.zeros((1, rows), jnp.int32)
        for n in range(start_ref.shape[1]):
            out = jnp.where(seg == n, start_ref[0, n], out)
        return out

    seg = seg_ref[0]
    first_row = jnp.zeros((1, rows), jnp.int32)
    end_row = jnp.zeros((1, rows), jnp.int32)
    doc_row = jnp.zeros((1, rows), jnp.int32)
    segs = start_ref.shape[1]
    for n in range(segs):
        here = seg == n
        first_row = jnp.where(here, start_ref[0, n], first_row)
        end_row = jnp.where(here, start_ref[0, n + 1] if n + 1 < segs else rows * NZ, end_row)
        doc_row = jnp.where(here, index_ref[0, n], doc_row)
    spot = me_z * rows + lax.broadcasted_iota(jnp.int32, (1, rows), 1)
    code_row = doc_row + jnp.where(spot + 1 < end_row, docs, 0)
    i_pos = lax.broadcasted_iota(jnp.int32, (rows, rows), 0)
    j_pos = lax.broadcasted_iota(jnp.int32, (rows, rows), 1)

    def column_of(row):
        full = jnp.broadcast_to(row.astype(jnp.float32), (rows, rows))
        return jnp.sum(jnp.where(i_pos == j_pos, full, 0.0), axis=1, keepdims=True)

    first = column_of(first_row).astype(jnp.int32)
    top, bottom, helper = me_z == NZ - 1, me_z == 0, me_z == NZ - 2
    gw = per * HEAD_DIM

    def query_copy(g):
        cols = pl.ds(g * gw, gw)
        return remote(
            q_ref.at[0, :, cols], q_ref.at[1, :, cols], q_send.at[0], q_recv.at[g], dev(z=lax.rem(me_z + NZ - 1, NZ))
        )

    def segment_copy():
        return remote(seg_ref.at[0], seg_ref.at[1], q_send.at[1], q_recv.at[groups], dev(z=lax.rem(me_z + NZ - 1, NZ)))

    def part_copies(g):
        cols = pl.ds(g * gw, gw)
        above = dev(z=lax.rem(me_z + 1, NZ))
        return [
            remote(over.at[:, cols], over.at[:, cols], o_send.at[0], o_recv.at[0, g], above),
            remote(under_sum.at[g], under_sum.at[g], o_send.at[1], o_recv.at[1, g], above),
        ]

    if NZ > 1:
        @pl.when(top)
        def _():
            segment_copy().start()
            for g in range(groups):
                query_copy(g).start()

    lines = NX * PAD
    lanes = lax.broadcasted_iota(jnp.int32, (rows, lines), 1)
    sub = lax.broadcasted_iota(jnp.int32, (rows, lines), 0)
    placed = jnp.where(lanes == sub + me_x * PAD, column_of(code_row), 0.0)
    code_line = jnp.sum(placed, axis=0, keepdims=True) * jnp.where(me_t == 0, 1.0, 0.0)
    gap = jnp.zeros((1, PAD - rows), jnp.int32)
    for z in range(NZ):
        pieces = []
        for x in range(NX):
            part = target_ref[x * NC:x * NC + 1, z * rows:(z + 1) * rows]
            for c in range(1, NC):
                part = jnp.where(me_c == c, target_ref[x * NC + c:x * NC + c + 1, z * rows:(z + 1) * rows], part)
            pieces += [part, gap]
        lab_ref[z] = jnp.concatenate(pieces, axis=1)

    def attend(g, *jobs):
        cols = slice(g * HEAD_DIM, (g + 1) * HEAD_DIM)
        span = range(g * per, (g + 1) * per)
        raws, parts = [], {}
        for who, block in jobs:
            kk = kv[me_z if block is None else block, 0, :, cols]
            for h in span:
                raws.append(dot(q_ref[who, :, h * HEAD_DIM:(h + 1) * HEAD_DIM], kk, NT))
        wts = []
        for i, raw in enumerate(raws):
            who, block = jobs[i // per]
            if block is None:
                seen = (me_z * rows + j_pos >= first) & (j_pos <= i_pos)
            else:
                seen = block * rows + j_pos >= (first if who == 0 else top_first[:, :1])
            capped = ATTENTION_CAP * jnp.tanh(raw * (HEAD_DIM ** (-0.5) / ATTENTION_CAP))
            wts.append(jnp.where(seen, jnp.exp(capped), 0.0))
        for i, wt in enumerate(wts):
            who, block = jobs[i // per]
            vv = kv[me_z if block is None else block, 1, :, cols]
            up = dot(wt.astype(jnp.bfloat16), vv, NN)
            low = jnp.broadcast_to(jnp.sum(wt, axis=1, keepdims=True), (rows, 128))
            at = who * heads + span[i % per]
            if at in parts:
                parts[at] = (parts[at][0] + up, parts[at][1] + low)
            elif who == 0 and block is not None:
                parts[at] = (num[at] + up, den[at] + low)
            else:
                parts[at] = (up, low)
        for at, (up, low) in parts.items():
            num[at] = up
            den[at] = low

    def arrived(block, g):
        kv_copy(block, g).wait_recv()

        @pl.when(me_z < NZ - 2)
        def _():
            kv_copy(block, g).start()

    @pl.when(me_z >= 0)
    def _():
        for g in range(groups):
            attend(g, (0, None))

    under = jnp.logical_not(top) if NZ > 2 else me_z >= 0

    def tell(i, z):
        pl.semaphore_signal(token.at[i], inc=1, device_id=dev(z=lax.rem(z + NZ, NZ)), device_id_type=MESH)

    if NZ > 1:
        @pl.when(bottom)
        def _():
            tell(0, me_z + 1)

        @pl.when(top)
        def _():
            tell(1, me_z - 1)

        @pl.when(jnp.logical_not(bottom | top))
        def _():
            pl.semaphore_wait(token.at[1], 1)
            tell(1, me_z - 1)
            pl.semaphore_wait(token.at[0], 1)
            tell(0, me_z + 1)

    for block in range(NZ - 3, 0, -1):
        @pl.when((block < me_z) & jnp.logical_not(top))
        def _(block=block):
            for g in range(groups):
                arrived(block, g)
                attend(g, (0, block))

    if NZ > 1:
        @pl.when(helper)
        def _():
            segment_copy().wait_recv()
            top_first[...] = jnp.broadcast_to(column_of(first_of(seg_ref[1])).astype(jnp.int32), (rows, 128))
            under_sum[...] = jnp.zeros(under_sum.shape, jnp.float32)
    def att_copy(g, peer, idx):
        ref = att.at[me_t, :, pl.ds(g * gw, gw)]
        return remote(ref, ref, att_send.at[idx], att_recv.at[me_t, g], dev(t=peer))

    step = 256 if fw % 256 == 0 else fw

    def project(t, g, begin):
        base = pl.multiple_of(t * qw + g * gw, gw)
        left = att[t, :, g * gw:(g + 1) * gw]
        for n in range(fw // step):
            cols = slice(n * step, (n + 1) * step)
            got = dot(left, w_ref[pl.ds(base, gw), cols], NN)
            branch[:, cols] = got if begin else branch[:, cols] + got

    for g in range(groups):
        if NZ > 1:
            @pl.when((me_z > 0) & jnp.logical_not(top | helper))
            def _(g=g):
                arrived(0, g)
                attend(g, (0, 0))

            @pl.when(helper)
            def _(g=g):
                query_copy(g).wait_recv()
                if NZ > 2:
                    arrived(0, g)
                    attend(g, (0, 0), *[(1, block) for block in range(NZ - 1)])
                else:
                    attend(g, (1, 0))

            @pl.when(top)
            def _(g=g):
                for c in part_copies(g):
                    c.wait_recv()
                for h in range(g * per, (g + 1) * per):
                    num[h] = num[h] + over[:, h * HEAD_DIM:(h + 1) * HEAD_DIM].astype(jnp.float32)
                    r = h - g * per
                    den[h] = den[h] + jnp.broadcast_to(column_of(under_sum[g, r:r + 1, :rows]), (rows, 128))

        for h in range(g * per, (g + 1) * per):
            att[me_t, :, h * HEAD_DIM:(h + 1) * HEAD_DIM] = (num[h] / den[h][:, :1]).astype(jnp.bfloat16)
        for i, p in enumerate(others(me_t, NY)):
            att_copy(g, p, i).start()
        if NZ > 1:
            @pl.when(helper)
            def _(g=g):
                for h in range(g * per, (g + 1) * per):
                    over[:, h * HEAD_DIM:(h + 1) * HEAD_DIM] = num[heads + h].astype(jnp.bfloat16)
                    wide = jnp.broadcast_to(den[heads + h][:, :1], (rows, rows))
                    r = h - g * per
                    under_sum[g, r:r + 1, :rows] = jnp.sum(jnp.where(i_pos == j_pos, wide, 0.0), axis=0, keepdims=True)
                for c in part_copies(g):
                    c.start()

        if g == 0:
            w_copy.wait()
        project(me_t, g, g == 0)
    for g in range(groups):
        for p in others(me_t, NY):
            ref = att.at[p, :, pl.ds(g * gw, gw)]
            remote(ref, ref, att_send.at[0], att_recv.at[p, g], dev()).wait_recv()
            project(p, g, False)

    for c in loads[7:10]:
        c.wait()
    br = branch[...]
    carried = res_ref[...].astype(jnp.float32)
    gained = pg_ref[...].reshape(1, fw) * br
    lane = lax.broadcasted_iota(jnp.int32, (rows, 128), 1)
    packed = jnp.zeros((rows, 128), jnp.float32)
    for i, prod in enumerate((br * br, carried * carried, carried * gained, gained * gained)):
        packed = jnp.where(lane == i, jnp.sum(prod, axis=1, keepdims=True), packed)
    stat[me_t] = packed

    def stat_copy(peer, i):
        return remote(stat.at[me_t], stat.at[me_t], st_send.at[i], st_recv.at[me_t], dev(t=peer))

    for i, p in enumerate(others(me_t, NY)):
        stat_copy(p, i).start()
    for p in others(me_t, NY):
        remote(stat.at[p], stat.at[p], st_send.at[0], st_recv.at[p], dev()).wait_recv()
    total = stat[0]
    for t in range(1, NY):
        total = total + stat[t]
    sq_branch, sq_carried, cross, sq_gained = (total[:, i:i + 1] for i in range(4))
    inv_branch = 1.0 / jnp.sqrt(sq_branch / D + EPSILON)
    sq_total = sq_carried + 2.0 * inv_branch * cross + inv_branch * inv_branch * sq_gained
    inv_total = 1.0 / jnp.sqrt(sq_total / D + EPSILON)
    hid[me_z, me_t, me_x, :rows, :] = (
        fg_ref[...].reshape(1, fw) * (carried + gained * inv_branch) * inv_total
    ).astype(jnp.bfloat16)

    y_peers = others(me_t, NY)
    x_peers = others(me_x, NX)
    cut = min(rows, (rows // 2 + 7) // 8 * 8)
    spans = [(0, cut)] + ([(cut, rows - cut)] if cut < rows else [])
    K = len(spans)

    def xdev(x):
        return dev(d=x * NC + me_c)

    def block(z, t, x, k):
        return hid.at[z, t, x, pl.ds(*spans[k]), :]

    def send(z, t, x, k, sem, device):
        return remote(block(z, t, x, k), block(z, t, x, k), sem, hid_recv.at[z, t, x, k], device)

    def landed(z, t, x, k):
        send(z, t, x, k, z_send.at[0], dev()).wait_recv()

    def step_of(n):
        if n == 0:
            return me_z
        out = jnp.where(n <= me_z, me_z - n, n)
        return jnp.where(top, 0 if n == 1 else me_z - n + 1, out) if NZ > 2 else out

    def climbs(z):
        up = jnp.logical_not(top) & (z <= me_z)
        return up & jnp.logical_not(helper & (z == 0)) if NZ > 2 else up

    def falls(z):
        return (me_z > 0) & (z > me_z) & (z < NZ - 1)

    def spread(n, act, wait):
        z = step_of(n)
        for k in range(K):
            if wait and n > 0:
                landed(z, me_t, me_x, k)
            for i, p in enumerate(x_peers):
                act(send(z, me_t, me_x, k, x_send.at[0, i], xdev(p)))
            for i, p in enumerate(y_peers):
                act(send(z, me_t, me_x, k, y_send.at[0, i], dev(t=p)))

            if n > 0:
                @pl.when(falls(z))
                def _(k=k):
                    act(send(z, me_t, me_x, k, d_send.at[z], dev(z=lax.rem(me_z + NZ - 1, NZ))))

            @pl.when(climbs(z))
            def _(k=k):
                act(send(z, me_t, me_x, k, z_send.at[z], dev(z=lax.rem(me_z + 1, NZ))))
        if n == 0 and NZ > 2:
            @pl.when(bottom)
            def _():
                for k in range(K):
                    act(send(me_z, me_t, me_x, k, z_send.at[NZ - 1], dev(z=NZ - 1)))
        if n == 0:
            for off in range(1, NZ):
                @pl.when((off <= me_z) & (top | (off == 1)))
                def _(off=off):
                    for k in range(K):
                        p = lax.rem(me_z + NZ - off, NZ)
                        act(send(me_z, me_t, me_x, k, d_send.at[off - 1], dev(z=p)))

    def lift(act):
        for j, x in enumerate(x_peers):
            for i, t in enumerate(y_peers):
                for k in range(K):
                    act(send(me_z, t, x, k, u_send.at[j, i], dev(z=NZ - 1)))

    def relay(n, act, wait):
        z = step_of(n)
        for j, x in enumerate(x_peers):
            if wait:
                landed(z, me_t, x, 0)
            for i, p in enumerate(y_peers):
                act(send(z, me_t, x, 0, y_send.at[1 + j, i], dev(t=p)))
        for j, t in enumerate(y_peers):
            if wait:
                landed(z, t, me_x, K - 1)
            if K > 1:
                for i, p in enumerate(x_peers):
                    act(send(z, t, me_x, K - 1, x_send.at[1 + j, i], xdev(p)))

    def start(c):
        c.start()

    count = voc_hbm.shape[-2]
    home = (me_x * NZ + me_z) * NY + me_t
    row_ids = lax.broadcasted_iota(jnp.int32, (count, lines), 0)

    def product(c, z, t):
        right = hid[z, t].reshape(lines, fw)
        if len(voc_ref.shape) == 3:
            start_col = t * fw if isinstance(t, int) else pl.multiple_of(t * fw, 128)
            left = voc_ref[c, :, pl.ds(start_col, fw)]
        else:
            left = voc_ref[c, t]
        return dot(left, right, NT)

    def gather(n, z, t, begin):
        @pl.loop(0, NC)
        def _(c):
            got = product(c, z, t)
            held[n, c] = got if begin else held[n, c] + got

    def finish(n, z, t, begin):
        label = lab_ref[z]

        def part(c, sums):
            acc = product(c, z, t)
            if not begin:
                acc = held[n, c] + acc
            capped = LOGIT_CAP * jnp.tanh(acc * (1.0 / LOGIT_CAP))
            base = (((me_x * NC + c) * NZ + me_z) * NY + me_t) * count
            tot = sums[0] + jnp.sum(jnp.exp(capped), axis=0, keepdims=True)
            cho = sums[1] + jnp.sum(jnp.where(row_ids == label - base, capped, 0.0), axis=0, keepdims=True)
            return tot, cho

        zero = jnp.zeros((1, lines), jnp.float32)
        return lax.fori_loop(0, NC, part, (zero, zero))

    def begin_slice(n):
        z = step_of(n)
        for x in x_peers:
            for k in range(1, K):
                landed(z, me_t, x, k)
        if n > 0 and NZ > 2:
            @pl.when(top)
            def _():
                for x in x_peers:
                    landed(z, me_t, x, 0)
        if n == 0:
            voc_ready()
        if NY > 1:
            gather(n, z, me_t, True)

    def end_slice(n, before_last=None):
        z = step_of(n)
        if n > 0 and NZ > 2:
            @pl.when(top)
            def _():
                for t in y_peers:
                    landed(z, t, me_x, K - 1)
        last = me_t
        for i, t in enumerate(y_peers):
            for k in range(K - 1):
                landed(z, t, me_x, k)
            for x in x_peers:
                for k in range(K):
                    landed(z, t, x, k)
            last = t
            if i + 1 < len(y_peers):
                gather(n, z, t, False)
        if before_last is not None:
            before_last()
        return z, *finish(n, z, last, NY == 1)

    family = [(x, z, t) for x in range(NX) for z in range(NZ) for t in range(NY)]
    G = len(family)

    def wrap(v, n):
        return jnp.where(v >= n, v - n, v)

    def kin_of(i):
        return wrap(me_x + i // (NZ * NY), NX), wrap(me_z + i // NY % NZ, NZ), wrap(me_t + i % NY, NY)

    def kin(i):
        x, z, t = kin_of(i)
        return dev(d=x * NC + me_c, z=z, t=t)

    def early(i):
        return remote(early_buf.at[home], early_buf.at[home], f_send.at[0], f_recv.at[0], kin(i))

    def late(i):
        return remote(late_buf.at[home], late_buf.at[home], f_send.at[1], f_recv.at[1], kin(i))

    def send_early():
        for i in range(1, G):
            early(i).start()

    def voc_ready():
        loads[11].wait()
        for p in twin:
            other = lax.rem(p, NC)
            remote(voc_hbm, voc_ref.at[other], voc_send.at[0], voc_recv.at[other], dev()).wait_recv()

    def score(n):
        if n + 1 < NZ:
            z, tot, cho = end_slice(n)
            early_buf[home, pl.ds(z, 1), :] = tot
            early_buf[home, pl.ds(NZ + z, 1), :] = cho
        else:
            early_buf[home, pl.ds(step_of(n), 1), :] = code_line
            early_buf[home, pl.ds(NZ + step_of(n), 1), :] = jnp.zeros((1, lines), jnp.float32)
            z, tot, cho = end_slice(n, send_early)
            late_buf[home, 0:1, :] = tot
            late_buf[home, 1:2, :] = cho

    if NZ > 1:
        @pl.when(top)
        def _():
            pl.semaphore_wait(token.at[0], 1)

        @pl.when(bottom)
        def _():
            pl.semaphore_wait(token.at[1], 1)

    spread(0, start, True)

    @pl.when(bottom)
    def _():
        relay(0, start, True)

    if NZ > 1:
        spread(1, start, True)

        @pl.when(jnp.logical_not(bottom))
        def _():
            relay(0, start, True)

    for n in range(2, NZ):
        @pl.when(n <= me_z)
        def _(n=n):
            spread(n, start, True)

    for n in range(2, NZ):
        @pl.when((n == me_z + 1) & jnp.logical_not(bottom | helper))
        def _(n=n):
            spread(n, start, True)

    if NZ > 1:
        @pl.when(under)
        def _():
            relay(1, start, True)

    if NZ > 2:
        @pl.when(helper)
        def _():
            spread(NZ - 1, start, True)

    for n in range(2, NZ):
        @pl.when((n > me_z + 1) | ((n > me_z) & bottom & jnp.logical_not(helper)))
        def _(n=n):
            spread(n, start, True)

        if n == 2:
            begin_slice(0)
        else:
            begin_slice(n - 1)
        score(n - 2)
        if n == 2 and NZ > 3:
            begin_slice(1)

        @pl.when(under)
        def _(n=n):
            if n == 2:
                pl.when(helper)(lambda: lift(start))
            relay(n, start, True)
            if n == 2:
                pl.when(jnp.logical_not(helper))(lambda: lift(start))

    if NZ < 3:
        begin_slice(0)
    if NZ == 3:
        begin_slice(1)
    if NZ > 1:
        begin_slice(NZ - 1)
        score(NZ - 2)
    score(NZ - 1)
    for i in range(1, G):
        late(i).start()
    def others_of(buf, k):
        ref = buf.at[pl.ds(0, G - 1)]
        return remote(ref, ref, f_send.at[k], f_recv.at[k], dev())

    if G > 1:
        others_of(early_buf, 0).wait_recv()

    def last_of(z):
        return NZ - 1 if z < NZ - 1 else min(1, max(NZ - 2, 0))

    def summed(buf, z):
        out = None
        for x in range(NX):
            for t in range(NY):
                part = buf[(x * NZ + z) * NY + t]
                out = part if out is None else out + part
        return out

    empty = jnp.zeros((1, lines), jnp.float32)
    totals, chosen, codes = [empty] * NZ, [empty] * NZ, [empty] * NZ
    for z in range(NZ):
        sums = summed(early_buf, z)
        for w in range(NZ):
            if w == last_of(z):
                codes[z] = sums[w:w + 1]
            else:
                totals[w] = totals[w] + sums[w:w + 1]
                chosen[w] = chosen[w] + sums[NZ + w:NZ + w + 1]
    if G > 1:
        others_of(late_buf, 1).wait_recv()
    for z in range(NZ):
        sums = summed(late_buf, z)
        totals[last_of(z)] = totals[last_of(z)] + sums[0:1]
        chosen[last_of(z)] = chosen[last_of(z)] + sums[1:2]
    totals, chosen, code = (jnp.concatenate(p, axis=0) for p in (totals, chosen, codes))
    inside = lax.rem(lax.broadcasted_iota(jnp.int32, (NZ, lines), 1), PAD) < rows
    counted = jnp.where(inside & (code >= docs), 1.0, 0.0)
    doc = jnp.where(code >= docs, code - docs, code)
    logprob = jnp.where(inside, counted * (chosen - jnp.log(totals)), 0.0)
    names = lax.broadcasted_iota(jnp.int32, (docs, lines), 0).astype(jnp.float32)
    like = jnp.zeros((docs, lines), jnp.float32)
    cnt = jnp.zeros((docs, lines), jnp.float32)
    for r in range(NZ):
        hit = names == doc[r:r + 1, :]
        like = like + jnp.where(hit, logprob[r:r + 1, :], 0.0)
        cnt = cnt + jnp.where(hit, counted[r:r + 1, :], 0.0)
    docs_eye = lax.broadcasted_iota(jnp.int32, (docs, 128), 0) == lax.broadcasted_iota(jnp.int32, (docs, 128), 1)
    sums = [
        jnp.sum(jnp.where(docs_eye, jnp.sum(v, axis=1, keepdims=True), 0.0), axis=0, keepdims=True)
        for v in (like, cnt)
    ]
    twin_buf[me_c, 0:1, :] = sums[0]
    twin_buf[me_c, 1:2, :] = sums[1]
    twin_copies = [
        remote(twin_buf.at[me_c], twin_buf.at[me_c], tw_send.at[0], tw_recv.at[me_c], dev(d=p)) for p in twin
    ]
    for c in twin_copies:
        c.start()
    mine = jnp.zeros((1, rows), jnp.float32)
    for z in range(NZ):
        for x in range(NX):
            mine = jnp.where((me_z == z) & (me_x == x), logprob[z:z + 1, x * PAD:x * PAD + rows], mine)
    out_ref[0:1, :rows] = mine
    for i, p in enumerate(others(me_t, NY)):
        remote(att.at[me_t], att.at[me_t], att_send.at[i], att_recv.at[me_t, 0], dev()).wait_send()
        stat_copy(p, i).wait_send()

    def sent(ref, sem):
        remote(ref, ref, sem, hid_recv.at[0, 0, 0, 0], dev()).wait_send()

    def portion(k, n):
        return hid.at[pl.ds(0, n), 0, 0, pl.ds(*k), :]

    whole = (0, rows)
    for i in range(len(x_peers)):
        sent(portion(whole, NZ), x_send.at[0, i])
    for i in range(len(y_peers)):
        sent(portion(whole, NZ), y_send.at[0, i])

    def relays_sent(n):
        for j in range(len(x_peers)):
            for i in range(len(y_peers)):
                sent(portion(spans[0], n), y_send.at[1 + j, i])
        for j in range(len(y_peers)):
            if K > 1:
                for i in range(len(x_peers)):
                    sent(portion(spans[K - 1], n), x_send.at[1 + j, i])

    @pl.when(under)
    def _():
        relays_sent(NZ)
        if NZ > 2:
            for j in range(len(x_peers)):
                for i in range(len(y_peers)):
                    sent(portion(whole, 1), u_send.at[j, i])

    if NZ > 2:
        @pl.when(bottom)
        def _():
            sent(portion(whole, 1), z_send.at[NZ - 1])

        @pl.when(top)
        def _():
            relays_sent(1)

    for z in range(NZ - 1):
        @pl.when(climbs(z))
        def _(z=z):
            sent(portion(whole, 1), z_send.at[z])

        @pl.when(((z < me_z) & (top | (z == 0))) | falls(z))
        def _(z=z):
            sent(portion(whole, 1), d_send.at[z])
    if NZ > 1:
        @pl.when(top)
        def _():
            segment_copy().wait_send()
            remote(q_ref.at[0], q_ref.at[1], q_send.at[0], q_recv.at[0], dev()).wait_send()

        @pl.when(helper)
        def _():
            remote(over, over, o_send.at[0], o_recv.at[0, 0], dev()).wait_send()
            remote(under_sum, under_sum, o_send.at[1], o_recv.at[1, 0], dev()).wait_send()

    for block in range(NZ - 2):
        @pl.when((me_z >= block) & (me_z < NZ - 2))
        def _(block=block):
            kv_sent(block)
    if G > 1:
        others_of(early_buf, 0).wait_send()
        others_of(late_buf, 1).wait_send()
    for c in voc_copies:
        c.wait_send()
    for p in twin:
        other = lax.rem(p, NC)
        remote(twin_buf.at[other], twin_buf.at[other], tw_send.at[0], tw_recv.at[other], dev()).wait_recv()
    for c in twin_copies:
        c.wait_send()
    both = twin_buf[0]
    for c in range(1, NC):
        both = both + twin_buf[c]
    out_ref[1:3, :] = both


def split(packed, lp_ref, like_ref, cnt_ref):
    lp_ref[...] = packed[0:1, :lp_ref.shape[1]]
    like_ref[...] = packed[1:2, :like_ref.shape[1]]
    cnt_ref[...] = packed[2:3, :cnt_ref.shape[1]]


def local(
    mesh, query_vectors, key_vectors, value_vectors, out_weight, residual, post_gain, final_gain,
    vocab_weight, segment_ids, doc_starts, doc_index, targets,
):
    ND, NZ, NY = mesh.shape["dp"], mesh.shape["seq"], mesh.shape["tensor"]
    rows = query_vectors.shape[0]
    docs = doc_starts.shape[1] * ND
    blocks = ND * NZ
    fw = out_weight.shape[1]
    voc = vocab_weight
    if fw % 128 != 0:
        voc = voc.reshape(voc.shape[0], NY, fw).transpose(1, 0, 2)
    kvw, qw = key_vectors.shape[1], query_vectors.shape[1]
    heads = qw // HEAD_DIM
    groups = kvw // HEAD_DIM
    NC = 2 if ND % 2 == 0 else 1
    NX = ND // NC
    R = blocks * PAD // 128
    f32, bf16, i32 = jnp.float32, jnp.bfloat16, jnp.int32
    dma = pltpu.SemaphoreType.DMA
    lines = NX * PAD
    G = NX * NZ * NY
    anyspace = pl.BlockSpec(memory_space=pl.ANY)
    packed = pl.pallas_call(
        functools.partial(body, (ND, NZ, NY, docs)),
        out_shape=jax.ShapeDtypeStruct((8, 128), f32),
        in_specs=[anyspace] * 12,
        out_specs=pl.BlockSpec(memory_space=pltpu.VMEM),
        scratch_shapes=[
            pltpu.VMEM((2, *query_vectors.shape), bf16),
            pltpu.VMEM((rows, 128), i32),
            pltpu.VMEM(query_vectors.shape, bf16),
            pltpu.VMEM((groups, 8, 128), f32),
            pltpu.VMEM(residual.shape, bf16),
            pltpu.VMEM(post_gain.shape, f32),
            pltpu.VMEM(final_gain.shape, f32),
            pltpu.VMEM((2, *segment_ids.shape), i32),
            pltpu.SMEM(doc_starts.shape, i32),
            pltpu.SMEM(doc_index.shape, i32),
            pltpu.VMEM(targets.shape, i32),
            pltpu.VMEM(out_weight.shape, bf16),
            pltpu.VMEM((NC, *voc.shape), bf16),
            pltpu.VMEM((NZ, 2, rows, kvw), bf16),
            pltpu.VMEM((2 * heads, rows, HEAD_DIM), f32),
            pltpu.VMEM((2 * heads, rows, 128), f32),
            pltpu.VMEM((NY, rows, qw), bf16),
            pltpu.VMEM((rows, fw), f32),
            pltpu.VMEM((NY, rows, 128), f32),
            pltpu.VMEM((NZ, NY, NX, PAD, fw), bf16),
            pltpu.VMEM((NZ, NC, voc.shape[-2], lines), f32),
            pltpu.VMEM((NZ, 1, lines), i32),
            pltpu.VMEM((G, 2 * NZ, lines), f32),
            pltpu.VMEM((G, 2, lines), f32),
            pltpu.VMEM((NC, 2, 128), f32),
            dma((12,)),
            dma((2,)), dma((groups + 1,)),
            dma((2,)), dma((2, groups)),
            dma((NZ,)), dma((NZ, groups)),
            dma((NY,)), dma((NY, groups)),
            dma((NY,)), dma((NY,)),
            dma((NZ, NY, NX, 2)),
            dma((NZ,)),
            dma((NZ,)),
            dma((NX, NY)),
            pltpu.SemaphoreType.REGULAR((2,)),
            dma((NX, NY)),
            dma((NY, NX)),
            dma((1,)), dma((NC,)),
            dma((2,)), dma((2,)),
            dma((1,)), dma((NC,)),
        ],
        compiler_params=pltpu.CompilerParams(
            collective_id=0, has_side_effects=True, vmem_limit_bytes=60 * 1024 * 1024
        ),
        name="packed_loglik",
    )(
        query_vectors, key_vectors, value_vectors, out_weight, residual, post_gain, final_gain, voc,
        segment_ids, doc_starts, doc_index, targets,
    )
    sums = jax.ShapeDtypeStruct((1, docs), f32)
    logprob, like, counts = pl.pallas_call(
        split, out_shape=(jax.ShapeDtypeStruct((1, rows), f32), sums, sums), name="split"
    )(packed)
    return (logprob, like[0], counts[0])


def solution(mesh):
    in_specs = (
        P(("dp", "seq"), "tensor"),
        P(("dp", "seq"), "tensor"),
        P(("dp", "seq"), "tensor"),
        P(None, "tensor"),
        P(("dp", "seq"), "tensor"),
        P("tensor"),
        P("tensor"),
        P(("dp", "seq", "tensor"), None),
        P("dp", "seq"),
        P("dp", None),
        P("dp", None),
        P(),
    )
    out_specs = (P("dp", "seq"), P(), P())
    return jax.shard_map(
        functools.partial(local, mesh), mesh=mesh, in_specs=in_specs, out_specs=out_specs, check_vma=False
    )
```

```python
import functools

import jax
import jax.numpy as jnp
from jax import lax
from jax.experimental import pallas as pl
from jax.experimental.pallas import tpu as pltpu
from jax.sharding import PartitionSpec as P

HEAD_DIM = 256
ATTENTION_CAP = 50.0
LOGIT_CAP = 30.0
EPSILON = 1e-06
MESH = pl.DeviceIdType.MESH
PAD = 64
NT = (((1,), (1,)), ((), ()))
NN = (((1,), (0,)), ((), ()))


def dot(a, b, dims):
    return lax.dot_general(a, b, dims, preferred_element_type=jnp.float32)


def body(
    sizes,
    q_hbm, k_hbm, v_hbm, w_hbm, res_hbm, pg_hbm, fg_hbm, voc_hbm, seg_hbm, start_hbm, index_hbm, target_hbm,
    out_ref,
    q_ref, top_first, over, under_sum, res_ref, pg_ref, fg_ref, seg_ref, start_ref, index_ref, target_ref,
    w_ref, voc_ref, kv, num, den, att, branch, stat, hid, held, lab_ref, early_buf, late_buf, twin_buf,
    local_sem, q_send, q_recv, o_send, o_recv, kv_send, kv_recv, att_send, att_recv, st_send, st_recv,
    hid_recv, z_send, d_send, u_send, token, y_send, x_send, voc_send, voc_recv, f_send, f_recv, tw_send, tw_recv,
):
    ND, NZ, NY, docs = sizes
    NC = 2 if ND % 2 == 0 else 1
    NX = ND // NC
    D = voc_hbm.shape[-1] if voc_hbm.ndim == 2 else voc_hbm.shape[0] * voc_hbm.shape[2]
    me_d, me_z, me_t = lax.axis_index("dp"), lax.axis_index("seq"), lax.axis_index("tensor")
    me_x, me_c = me_d // NC, me_d % NC
    twin = [me_x * NC + 1 - me_c] if NC == 2 else []
    rows = q_hbm.shape[0]
    kvw = k_hbm.shape[1]
    groups = kvw // HEAD_DIM
    per = q_hbm.shape[1] // kvw
    heads = groups * per
    qw = q_hbm.shape[1]
    fw = w_hbm.shape[1]

    pairs = [
        (k_hbm, kv.at[me_z, 0]), (v_hbm, kv.at[me_z, 1]), (q_hbm, q_ref.at[0]), (seg_hbm, seg_ref.at[0]), (start_hbm, start_ref),
        (index_hbm, index_ref), (target_hbm, target_ref), (res_hbm, res_ref), (pg_hbm, pg_ref), (fg_hbm, fg_ref),
        (w_hbm, w_ref), (voc_hbm, voc_ref.at[me_c]),
    ]
    loads = [pltpu.make_async_copy(src, dst, local_sem.at[i]) for i, (src, dst) in enumerate(pairs)]
    for c in loads:
        c.start()
    w_copy = loads[10]

    def dev(d=None, z=None, t=None):
        return (me_d if d is None else d, me_z if z is None else z, me_t if t is None else t)

    def remote(src, dst, send, recv, device):
        return pltpu.make_async_remote_copy(
            src_ref=src, dst_ref=dst, send_sem=send, recv_sem=recv, device_id=device, device_id_type=MESH
        )

    def others(me, n):
        return [jnp.where(me + i >= n, me + i - n, me + i) for i in range(1, n)]

    barrier = pltpu.get_barrier_semaphore()
    peers = [dev(d=p * NC + me_c) for p in others(me_x, NX)] + [dev(d=p) for p in twin]
    peers += [dev(t=p) for p in others(me_t, NY)]
    ups = [(me_z + 1 < NZ, dev(z=lax.rem(me_z + 1, NZ))), (me_z >= 1, dev(z=lax.rem(me_z + NZ - 1, NZ)))]
    for p in peers:
        pl.semaphore_signal(barrier, inc=1, device_id=p, device_id_type=MESH)
    for there, p in ups:
        @pl.when(there)
        def _(p=p):
            pl.semaphore_signal(barrier, inc=1, device_id=p, device_id_type=MESH)
    for c in loads[:2]:
        c.wait()

    def kv_copy(block, g):
        ref = kv.at[block, :, :, pl.ds(g * HEAD_DIM, HEAD_DIM)]
        return remote(ref, ref, kv_send.at[block], kv_recv.at[block, g], dev(z=lax.rem(me_z + 1, NZ)))

    def kv_sent(block):
        remote(kv.at[block], kv.at[block], kv_send.at[block], kv_recv.at[block, 0], dev()).wait_send()

    ends = lax.div(me_z + NZ - 1, NZ) + lax.div(2 * NZ - 2 - me_z, NZ)
    pl.semaphore_wait(barrier, len(peers) + ends)
    @pl.when(me_z < NZ - 2)
    def _():
        for g in range(groups):
            kv_copy(me_z, g).start()
    voc_copies = [
        remote(voc_hbm, voc_ref.at[me_c], voc_send.at[0], voc_recv.at[me_c], dev(d=p)) for p in twin
    ]
    for c in voc_copies:
        c.start()
    for c in loads[2:7]:
        c.wait()
    def first_of(seg):
        out = jnp.zeros((1, rows), jnp.int32)
        for n in range(start_ref.shape[1]):
            out = jnp.where(seg == n, start_ref[0, n], out)
        return out

    seg = seg_ref[0]
    first_row = jnp.zeros((1, rows), jnp.int32)
    end_row = jnp.zeros((1, rows), jnp.int32)
    doc_row = jnp.zeros((1, rows), jnp.int32)
    segs = start_ref.shape[1]
    for n in range(segs):
        here = seg == n
        first_row = jnp.where(here, start_ref[0, n], first_row)
        end_row = jnp.where(here, start_ref[0, n + 1] if n + 1 < segs else rows * NZ, end_row)
        doc_row = jnp.where(here, index_ref[0, n], doc_row)
    spot = me_z * rows + lax.broadcasted_iota(jnp.int32, (1, rows), 1)
    code_row = doc_row + jnp.where(spot + 1 < end_row, docs, 0)
    i_pos = lax.broadcasted_iota(jnp.int32, (rows, rows), 0)
    j_pos = lax.broadcasted_iota(jnp.int32, (rows, rows), 1)

    def column_of(row):
        full = jnp.broadcast_to(row.astype(jnp.float32), (rows, rows))
        return jnp.sum(jnp.where(i_pos == j_pos, full, 0.0), axis=1, keepdims=True)

    first = column_of(first_row).astype(jnp.int32)
    top, bottom, helper = me_z == NZ - 1, me_z == 0, me_z == NZ - 2
    gw = per * HEAD_DIM

    def query_copy(g):
        cols = pl.ds(g * gw, gw)
        return remote(
            q_ref.at[0, :, cols], q_ref.at[1, :, cols], q_send.at[0], q_recv.at[g], dev(z=lax.rem(me_z + NZ - 1, NZ))
        )

    def segment_copy():
        return remote(seg_ref.at[0], seg_ref.at[1], q_send.at[1], q_recv.at[groups], dev(z=lax.rem(me_z + NZ - 1, NZ)))

    def part_copies(g):
        cols = pl.ds(g * gw, gw)
        above = dev(z=lax.rem(me_z + 1, NZ))
        return [
            remote(over.at[:, cols], over.at[:, cols], o_send.at[0], o_recv.at[0, g], above),
            remote(under_sum.at[g], under_sum.at[g], o_send.at[1], o_recv.at[1, g], above),
        ]

    if NZ > 1:
        @pl.when(top)
        def _():
            segment_copy().start()
            for g in range(groups):
                query_copy(g).start()

    lines = NX * PAD
    lanes = lax.broadcasted_iota(jnp.int32, (rows, lines), 1)
    sub = lax.broadcasted_iota(jnp.int32, (rows, lines), 0)
    placed = jnp.where(lanes == sub + me_x * PAD, column_of(code_row), 0.0)
    code_line = jnp.sum(placed, axis=0, keepdims=True) * jnp.where(me_t == 0, 1.0, 0.0)
    gap = jnp.zeros((1, PAD - rows), jnp.int32)
    for z in range(NZ):
        pieces = []
        for x in range(NX):
            part = target_ref[x * NC:x * NC + 1, z * rows:(z + 1) * rows]
            for c in range(1, NC):
                part = jnp.where(me_c == c, target_ref[x * NC + c:x * NC + c + 1, z * rows:(z + 1) * rows], part)
            pieces += [part, gap]
        lab_ref[z] = jnp.concatenate(pieces, axis=1)

    def attend(g, *jobs):
        cols = slice(g * HEAD_DIM, (g + 1) * HEAD_DIM)
        span = range(g * per, (g + 1) * per)
        raws, parts = [], {}
        for who, block in jobs:
            kk = kv[me_z if block is None else block, 0, :, cols]
            for h in span:
                raws.append(dot(q_ref[who, :, h * HEAD_DIM:(h + 1) * HEAD_DIM], kk, NT))
        wts = []
        for i, raw in enumerate(raws):
            who, block = jobs[i // per]
            if block is None:
                seen = (me_z * rows + j_pos >= first) & (j_pos <= i_pos)
            else:
                seen = block * rows + j_pos >= (first if who == 0 else top_first[:, :1])
            capped = ATTENTION_CAP * jnp.tanh(raw * (HEAD_DIM ** (-0.5) / ATTENTION_CAP))
            wts.append(jnp.where(seen, jnp.exp(capped), 0.0))
        for i, wt in enumerate(wts):
            who, block = jobs[i // per]
            vv = kv[me_z if block is None else block, 1, :, cols]
            up = dot(wt.astype(jnp.bfloat16), vv, NN)
            low = jnp.broadcast_to(jnp.sum(wt, axis=1, keepdims=True), (rows, 128))
            at = who * heads + span[i % per]
            if at in parts:
                parts[at] = (parts[at][0] + up, parts[at][1] + low)
            elif who == 0 and block is not None:
                parts[at] = (num[at] + up, den[at] + low)
            else:
                parts[at] = (up, low)
        for at, (up, low) in parts.items():
            num[at] = up
            den[at] = low

    def arrived(block, g):
        kv_copy(block, g).wait_recv()

        @pl.when(me_z < NZ - 2)
        def _():
            kv_copy(block, g).start()

    @pl.when(me_z >= 0)
    def _():
        for g in range(groups):
            attend(g, (0, None))

    under = jnp.logical_not(top) if NZ > 2 else me_z >= 0

    def tell(i, z):
        pl.semaphore_signal(token.at[i], inc=1, device_id=dev(z=lax.rem(z + NZ, NZ)), device_id_type=MESH)

    if NZ > 1:
        @pl.when(bottom)
        def _():
            tell(0, me_z + 1)

        @pl.when(top)
        def _():
            tell(1, me_z - 1)

        @pl.when(jnp.logical_not(bottom | top))
        def _():
            pl.semaphore_wait(token.at[1], 1)
            tell(1, me_z - 1)
            pl.semaphore_wait(token.at[0], 1)
            tell(0, me_z + 1)

    for block in range(NZ - 3, 0, -1):
        @pl.when((block < me_z) & jnp.logical_not(top))
        def _(block=block):
            for g in range(groups):
                arrived(block, g)
                attend(g, (0, block))

    if NZ > 1:
        @pl.when(helper)
        def _():
            segment_copy().wait_recv()
            top_first[...] = jnp.broadcast_to(column_of(first_of(seg_ref[1])).astype(jnp.int32), (rows, 128))
            under_sum[...] = jnp.zeros(under_sum.shape, jnp.float32)
    def att_copy(g, peer, idx):
        ref = att.at[me_t, :, pl.ds(g * gw, gw)]
        return remote(ref, ref, att_send.at[idx], att_recv.at[me_t, g], dev(t=peer))

    step = 256 if fw % 256 == 0 else fw

    def project(t, g, begin):
        base = pl.multiple_of(t * qw + g * gw, gw)
        left = att[t, :, g * gw:(g + 1) * gw]
        for n in range(fw // step):
            cols = slice(n * step, (n + 1) * step)
            got = dot(left, w_ref[pl.ds(base, gw), cols], NN)
            branch[:, cols] = got if begin else branch[:, cols] + got

    for g in range(groups):
        if NZ > 1:
            @pl.when((me_z > 0) & jnp.logical_not(top | helper))
            def _(g=g):
                arrived(0, g)
                attend(g, (0, 0))

            @pl.when(helper)
            def _(g=g):
                query_copy(g).wait_recv()
                if NZ > 2:
                    arrived(0, g)
                    attend(g, (0, 0), *[(1, block) for block in range(NZ - 1)])
                else:
                    attend(g, (1, 0))

            @pl.when(top)
            def _(g=g):
                for c in part_copies(g):
                    c.wait_recv()
                for h in range(g * per, (g + 1) * per):
                    num[h] = num[h] + over[:, h * HEAD_DIM:(h + 1) * HEAD_DIM].astype(jnp.float32)
                    r = h - g * per
                    den[h] = den[h] + jnp.broadcast_to(column_of(under_sum[g, r:r + 1, :rows]), (rows, 128))

        for h in range(g * per, (g + 1) * per):
            att[me_t, :, h * HEAD_DIM:(h + 1) * HEAD_DIM] = (num[h] / den[h][:, :1]).astype(jnp.bfloat16)
        for i, p in enumerate(others(me_t, NY)):
            att_copy(g, p, i).start()
        if NZ > 1:
            @pl.when(helper)
            def _(g=g):
                for h in range(g * per, (g + 1) * per):
                    over[:, h * HEAD_DIM:(h + 1) * HEAD_DIM] = num[heads + h].astype(jnp.bfloat16)
                    wide = jnp.broadcast_to(den[heads + h][:, :1], (rows, rows))
                    r = h - g * per
                    under_sum[g, r:r + 1, :rows] = jnp.sum(jnp.where(i_pos == j_pos, wide, 0.0), axis=0, keepdims=True)
                for c in part_copies(g):
                    c.start()

        if g == 0:
            w_copy.wait()
        project(me_t, g, g == 0)
    for g in range(groups):
        for p in others(me_t, NY):
            ref = att.at[p, :, pl.ds(g * gw, gw)]
            remote(ref, ref, att_send.at[0], att_recv.at[p, g], dev()).wait_recv()
            project(p, g, False)

    for c in loads[7:10]:
        c.wait()
    br = branch[...]
    carried = res_ref[...].astype(jnp.float32)
    gained = pg_ref[...].reshape(1, fw) * br
    lane = lax.broadcasted_iota(jnp.int32, (rows, 128), 1)
    packed = jnp.zeros((rows, 128), jnp.float32)
    for i, prod in enumerate((br * br, carried * carried, carried * gained, gained * gained)):
        packed = jnp.where(lane == i, jnp.sum(prod, axis=1, keepdims=True), packed)
    stat[me_t] = packed

    def stat_copy(peer, i):
        return remote(stat.at[me_t], stat.at[me_t], st_send.at[i], st_recv.at[me_t], dev(t=peer))

    for i, p in enumerate(others(me_t, NY)):
        stat_copy(p, i).start()
    for p in others(me_t, NY):
        remote(stat.at[p], stat.at[p], st_send.at[0], st_recv.at[p], dev()).wait_recv()
    total = stat[0]
    for t in range(1, NY):
        total = total + stat[t]
    sq_branch, sq_carried, cross, sq_gained = (total[:, i:i + 1] for i in range(4))
    inv_branch = 1.0 / jnp.sqrt(sq_branch / D + EPSILON)
    sq_total = sq_carried + 2.0 * inv_branch * cross + inv_branch * inv_branch * sq_gained
    inv_total = 1.0 / jnp.sqrt(sq_total / D + EPSILON)
    hid[me_z, me_t, me_x, :rows, :] = (
        fg_ref[...].reshape(1, fw) * (carried + gained * inv_branch) * inv_total
    ).astype(jnp.bfloat16)

    y_peers = others(me_t, NY)
    x_peers = others(me_x, NX)
    cut = min(rows, (rows // 2 + 7) // 8 * 8)
    spans = [(0, cut)] + ([(cut, rows - cut)] if cut < rows else [])
    K = len(spans)

    def xdev(x):
        return dev(d=x * NC + me_c)

    def block(z, t, x, k):
        return hid.at[z, t, x, pl.ds(*spans[k]), :]

    def send(z, t, x, k, sem, device):
        return remote(block(z, t, x, k), block(z, t, x, k), sem, hid_recv.at[z, t, x, k], device)

    def landed(z, t, x, k):
        send(z, t, x, k, z_send.at[0], dev()).wait_recv()

    def step_of(n):
        if n == 0:
            return me_z
        out = jnp.where(n <= me_z, me_z - n, n)
        return jnp.where(top, 0 if n == 1 else me_z - n + 1, out) if NZ > 2 else out

    def climbs(z):
        up = jnp.logical_not(top) & (z <= me_z)
        return up & jnp.logical_not(helper & (z == 0)) if NZ > 2 else up

    def falls(z):
        return (me_z > 0) & (z > me_z) & (z < NZ - 1)

    def spread(n, act, wait):
        z = step_of(n)
        for k in range(K):
            if wait and n > 0:
                landed(z, me_t, me_x, k)
            for i, p in enumerate(x_peers):
                act(send(z, me_t, me_x, k, x_send.at[0, i], xdev(p)))
            for i, p in enumerate(y_peers):
                act(send(z, me_t, me_x, k, y_send.at[0, i], dev(t=p)))

            if n > 0:
                @pl.when(falls(z))
                def _(k=k):
                    act(send(z, me_t, me_x, k, d_send.at[z], dev(z=lax.rem(me_z + NZ - 1, NZ))))

            @pl.when(climbs(z))
            def _(k=k):
                act(send(z, me_t, me_x, k, z_send.at[z], dev(z=lax.rem(me_z + 1, NZ))))
        if n == 0 and NZ > 2:
            @pl.when(bottom)
            def _():
                for k in range(K):
                    act(send(me_z, me_t, me_x, k, z_send.at[NZ - 1], dev(z=NZ - 1)))
        if n == 0:
            for off in range(1, NZ):
                @pl.when((off <= me_z) & (top | (off == 1)))
                def _(off=off):
                    for k in range(K):
                        p = lax.rem(me_z + NZ - off, NZ)
                        act(send(me_z, me_t, me_x, k, d_send.at[off - 1], dev(z=p)))

    def lift(act):
        for j, x in enumerate(x_peers):
            for i, t in enumerate(y_peers):
                for k in range(K):
                    act(send(me_z, t, x, k, u_send.at[j, i], dev(z=NZ - 1)))

    def relay(n, act, wait):
        z = step_of(n)
        for j, x in enumerate(x_peers):
            if wait:
                landed(z, me_t, x, 0)
            for i, p in enumerate(y_peers):
                act(send(z, me_t, x, 0, y_send.at[1 + j, i], dev(t=p)))
        for j, t in enumerate(y_peers):
            if wait:
                landed(z, t, me_x, K - 1)
            if K > 1:
                for i, p in enumerate(x_peers):
                    act(send(z, t, me_x, K - 1, x_send.at[1 + j, i], xdev(p)))

    def start(c):
        c.start()

    count = voc_hbm.shape[-2]
    home = (me_x * NZ + me_z) * NY + me_t
    row_ids = lax.broadcasted_iota(jnp.int32, (count, lines), 0)

    def product(c, z, t):
        right = hid[z, t].reshape(lines, fw)
        if len(voc_ref.shape) == 3:
            start_col = t * fw if isinstance(t, int) else pl.multiple_of(t * fw, 128)
            left = voc_ref[c, :, pl.ds(start_col, fw)]
        else:
            left = voc_ref[c, t]
        return dot(left, right, NT)

    def gather(n, z, t, begin):
        @pl.loop(0, NC)
        def _(c):
            got = product(c, z, t)
            held[n, c] = got if begin else held[n, c] + got

    def finish(n, z, t, begin):
        label = lab_ref[z]

        def part(c, sums):
            acc = product(c, z, t)
            if not begin:
                acc = held[n, c] + acc
            capped = LOGIT_CAP * jnp.tanh(acc * (1.0 / LOGIT_CAP))
            base = (((me_x * NC + c) * NZ + me_z) * NY + me_t) * count
            tot = sums[0] + jnp.sum(jnp.exp(capped), axis=0, keepdims=True)
            cho = sums[1] + jnp.sum(jnp.where(row_ids == label - base, capped, 0.0), axis=0, keepdims=True)
            return tot, cho

        zero = jnp.zeros((1, lines), jnp.float32)
        return lax.fori_loop(0, NC, part, (zero, zero))

    def begin_slice(n):
        z = step_of(n)
        for x in x_peers:
            for k in range(1, K):
                landed(z, me_t, x, k)
        if n > 0 and NZ > 2:
            @pl.when(top)
            def _():
                for x in x_peers:
                    landed(z, me_t, x, 0)
        if n == 0:
            voc_ready()
        if NY > 1:
            gather(n, z, me_t, True)

    def end_slice(n, before_last=None):
        z = step_of(n)
        if n > 0 and NZ > 2:
            @pl.when(top)
            def _():
                for t in y_peers:
                    landed(z, t, me_x, K - 1)
        last = me_t
        for i, t in enumerate(y_peers):
            for k in range(K - 1):
                landed(z, t, me_x, k)
            for x in x_peers:
                for k in range(K):
                    landed(z, t, x, k)
            last = t
            if i + 1 < len(y_peers):
                gather(n, z, t, False)
        if before_last is not None:
            before_last()
        return z, *finish(n, z, last, NY == 1)

    family = [(x, z, t) for x in range(NX) for z in range(NZ) for t in range(NY)]
    G = len(family)

    def wrap(v, n):
        return jnp.where(v >= n, v - n, v)

    def kin_of(i):
        return wrap(me_x + i // (NZ * NY), NX), wrap(me_z + i // NY % NZ, NZ), wrap(me_t + i % NY, NY)

    def kin(i):
        x, z, t = kin_of(i)
        return dev(d=x * NC + me_c, z=z, t=t)

    def early(i):
        return remote(early_buf.at[home], early_buf.at[home], f_send.at[0], f_recv.at[0], kin(i))

    def late(i):
        return remote(late_buf.at[home], late_buf.at[home], f_send.at[1], f_recv.at[1], kin(i))

    def send_early():
        for i in range(1, G):
            early(i).start()

    def voc_ready():
        loads[11].wait()
        for p in twin:
            other = lax.rem(p, NC)
            remote(voc_hbm, voc_ref.at[other], voc_send.at[0], voc_recv.at[other], dev()).wait_recv()

    def score(n):
        if n + 1 < NZ:
            z, tot, cho = end_slice(n)
            early_buf[home, pl.ds(z, 1), :] = tot
            early_buf[home, pl.ds(NZ + z, 1), :] = cho
        else:
            early_buf[home, pl.ds(step_of(n), 1), :] = code_line
            early_buf[home, pl.ds(NZ + step_of(n), 1), :] = jnp.zeros((1, lines), jnp.float32)
            z, tot, cho = end_slice(n, send_early)
            late_buf[home, 0:1, :] = tot
            late_buf[home, 1:2, :] = cho

    if NZ > 1:
        @pl.when(top)
        def _():
            pl.semaphore_wait(token.at[0], 1)

        @pl.when(bottom)
        def _():
            pl.semaphore_wait(token.at[1], 1)

    spread(0, start, True)

    @pl.when(bottom | helper)
    def _():
        relay(0, start, True)

    if NZ > 1:
        spread(1, start, True)

        @pl.when(jnp.logical_not(bottom | helper))
        def _():
            relay(0, start, True)

    for n in range(2, NZ):
        @pl.when(n <= me_z)
        def _(n=n):
            spread(n, start, True)

    for n in range(2, NZ):
        @pl.when((n == me_z + 1) & jnp.logical_not(bottom | helper))
        def _(n=n):
            spread(n, start, True)

    if NZ > 1:
        @pl.when(under)
        def _():
            relay(1, start, True)

    if NZ > 2:
        @pl.when(helper)
        def _():
            spread(NZ - 1, start, True)

    for n in range(2, NZ):
        @pl.when((n > me_z + 1) | ((n > me_z) & bottom & jnp.logical_not(helper)))
        def _(n=n):
            spread(n, start, True)

        if n == 2:
            begin_slice(0)
        else:
            begin_slice(n - 1)
        score(n - 2)
        if n == 2 and NZ > 3:
            begin_slice(1)

        @pl.when(under)
        def _(n=n):
            if n == 2:
                pl.when(helper)(lambda: lift(start))
            relay(n, start, True)
            if n == 2:
                pl.when(jnp.logical_not(helper))(lambda: lift(start))

    if NZ < 3:
        begin_slice(0)
    if NZ == 3:
        begin_slice(1)
    if NZ > 1:
        begin_slice(NZ - 1)
        score(NZ - 2)
    score(NZ - 1)
    for i in range(1, G):
        late(i).start()
    def others_of(buf, k):
        ref = buf.at[pl.ds(0, G - 1)]
        return remote(ref, ref, f_send.at[k], f_recv.at[k], dev())

    if G > 1:
        others_of(early_buf, 0).wait_recv()

    def last_of(z):
        return NZ - 1 if z < NZ - 1 else min(1, max(NZ - 2, 0))

    def summed(buf, z):
        out = None
        for x in range(NX):
            for t in range(NY):
                part = buf[(x * NZ + z) * NY + t]
                out = part if out is None else out + part
        return out

    empty = jnp.zeros((1, lines), jnp.float32)
    totals, chosen, codes = [empty] * NZ, [empty] * NZ, [empty] * NZ
    for z in range(NZ):
        sums = summed(early_buf, z)
        for w in range(NZ):
            if w == last_of(z):
                codes[z] = sums[w:w + 1]
            else:
                totals[w] = totals[w] + sums[w:w + 1]
                chosen[w] = chosen[w] + sums[NZ + w:NZ + w + 1]
    if G > 1:
        others_of(late_buf, 1).wait_recv()
    for z in range(NZ):
        sums = summed(late_buf, z)
        totals[last_of(z)] = totals[last_of(z)] + sums[0:1]
        chosen[last_of(z)] = chosen[last_of(z)] + sums[1:2]
    totals, chosen, code = (jnp.concatenate(p, axis=0) for p in (totals, chosen, codes))
    inside = lax.rem(lax.broadcasted_iota(jnp.int32, (NZ, lines), 1), PAD) < rows
    counted = jnp.where(inside & (code >= docs), 1.0, 0.0)
    doc = jnp.where(code >= docs, code - docs, code)
    logprob = jnp.where(inside, counted * (chosen - jnp.log(totals)), 0.0)
    names = lax.broadcasted_iota(jnp.int32, (docs, lines), 0).astype(jnp.float32)
    like = jnp.zeros((docs, lines), jnp.float32)
    cnt = jnp.zeros((docs, lines), jnp.float32)
    for r in range(NZ):
        hit = names == doc[r:r + 1, :]
        like = like + jnp.where(hit, logprob[r:r + 1, :], 0.0)
        cnt = cnt + jnp.where(hit, counted[r:r + 1, :], 0.0)
    docs_eye = lax.broadcasted_iota(jnp.int32, (docs, 128), 0) == lax.broadcasted_iota(jnp.int32, (docs, 128), 1)
    sums = [
        jnp.sum(jnp.where(docs_eye, jnp.sum(v, axis=1, keepdims=True), 0.0), axis=0, keepdims=True)
        for v in (like, cnt)
    ]
    twin_buf[me_c, 0:1, :] = sums[0]
    twin_buf[me_c, 1:2, :] = sums[1]
    twin_copies = [
        remote(twin_buf.at[me_c], twin_buf.at[me_c], tw_send.at[0], tw_recv.at[me_c], dev(d=p)) for p in twin
    ]
    for c in twin_copies:
        c.start()
    mine = jnp.zeros((1, rows), jnp.float32)
    for z in range(NZ):
        for x in range(NX):
            mine = jnp.where((me_z == z) & (me_x == x), logprob[z:z + 1, x * PAD:x * PAD + rows], mine)
    out_ref[0:1, :rows] = mine
    for i, p in enumerate(others(me_t, NY)):
        remote(att.at[me_t], att.at[me_t], att_send.at[i], att_recv.at[me_t, 0], dev()).wait_send()
        stat_copy(p, i).wait_send()

    def sent(ref, sem):
        remote(ref, ref, sem, hid_recv.at[0, 0, 0, 0], dev()).wait_send()

    def portion(k, n):
        return hid.at[pl.ds(0, n), 0, 0, pl.ds(*k), :]

    whole = (0, rows)
    for i in range(len(x_peers)):
        sent(portion(whole, NZ), x_send.at[0, i])
    for i in range(len(y_peers)):
        sent(portion(whole, NZ), y_send.at[0, i])

    def relays_sent(n):
        for j in range(len(x_peers)):
            for i in range(len(y_peers)):
                sent(portion(spans[0], n), y_send.at[1 + j, i])
        for j in range(len(y_peers)):
            if K > 1:
                for i in range(len(x_peers)):
                    sent(portion(spans[K - 1], n), x_send.at[1 + j, i])

    @pl.when(under)
    def _():
        relays_sent(NZ)
        if NZ > 2:
            for j in range(len(x_peers)):
                for i in range(len(y_peers)):
                    sent(portion(whole, 1), u_send.at[j, i])

    if NZ > 2:
        @pl.when(bottom)
        def _():
            sent(portion(whole, 1), z_send.at[NZ - 1])

        @pl.when(top)
        def _():
            relays_sent(1)

    for z in range(NZ - 1):
        @pl.when(climbs(z))
        def _(z=z):
            sent(portion(whole, 1), z_send.at[z])

        @pl.when(((z < me_z) & (top | (z == 0))) | falls(z))
        def _(z=z):
            sent(portion(whole, 1), d_send.at[z])
    if NZ > 1:
        @pl.when(top)
        def _():
            segment_copy().wait_send()
            remote(q_ref.at[0], q_ref.at[1], q_send.at[0], q_recv.at[0], dev()).wait_send()

        @pl.when(helper)
        def _():
            remote(over, over, o_send.at[0], o_recv.at[0, 0], dev()).wait_send()
            remote(under_sum, under_sum, o_send.at[1], o_recv.at[1, 0], dev()).wait_send()

    for block in range(NZ - 2):
        @pl.when((me_z >= block) & (me_z < NZ - 2))
        def _(block=block):
            kv_sent(block)
    if G > 1:
        others_of(early_buf, 0).wait_send()
        others_of(late_buf, 1).wait_send()
    for c in voc_copies:
        c.wait_send()
    for p in twin:
        other = lax.rem(p, NC)
        remote(twin_buf.at[other], twin_buf.at[other], tw_send.at[0], tw_recv.at[other], dev()).wait_recv()
    for c in twin_copies:
        c.wait_send()
    both = twin_buf[0]
    for c in range(1, NC):
        both = both + twin_buf[c]
    out_ref[1:3, :] = both


def split(packed, lp_ref, like_ref, cnt_ref):
    lp_ref[...] = packed[0:1, :lp_ref.shape[1]]
    like_ref[...] = packed[1:2, :like_ref.shape[1]]
    cnt_ref[...] = packed[2:3, :cnt_ref.shape[1]]


def local(
    mesh, query_vectors, key_vectors, value_vectors, out_weight, residual, post_gain, final_gain,
    vocab_weight, segment_ids, doc_starts, doc_index, targets,
):
    ND, NZ, NY = mesh.shape["dp"], mesh.shape["seq"], mesh.shape["tensor"]
    rows = query_vectors.shape[0]
    docs = doc_starts.shape[1] * ND
    blocks = ND * NZ
    fw = out_weight.shape[1]
    voc = vocab_weight
    if fw % 128 != 0:
        voc = voc.reshape(voc.shape[0], NY, fw).transpose(1, 0, 2)
    kvw, qw = key_vectors.shape[1], query_vectors.shape[1]
    heads = qw // HEAD_DIM
    groups = kvw // HEAD_DIM
    NC = 2 if ND % 2 == 0 else 1
    NX = ND // NC
    R = blocks * PAD // 128
    f32, bf16, i32 = jnp.float32, jnp.bfloat16, jnp.int32
    dma = pltpu.SemaphoreType.DMA
    lines = NX * PAD
    G = NX * NZ * NY
    anyspace = pl.BlockSpec(memory_space=pl.ANY)
    packed = pl.pallas_call(
        functools.partial(body, (ND, NZ, NY, docs)),
        out_shape=jax.ShapeDtypeStruct((8, 128), f32),
        in_specs=[anyspace] * 12,
        out_specs=pl.BlockSpec(memory_space=pltpu.VMEM),
        scratch_shapes=[
            pltpu.VMEM((2, *query_vectors.shape), bf16),
            pltpu.VMEM((rows, 128), i32),
            pltpu.VMEM(query_vectors.shape, bf16),
            pltpu.VMEM((groups, 8, 128), f32),
            pltpu.VMEM(residual.shape, bf16),
            pltpu.VMEM(post_gain.shape, f32),
            pltpu.VMEM(final_gain.shape, f32),
            pltpu.VMEM((2, *segment_ids.shape), i32),
            pltpu.SMEM(doc_starts.shape, i32),
            pltpu.SMEM(doc_index.shape, i32),
            pltpu.VMEM(targets.shape, i32),
            pltpu.VMEM(out_weight.shape, bf16),
            pltpu.VMEM((NC, *voc.shape), bf16),
            pltpu.VMEM((NZ, 2, rows, kvw), bf16),
            pltpu.VMEM((2 * heads, rows, HEAD_DIM), f32),
            pltpu.VMEM((2 * heads, rows, 128), f32),
            pltpu.VMEM((NY, rows, qw), bf16),
            pltpu.VMEM((rows, fw), f32),
            pltpu.VMEM((NY, rows, 128), f32),
            pltpu.VMEM((NZ, NY, NX, PAD, fw), bf16),
            pltpu.VMEM((NZ, NC, voc.shape[-2], lines), f32),
            pltpu.VMEM((NZ, 1, lines), i32),
            pltpu.VMEM((G, 2 * NZ, lines), f32),
            pltpu.VMEM((G, 2, lines), f32),
            pltpu.VMEM((NC, 2, 128), f32),
            dma((12,)),
            dma((2,)), dma((groups + 1,)),
            dma((2,)), dma((2, groups)),
            dma((NZ,)), dma((NZ, groups)),
            dma((NY,)), dma((NY, groups)),
            dma((NY,)), dma((NY,)),
            dma((NZ, NY, NX, 2)),
            dma((NZ,)),
            dma((NZ,)),
            dma((NX, NY)),
            pltpu.SemaphoreType.REGULAR((2,)),
            dma((NX, NY)),
            dma((NY, NX)),
            dma((1,)), dma((NC,)),
            dma((2,)), dma((2,)),
            dma((1,)), dma((NC,)),
        ],
        compiler_params=pltpu.CompilerParams(
            collective_id=0, has_side_effects=True, vmem_limit_bytes=60 * 1024 * 1024
        ),
        name="packed_loglik",
    )(
        query_vectors, key_vectors, value_vectors, out_weight, residual, post_gain, final_gain, voc,
        segment_ids, doc_starts, doc_index, targets,
    )
    sums = jax.ShapeDtypeStruct((1, docs), f32)
    logprob, like, counts = pl.pallas_call(
        split, out_shape=(jax.ShapeDtypeStruct((1, rows), f32), sums, sums), name="split"
    )(packed)
    return (logprob, like[0], counts[0])


def solution(mesh):
    in_specs = (
        P(("dp", "seq"), "tensor"),
        P(("dp", "seq"), "tensor"),
        P(("dp", "seq"), "tensor"),
        P(None, "tensor"),
        P(("dp", "seq"), "tensor"),
        P("tensor"),
        P("tensor"),
        P(("dp", "seq", "tensor"), None),
        P("dp", "seq"),
        P("dp", None),
        P("dp", None),
        P(),
    )
    out_specs = (P("dp", "seq"), P(), P())
    return jax.shard_map(
        functools.partial(local, mesh), mesh=mesh, in_specs=in_specs, out_specs=out_specs, check_vma=False
    )
```
